8 devices in a mesh: pair: 1 (over z), tp: 2 (over y), side: 4 (over x, core).
Axes of the slice: x: 2, y: 2, z: 1, core: 2. Of those that a mesh axis runs over, the one named last changes fastest.
Arguments:
- x: bfloat16 [2048, 4096], P(('pair', 'side'))
- req_len: int32 [4], P('pair')
- dest: int32 [4], P('pair')
- w_qkv: bfloat16 [2, 4096, 12288], replicated
- w_out: bfloat16 [2, 4096, 4096], replicated
- w_gate: bfloat16 [2, 4096, 11008], replicated
- w_up: bfloat16 [2, 4096, 11008], replicated
- w_down: bfloat16 [2, 11008, 4096], replicated
- y_tok: bfloat16 [4, 32, 4096], P(('pair', 'side'))
- k_cache: bfloat16 [4, 2, 32, 64, 32, 128], P(('pair', 'side'), None, None, None, 'tp')
- v_cache: bfloat16 [4, 2, 32, 64, 32, 128], P(('pair', 'side'), None, None, None, 'tp')
- c_len: int32 [4, 32], P(('pair', 'side'))
Outputs:
- output 1: bfloat16 [2048, 4096], P(('pair', 'side'))
- output 2: bfloat16 [4, 32, 4096], P(('pair', 'side'))
- output 3: bfloat16 [4, 2, 896, 32, 128], P(('pair', 'side'), None, None, 'tp')
- output 4: bfloat16 [4, 2, 896, 32, 128], P(('pair', 'side'), None, None, 'tp')
- output 5: bfloat16 [4, 2, 32, 64, 32, 128], P(('pair', 'side'), None, None, None, 'tp')
- output 6: bfloat16 [4, 2, 32, 64, 32, 128], P(('pair', 'side'), None, None, None, 'tp')
All inputs are finite; a program needn't handle non-finite values.
Results may differ from the reference program's by a relative error of at most 0.0168853.
Values are sent between devices in bfloat16 or wider.
A program may use at most 3.5 GiB of HBM per device.

```python
import jax
import jax.numpy as jnp
from jax import lax

TP_SIZE = 2
SIDE_SIZE = 4
MODEL_DIM = 4096
HEADS = 32
KV_HEADS = 32
HEAD_DIM = 128
FF_DIM = 11008
LAYERS = 2
PROMPT_ROWS = 512
BATCH = 32
CACHE_LEN = 64
SEQ_LEN = PROMPT_ROWS * SIDE_SIZE
MAX_REQ = 2 * PROMPT_ROWS - PROMPT_ROWS // 4
GROUP_REP = HEADS // KV_HEADS
KV_LOCAL = KV_HEADS // TP_SIZE
Q_COLS = HEADS * HEAD_DIM
KV_COLS = KV_HEADS * HEAD_DIM
ROPE_BASE = 10000.0
NORM_EPS = 1e-5


def draw_normal(key, shape, scale):
    return (jax.random.normal(key, shape, jnp.float32) * scale).astype(jnp.bfloat16)


def draw_lengths(key):
    quarter = PROMPT_ROWS // 4
    eighth = PROMPT_ROWS // 8
    key_first, key_gap = jax.random.split(key)
    first_len = jax.random.randint(key_first, (SIDE_SIZE // 2,), quarter, 2 * PROMPT_ROWS - quarter + 1)
    gap_len = jax.random.randint(key_gap, (SIDE_SIZE // 2,), 0, eighth + 1)
    first_len = first_len.at[0].set(MAX_REQ)
    gap_len = gap_len.at[0].set(eighth)
    second_len = 2 * PROMPT_ROWS - gap_len - first_len
    return jnp.stack([first_len, second_len], axis=1).reshape(SIDE_SIZE).astype(jnp.int32)


def draw_cache_lengths(key):
    lengths = jax.random.randint(key, (SIDE_SIZE, BATCH), CACHE_LEN // 2, CACHE_LEN)
    lengths = lengths.at[:, 0].set(CACHE_LEN - 1)
    lengths = lengths.at[:, 1].set(CACHE_LEN // 2)
    return lengths.astype(jnp.int32)


def setup_inputs(seed: int = 0, part: int = 0) -> dict:
    part_keys = jax.random.split(jax.random.fold_in(jax.random.key(seed), part), 7)
    weight_keys = jax.random.split(jax.random.key(seed + 1), 5)
    cache_shape = (SIDE_SIZE, LAYERS, BATCH, CACHE_LEN, KV_HEADS, HEAD_DIM)
    return {
        'x': draw_normal(part_keys[0], (SEQ_LEN, MODEL_DIM), 1.0),
        'req_len': draw_lengths(part_keys[1]),
        'dest': jax.random.permutation(part_keys[2], SIDE_SIZE).astype(jnp.int32),
        'w_qkv': draw_normal(weight_keys[0], (LAYERS, MODEL_DIM, Q_COLS + 2 * KV_COLS), MODEL_DIM ** -0.5),
        'w_out': draw_normal(weight_keys[1], (LAYERS, Q_COLS, MODEL_DIM), Q_COLS ** -0.5),
        'w_gate': draw_normal(weight_keys[2], (LAYERS, MODEL_DIM, FF_DIM), MODEL_DIM ** -0.5),
        'w_up': draw_normal(weight_keys[3], (LAYERS, MODEL_DIM, FF_DIM), MODEL_DIM ** -0.5),
        'w_down': draw_normal(weight_keys[4], (LAYERS, FF_DIM, MODEL_DIM), FF_DIM ** -0.5),
        'y_tok': draw_normal(part_keys[3], (SIDE_SIZE, BATCH, MODEL_DIM), 1.0),
        'k_cache': draw_normal(part_keys[4], cache_shape, 1.0),
        'v_cache': draw_normal(part_keys[5], cache_shape, 1.0),
        'c_len': draw_cache_lengths(part_keys[6]),
    }


def rms_norm(hidden):
    wide_vals = hidden.astype(jnp.float32)
    norm_scale = lax.rsqrt(jnp.mean(wide_vals * wide_vals, axis=-1, keepdims=True) + NORM_EPS)
    return (wide_vals * norm_scale).astype(jnp.bfloat16)


def rotary(vectors, positions):
    half_dim = HEAD_DIM // 2
    inv_freq = ROPE_BASE ** (-jnp.arange(half_dim, dtype=jnp.float32) / half_dim)
    angles = positions.astype(jnp.float32)[:, None, None] * inv_freq
    cos_val = jnp.cos(angles)
    sin_val = jnp.sin(angles)
    wide_vals = vectors.astype(jnp.float32)
    lead_half = wide_vals[..., :half_dim]
    tail_half = wide_vals[..., half_dim:]
    return jnp.concatenate([lead_half * cos_val - tail_half * sin_val, tail_half * cos_val + lead_half * sin_val], axis=-1).astype(jnp.bfloat16)


def b_order(array_in, axis):
    shape_in = array_in.shape
    split_shape = shape_in[:axis] + (KV_LOCAL, TP_SIZE) + shape_in[axis + 1:]
    return jnp.swapaxes(array_in.reshape(split_shape), axis, axis + 1).reshape(shape_in)


def split_qkv(w_qkv):
    return w_qkv[..., :Q_COLS], w_qkv[..., Q_COLS:Q_COLS + KV_COLS], w_qkv[..., Q_COLS + KV_COLS:]


def project(hidden, wq_l, wk_l, wv_l, positions):
    row_count = hidden.shape[0]
    normed = rms_norm(hidden)
    query = jnp.dot(normed, wq_l, preferred_element_type=jnp.float32).astype(jnp.bfloat16)
    key_new = jnp.dot(normed, wk_l, preferred_element_type=jnp.float32).astype(jnp.bfloat16)
    value_new = jnp.dot(normed, wv_l, preferred_element_type=jnp.float32).astype(jnp.bfloat16)
    query = rotary(query.reshape(row_count, HEADS, HEAD_DIM), positions)
    key_new = rotary(key_new.reshape(row_count, KV_HEADS, HEAD_DIM), positions)
    return query.reshape(row_count, KV_HEADS, GROUP_REP, HEAD_DIM), key_new, value_new.reshape(row_count, KV_HEADS, HEAD_DIM)


def finish_layer(hidden, context, wo_l, wg_l, wu_l, wd_l):
    attn_out = jnp.dot(context, wo_l, preferred_element_type=jnp.float32).astype(jnp.bfloat16)
    hidden = (hidden.astype(jnp.float32) + attn_out.astype(jnp.float32)).astype(jnp.bfloat16)
    normed = rms_norm(hidden)
    gate = jnp.dot(normed, wg_l, preferred_element_type=jnp.float32).astype(jnp.bfloat16)
    upper = jnp.dot(normed, wu_l, preferred_element_type=jnp.float32).astype(jnp.bfloat16)
    activated = (jax.nn.silu(gate.astype(jnp.float32)) * upper.astype(jnp.float32)).astype(jnp.bfloat16)
    down = jnp.dot(activated, wd_l, preferred_element_type=jnp.float32).astype(jnp.bfloat16)
    return (hidden.astype(jnp.float32) + down.astype(jnp.float32)).astype(jnp.bfloat16)


def prefill(x, req_len, w_qkv, w_out, w_gate, w_up, w_down):
    row_ids = jnp.arange(SEQ_LEN)
    past_end = row_ids[:, None] >= jnp.cumsum(req_len)[None, :]
    seg_id = jnp.sum(past_end.astype(jnp.int32), axis=1)
    positions = row_ids - jnp.sum(jnp.where(past_end, req_len[None, :], 0), axis=1)
    allowed = (seg_id[:, None] == seg_id[None, :]) & (row_ids[None, :] <= row_ids[:, None])
    w_q, w_k, w_v = split_qkv(w_qkv)

    def head_attention(operands):
        q_head, k_head, v_head = operands
        scores = jnp.einsum('srd,td->rst', q_head.astype(jnp.float32), k_head.astype(jnp.float32)) * HEAD_DIM ** -0.5
        scores = jnp.where(allowed[None], scores, -1e30)
        attn_prob = jax.nn.softmax(scores, axis=-1).astype(jnp.bfloat16)
        return jnp.einsum('rst,td->srd', attn_prob.astype(jnp.float32), v_head.astype(jnp.float32)).astype(jnp.bfloat16)

    def layer_step(hidden, weights):
        wq_l, wk_l, wv_l, wo_l, wg_l, wu_l, wd_l = weights
        query, key_new, value_new = project(hidden, wq_l, wk_l, wv_l, positions)
        context = lax.map(head_attention, (jnp.swapaxes(query, 0, 1), jnp.swapaxes(key_new, 0, 1), jnp.swapaxes(value_new, 0, 1)))
        context = jnp.swapaxes(context, 0, 1).reshape(SEQ_LEN, Q_COLS)
        return finish_layer(hidden, context, wo_l, wg_l, wu_l, wd_l), (key_new, value_new)

    return lax.scan(layer_step, x, (w_q, w_k, w_v, w_out, w_gate, w_up, w_down))


def install(full, req_len, dest):
    starts = jnp.cumsum(req_len) - req_len
    match = dest[None, :] == jnp.arange(SIDE_SIZE)[:, None]
    start_of = jnp.sum(jnp.where(match, starts[None, :], 0), axis=1)
    length_of = jnp.sum(jnp.where(match, req_len[None, :], 0), axis=1)
    padded = jnp.concatenate([full, jnp.zeros((LAYERS, MAX_REQ, KV_HEADS, HEAD_DIM), full.dtype)], axis=1)

    def one_group(start_row, length):
        piece = lax.dynamic_slice_in_dim(padded, start_row, MAX_REQ, axis=1)
        keep = (jnp.arange(MAX_REQ) < length)[None, :, None, None]
        return b_order(jnp.where(keep, piece, jnp.zeros_like(piece)), 2)

    return jax.vmap(one_group)(start_of, length_of)


def decode(y_tok, k_cache, v_cache, c_len, w_qkv, w_out, w_gate, w_up, w_down):
    w_q, w_k, w_v = split_qkv(w_qkv)
    wq_b = b_order(w_q.reshape(LAYERS, MODEL_DIM, KV_HEADS, GROUP_REP * HEAD_DIM), 2).reshape(LAYERS, MODEL_DIM, Q_COLS)
    wk_b = b_order(w_k.reshape(LAYERS, MODEL_DIM, KV_HEADS, HEAD_DIM), 2).reshape(LAYERS, MODEL_DIM, KV_COLS)
    wv_b = b_order(w_v.reshape(LAYERS, MODEL_DIM, KV_HEADS, HEAD_DIM), 2).reshape(LAYERS, MODEL_DIM, KV_COLS)
    wo_b = b_order(w_out.reshape(LAYERS, KV_HEADS, GROUP_REP * HEAD_DIM, MODEL_DIM), 1).reshape(LAYERS, Q_COLS, MODEL_DIM)
    cache_pos = jnp.arange(CACHE_LEN)

    def one_group(operands):
        tokens, k_group, v_group, lengths = operands
        visible = cache_pos[None, :] <= lengths[:, None]
        at_slot = (cache_pos[None, :] == lengths[:, None])[:, :, None, None]

        def layer_step(hidden, weights):
            wq_l, wk_l, wv_l, wo_l, wg_l, wu_l, wd_l, k_layer, v_layer = weights
            query, key_new, value_new = project(hidden, wq_l, wk_l, wv_l, lengths)
            k_layer = jnp.where(at_slot, key_new[:, None], k_layer)
            v_layer = jnp.where(at_slot, value_new[:, None], v_layer)
            scores = jnp.einsum('bkrd,btkd->bkrt', query.astype(jnp.float32), k_layer.astype(jnp.float32)) * HEAD_DIM ** -0.5
            scores = jnp.where(visible[:, None, None, :], scores, -1e30)
            attn_prob = jax.nn.softmax(scores, axis=-1).astype(jnp.bfloat16)
            context = jnp.einsum('bkrt,btkd->bkrd', attn_prob.astype(jnp.float32), v_layer.astype(jnp.float32)).astype(jnp.bfloat16)
            hidden = finish_layer(hidden, context.reshape(BATCH, Q_COLS), wo_l, wg_l, wu_l, wd_l)
            return hidden, (k_layer, v_layer)

        hidden, (k_new, v_new) = lax.scan(layer_step, tokens, (wq_b, wk_b, wv_b, wo_b, w_gate, w_up, w_down, k_group, v_group))
        return hidden, k_new, v_new

    return lax.map(one_group, (y_tok, k_cache, v_cache, c_len))


def reference(x, req_len, dest, w_qkv, w_out, w_gate, w_up, w_down, y_tok, k_cache, v_cache, c_len):
    hidden, (keys_all, values_all) = prefill(x, req_len, w_qkv, w_out, w_gate, w_up, w_down)
    k_prompt = install(keys_all, req_len, dest)
    v_prompt = install(values_all, req_len, dest)
    dec_out, k_new, v_new = decode(y_tok, k_cache, v_cache, c_len, w_qkv, w_out, w_gate, w_up, w_down)
    return (hidden, dec_out, k_prompt, v_prompt, k_new, v_new)
```

```python
import jax
import jax.numpy as jnp
from jax import lax
from jax.experimental import pallas as pl
from jax.experimental.pallas import tpu as pltpu
from jax.sharding import PartitionSpec as P

ROPE_BASE = 10000.0
NORM_EPS = 1e-5
NEG = -1e30
BF = jnp.bfloat16
F32 = jnp.float32
ANY = pl.BlockSpec(memory_space=pl.ANY)
SMEM = pl.BlockSpec(memory_space=pltpu.SMEM)
WHOLE = pl.BlockSpec(memory_space=pltpu.VMEM)
VMEM_LIMIT = 61 * 2**20
LOG2E = 1.4426950408889634
LANES = 128
WIDE = 256
CHUNK = 512
HALVES = (0, WIDE)
SUB = 16
PER = 4
EARLY_SENT = 5
dma = pltpu.make_async_copy
sds = jax.ShapeDtypeStruct
sem = pltpu.SemaphoreType.DMA


def at(start, size, multiple=LANES):
    return pl.ds(pl.multiple_of(start, multiple), size)


def cost(flops, size):
    return pl.CostEstimate(flops=flops, bytes_accessed=size, transcendentals=0)


def params(**kw):
    return pltpu.CompilerParams(vmem_limit_bytes=VMEM_LIMIT, **kw)


def remote(src, dst, send, recv, dev):
    return pltpu.make_async_remote_copy(src_ref=src, dst_ref=dst, send_sem=send, recv_sem=recv, device_id=dev, device_id_type=pl.DeviceIdType.MESH)


def meet(devices):
    barrier = pltpu.get_barrier_semaphore()
    for dev in devices:
        pl.semaphore_signal(barrier, device_id=dev, device_id_type=pl.DeviceIdType.MESH)
    pl.semaphore_wait(barrier, len(devices))


def each(count, fn):
    lax.fori_loop(0, count, lambda i, c: (fn(i), c)[1], 0)


def begin(copies):
    for cp in copies:
        cp.start()


def finish_all(copies):
    for cp in copies:
        cp.wait()


def norm_rows(src, dst, base, rows):
    def step(i):
        sl = at(base + i * SUB, SUB, SUB)
        wide = src[sl, :].astype(F32)
        scale = lax.rsqrt(jnp.mean(wide * wide, axis=-1, keepdims=True) + NORM_EPS)
        dst[sl, :] = (wide * scale).astype(BF)
    each(rows // SUB, step)


class Dims:
    def __init__(self, rows, dec, model, heads, head_dim, ff, max_req):
        self.rows, self.half = rows, rows // 2
        self.dec, self.dhalf = dec, dec // 2
        self.blk = self.half + self.dhalf
        self.all = 2 * self.blk
        self.model, self.heads, self.hd, self.ff = model, heads, head_dim, ff
        self.max_req = max_req
        self.loc = heads * head_dim
        self.window = LANES + 2 * rows
        self.lanes = (0, model, LANES)


def front_call(dm, layer, first, ins, w_qkv, tab_c, tab_s, perm, lengths, ends, kc, vc):
    nb = 4
    per_sec = dm.heads // PER
    steps = 3 * per_sec
    kv_steps = 2 * per_sec
    h, d, k = dm.half, dm.dhalf, dm.blk
    m = dm.all if first else k
    npass = dm.all // m
    width = PER * dm.hd
    lead = dm.window - dm.rows
    batch, cache = kc.shape[2], kc.shape[3]
    flat = cache * dm.heads
    ring = 3
    dsteps = batch // PER
    ni = len(ins)

    def kern(*refs):
        rin = refs[:ni]
        (w_ref, c_ref, s_ref, perm_ref, len_ref, end_ref, k_ref, v_ref, kvh, kv3, qh, dec, co, ci, do, di,
         xn, wb, kcat, qv, sd, dv, acc_a, acc_b, bias, sbuf, pbuf, cbuf, cr, dsc, dbuf, dout, o3, stat, raw,
         wsem, isem, csem, tsem, pss, prs, ess, ers, yss, yrs, lss, lrs) = refs[ni:]
        tp = lax.axis_index('tp')
        side = lax.axis_index('side')
        odd = lax.rem(side, 2)
        to_y = {'tp': 1 - tp}

        def wcopies(i):
            slot = lax.rem(i, nb)
            j = lax.rem(i, steps)
            sec = j // per_sec
            base = jnp.where(sec == 2, 0, (sec + 1) * 2 * dm.loc)
            out = []
            for n in range(PER):
                col = base + (2 * (PER * lax.rem(j, per_sec) + n) + tp) * dm.hd
                out.append(dma(w_ref.at[layer, :, at(col, dm.hd)], wb.at[slot, :, pl.ds(n * dm.hd, dm.hd)], wsem.at[slot, n]))
            return out

        def caches(i):
            slot = lax.rem(i, ring)
            b = at(PER * i, PER, PER)
            return [dma(ref.at[0, layer, b], cr.at[slot, n], csem.at[slot, n]) for n, ref in enumerate((k_ref, v_ref))]

        if first:
            parts = [(rin[0], 0, 0, h), (rin[1], 0, h, d), (rin[0], h, k, h), (rin[1], d, k + h, d)]
            loads = [dma(ref.at[pl.ds(src, n)], xn.at[pl.ds(dst, n)], isem.at[i]) for i, (ref, src, dst, n) in enumerate(parts)]
        else:
            own1, own2, peer1, ss_in = rin
            cut = own1.shape[1]
            head_cols, tail_cols = pl.ds(0, cut), pl.ds(cut, dm.model - cut)
            top, low_rows = pl.ds(0, k), pl.ds(k, k)
            loads = [dma(own1, xn.at[top, head_cols], isem.at[0]), dma(own2, xn.at[top, tail_cols], isem.at[1]),
                     dma(ss_in, stat.at[0], isem.at[2]), dma(peer1, xn.at[low_rows, head_cols], isem.at[3]), dma(own2, raw, tsem.at[0])]
        begin(loads)
        for i in range(nb - 1):
            begin(wcopies(jnp.int32(i)))
        begin(caches(jnp.int32(0)))

        def zero(i):
            kcat[:, i, pl.ds(0, lead), :] = jnp.zeros((2, lead, dm.hd), BF)
        each(dm.heads, zero)
        meet([{'side': lax.rem(side + i, 4)} for i in range(1, 4)] + [to_y])
        late = []
        if not first:
            loads[4].wait()
            late = [remote(raw, xn.at[low_rows, tail_cols], lss.at[0], lrs.at[0], to_y),
                    remote(ss_in, stat.at[1], lss.at[1], lrs.at[1], to_y)]
            begin(late[::-1])

        def own_part(j):
            return kcat.at[j // per_sec, at(PER * lax.rem(j, per_sec), PER, PER), pl.ds(lead, dm.rows)]

        def edge_part(j, row):
            return kcat.at[j // per_sec, at(PER * lax.rem(j, per_sec), PER, PER), pl.ds(row, LANES)]

        def peer_copy(j):
            dst = kcat.at[j // per_sec, at(PER * lax.rem(j, per_sec), PER, PER), pl.ds(LANES, dm.rows)]
            return remote(own_part(j), dst, pss.at[j], prs.at[j], {'side': side + 1})

        def edge_copy(j, to):
            row = dm.window - LANES if to == 2 else dm.rows
            return remote(edge_part(j, row), edge_part(j, (3 - to) * dm.rows), ess.at[j], ers.at[j], {'side': to})

        def send(j):
            pl.when(odd == 0)(lambda: peer_copy(j).start())
            pl.when(side == 1)(lambda: edge_copy(j, 2).start())

        def arrived(j):
            pl.when(odd == 1)(lambda: peer_copy(j).wait_recv())

            @pl.when(side == 2)
            def _():
                edge_copy(j, 2).wait_recv()
                edge_copy(j, 3).start()
            pl.when(side == 3)(lambda: edge_copy(j, 3).wait_recv())

        def sent(j):
            pl.when(odd == 0)(lambda: peer_copy(j).wait_send())
            pl.when(side == 1)(lambda: edge_copy(j, 2).wait_send())
            pl.when(side == 2)(lambda: edge_copy(j, 3).wait_send())

        def dots(i, rows, acc):
            @pl.when(i + nb - 1 < npass * steps)
            def _():
                begin(wcopies(i + nb - 1))
            finish_all(wcopies(i))
            acc[...] = jnp.dot(xn[rows, :], wb[lax.rem(i, nb)], preferred_element_type=F32)

        def epilogue(j, acc, blocks, is_q):
            sec, jj = j // per_sec, lax.rem(j, per_sec)
            for r0, b in blocks:
                rows = slice(r0, r0 + k)
                cv, sv = c_ref[at(b * k, k, SUB), :], s_ref[at(b * k, k, SUB), :]
                for n in range(PER):
                    head = PER * jj + n
                    val = acc[rows, n * dm.hd:(n + 1) * dm.hd].astype(BF).astype(F32)
                    rot = val * cv + pltpu.roll(val, dm.hd // 2, 1) * sv
                    low = (rot if is_q else jnp.where(sec == 1, val, rot)).astype(BF)
                    if is_q:
                        qv[head, at(b * h, h, SUB), :] = low[:h]
                    else:
                        kcat[sec, head, at(lead + b * h, h, SUB), :] = low[:h]
                    sd[sec, head, at(b * d, d, d), :] = low[h:]

        def run(p, blocks):
            rows = pl.ds(p * m, m)
            base = p * steps
            final = p == npass - 1
            last = kv_steps

            def done(j):
                if final:
                    pl.when(j > 0)(lambda: send(j - 1))

            dots(jnp.int32(base), rows, acc_a)

            def pair(q):
                dots(base + 2 * q + 1, rows, acc_b)
                epilogue(2 * q, acc_a, blocks, False)
                done(2 * q)
                dots(base + 2 * q + 2, rows, acc_a)
                epilogue(2 * q + 1, acc_b, blocks, False)
                done(2 * q + 1)
            each(last // 2 - 1, pair)
            dots(jnp.int32(base + last - 1), rows, acc_b)
            epilogue(jnp.int32(last - 2), acc_a, blocks, False)
            done(jnp.int32(last - 2))
            if final:
                epilogue(jnp.int32(last - 1), acc_b, blocks, False)
                done(jnp.int32(last - 1))
                return
            dots(jnp.int32(base + last), rows, acc_a)
            epilogue(jnp.int32(last - 1), acc_b, blocks, False)
            for n in range(1, per_sec):
                prev, acc = (acc_a, acc_b) if n % 2 else (acc_b, acc_a)
                dots(jnp.int32(base + last + n), rows, acc)
                epilogue(jnp.int32(last + n - 1), prev, blocks, True)
            epilogue(jnp.int32(steps - 1), acc, blocks, True)

        def apply_norm(n, base):
            total_sq = jnp.sum(stat[n], axis=1, keepdims=True)
            stat[n] = jnp.broadcast_to(lax.rsqrt(total_sq / dm.model + NORM_EPS), (k, LANES))

            def step(i):
                sl = at(base + i * SUB, SUB, SUB)
                for c in range(*dm.lanes):
                    xn[sl, c:c + LANES] = (xn[sl, c:c + LANES].astype(F32) * stat[n, at(i * SUB, SUB, SUB), :]).astype(BF)
            each(k // SUB, step)

        if first:
            finish_all(loads)
            norm_rows(xn, xn, 0, m)
            blocks = [(0, 0), (k, 1)]
        else:
            finish_all(loads[:3])
            apply_norm(0, 0)
            run(0, [(0, tp)])
            loads[3].wait()
            finish_all(late)
            apply_norm(1, k)
            blocks = [(0, 1 - tp)]
        run(npass - 1, blocks)

        def cols(g):
            return at(width * g, width)

        def ctx_send(g):
            return remote(cbuf.at[0, :, cols(g)], ci.at[:, cols(g)], yss.at[g], yrs.at[g], to_y)

        dec_send = remote(dout.at[at((1 - tp) * d, d, SUB)], di, yss.at[per_sec], yrs.at[per_sec], to_y)
        dec_keep = dma(dout.at[at(tp * d, d, SUB)], do, isem.at[0])

        def score(b, w, head, n):
            sbuf[n % 2, :, :w] = lax.dot_general(qv[head, b * h:(b + 1) * h, :], kcat[0, head, :w, :], (((1,), (1,)), ((), ())), preferred_element_type=F32)

        def value(ph, w, head, n):
            s = sbuf[n % 2, :, :w] * (dm.hd ** -0.5 * LOG2E) + bias[:, :w]
            p = jnp.exp2(s - jnp.max(s, axis=1, keepdims=True))
            pbuf[n % 2, :, :w] = p.astype(BF)
            tot = jnp.sum(p, axis=1, keepdims=True)
            o = jnp.dot(pbuf[n % 2, :, :w], kcat[1, head, :w, :], preferred_element_type=F32)
            cbuf[ph, :, at(head * dm.hd, dm.hd)] = (o / tot).astype(BF)

        def turn_rows(rows, out):
            x = jnp.concatenate([r.reshape(SUB * dm.heads, dm.hd) for r in rows], axis=1)
            y = jnp.dot(perm_ref[...], x, preferred_element_type=F32).astype(BF)
            for n, dst in enumerate(out):
                dst(y[:, n * dm.hd:(n + 1) * dm.hd].reshape(SUB, dm.heads, dm.hd))

        def decode():
            col = lax.broadcasted_iota(jnp.int32, (dm.heads, flat), 1)
            row = lax.broadcasted_iota(jnp.int32, (dm.heads, flat), 0)
            pos = jnp.where(lax.rem(col, dm.heads) == row, col // dm.heads, flat)
            scale = dm.hd ** -0.5

            def look(i, par):
                @pl.when(i + 1 < dsteps)
                def _():
                    begin(caches(i + 1))
                finish_all(caches(i))
                for n in range(PER):
                    keys = cr[lax.rem(i, ring), 0, n].reshape(flat, dm.hd)
                    dsc[par, n] = lax.dot_general(dv[2, PER * i + n], keys, (((1,), (1,)), ((), ())), preferred_element_type=F32)

            def gather(i, par):
                for n in range(PER):
                    bi = PER * i + n
                    q, kn, vn = dv[2, bi].astype(F32), dv[0, bi].astype(F32), dv[1, bi].astype(F32)
                    s = jnp.where(pos < len_ref[bi], dsc[par, n] * scale, NEG)
                    fresh = jnp.sum(q * kn, axis=1, keepdims=True) * scale
                    top = jnp.maximum(jnp.max(s, axis=1, keepdims=True), fresh)
                    p = jnp.exp(s - top)
                    pf = jnp.exp(fresh - top)
                    inv = 1.0 / (jnp.sum(p, axis=1, keepdims=True) + pf)
                    vals = cr[lax.rem(i, ring), 1, n].reshape(flat, dm.hd)
                    o = jnp.dot((p * inv).astype(BF), vals, preferred_element_type=F32)
                    dbuf[bi] = o + (pf * inv).astype(BF).astype(F32) * vn

            look(jnp.int32(0), 0)

            def two(t):
                look(2 * t + 1, 1)
                gather(2 * t, 0)
                look(2 * t + 2, 0)
                gather(2 * t + 1, 1)
            each(dsteps // 2 - 1, two)
            look(jnp.int32(dsteps - 1), 1)
            gather(jnp.int32(dsteps - 2), 0)
            gather(jnp.int32(dsteps - 1), 1)
            for n in range(dm.heads):
                dout[:, n * dm.hd:(n + 1) * dm.hd] = dbuf[:, n, :].astype(BF)

        def put(ref, *idx):
            def store(val):
                ref[idx] = val
            return store

        def turn_all():
            def block(i):
                for n in range(PER):
                    row = (PER * i + n) * SUB
                    sl, own = at(row, SUB, SUB), at(lead + row, SUB, SUB)
                    turn_rows([kcat[0, :, own, :], kcat[1, :, own, :]], [put(o3, 0, sl), put(o3, 1, sl)])
            each(dm.rows // SUB // PER, block)

        kv3_copy = dma(o3, kv3, tsem.at[0])
        kvh_copy = dma(kcat.at[:, :, pl.ds(lead, dm.rows)], kvh, tsem.at[1])
        q_copy = dma(qv, qh, tsem.at[2])
        dec_copy = dma(dv, dec, tsem.at[3])

        def stage(t):
            ph, g = t // per_sec, lax.rem(t, per_sec)
            b = lax.rem(1 + tp + ph, 2)

            @pl.when(ph == 0)
            def _():
                dots(npass * steps - per_sec + g, pl.ds((npass - 1) * m, m), acc_a)
                epilogue(kv_steps + g, acc_a, blocks, True)
                pl.when(g == 0)(lambda: send(kv_steps - 1))
                arrived(g)
                arrived(per_sec + g)

            @pl.when(t == per_sec)
            def _():
                for i in range(dm.dec // SUB):
                    sl = pl.ds(i * SUB, SUB)
                    turn_rows([sd[n, :, sl, :] for n in range(3)], [put(dv, n, sl) for n in range(3)])
                turn_all()
                begin([kv3_copy, kvh_copy, q_copy, dec_copy])
                ctx_send(per_sec - 1).start()
                decode()

            @pl.when(g == 0)
            def _():
                row0 = dm.rows * side + h * b
                for c in range(dm.window // LANES):
                    rows = row0 + lax.broadcasted_iota(jnp.int32, (h, LANES), 0)
                    col = dm.rows * side - lead + c * LANES + lax.broadcasted_iota(jnp.int32, (h, LANES), 1)
                    start = jnp.zeros_like(rows)
                    for r in range(4):
                        start = jnp.where(rows >= end_ref[r], end_ref[r], start)
                    bias[:, c * LANES:(c + 1) * LANES] = jnp.where((col >= start) & (col <= rows), 0.0, NEG)
            pl.when(t == per_sec)(lambda: begin([dec_send, dec_keep]))

            for bb, w in enumerate((dm.window - h, dm.window)):
                @pl.when(b == bb)
                def _(bb=bb, w=w):
                    score(bb, w, PER * g, 0)
                    for n in range(PER):
                        if n + 1 < PER:
                            score(bb, w, PER * g + n + 1, n + 1)
                        value(ph, w, PER * g + n, n)
            pl.when((ph == 0) & (g > 0))(lambda: ctx_send(g - 1).start())
        each(2 * per_sec, stage)

        keep = dma(cbuf.at[1], co, isem.at[1])
        keep.start()
        each(kv_steps, sent)
        finish_all([kv3_copy, kvh_copy, q_copy, dec_copy, dec_keep, dec_send])
        each(per_sec, lambda g: ctx_send(g).wait())
        keep.wait()

    heads = (dm.heads, dm.rows, dm.hd)
    three = (dm.heads, dm.hd)
    flops = 2 * dm.all * dm.model * width * steps
    outs = [(2,) + heads, (2, dm.rows) + three, heads, (3, dm.dec) + three, (h, dm.loc), (h, dm.loc), (d, dm.loc), (d, dm.loc)]
    acc = pltpu.VMEM((m, width), F32)
    vec = sem((kv_steps,))
    return pl.pallas_call(
        kern, out_shape=tuple(sds(s, BF) for s in outs),
        in_specs=[ANY] * (ni + 1) + [WHOLE] * 3 + [SMEM] * 2 + [ANY] * 2, out_specs=(ANY,) * len(outs),
        scratch_shapes=[
            pltpu.VMEM((dm.all, dm.model), BF), pltpu.VMEM((nb, dm.model, width), BF), pltpu.VMEM((2, dm.heads, dm.window, dm.hd), BF),
            pltpu.VMEM(heads, BF), pltpu.VMEM((3, dm.heads, dm.dec, dm.hd), BF), pltpu.VMEM((3, dm.dec) + three, BF), acc, acc,
            pltpu.VMEM((h, dm.window), F32), pltpu.VMEM((2, h, dm.window), F32), pltpu.VMEM((2, h, dm.window), BF), pltpu.VMEM((2, h, dm.loc), BF),
            pltpu.VMEM((ring, 2, PER, cache) + three, BF), pltpu.VMEM((2, PER, dm.heads, flat), F32), pltpu.VMEM((batch,) + three, F32),
            pltpu.VMEM((batch, dm.loc), BF), pltpu.VMEM((2, dm.rows) + three, BF), pltpu.VMEM((2, k, LANES), F32), pltpu.VMEM((k, dm.model - EARLY_SENT * CHUNK), BF),
            sem((nb, PER)), sem((4,)), sem((ring, 2)), sem((4,)), vec, vec, vec, vec,
            sem((per_sec + 1,)), sem((per_sec + 1,)), sem((2,)), sem((2,))],
        compiler_params=params(collective_id=layer, has_side_effects=True),
        cost_estimate=cost(flops, dm.model * width * steps * 2),
        name="front")(*ins, w_qkv, tab_c, tab_s, perm, lengths, ends, kc, vc)


def general_attention(dm, meta, qh, kvs):
    nk = LANES + 4 * dm.rows
    groups = dm.heads // PER
    hb = dm.half
    wmax = dm.max_req + hb + WIDE

    def kern(meta_ref, q_ref, *refs):
        srcs = refs[:4]
        o_ref, kcat, sc, bias, mx, ls, pv, lsem = refs[4:]
        g = pl.program_id(0)
        side = lax.axis_index('side')
        row0 = dm.rows * side + hb * meta_ref[0]
        copies = [dma(ref.at[:, at(PER * g, PER, PER)], kcat.at[:, :, at(LANES + dm.rows * (side ^ n), dm.rows)], lsem.at[n]) for n, ref in enumerate(srcs)]
        kcat[:, :, :LANES, :] = jnp.zeros((2, PER, LANES, dm.hd), BF)
        begin(copies)

        def seg_start(row):
            st = jnp.zeros_like(row)
            for r in range(4):
                st = jnp.where(row >= meta_ref[1 + r], meta_ref[1 + r], st)
            return st

        n = (row0 + hb - seg_start(row0) // LANES * LANES + WIDE - 1) // WIDE
        begin_col = row0 + hb - WIDE * n
        rows = row0 + lax.broadcasted_iota(jnp.int32, (hb, WIDE), 0)
        st_rows = seg_start(rows)
        lanes = lax.broadcasted_iota(jnp.int32, (hb, WIDE), 1)
        mx[...] = jnp.full_like(mx, NEG)
        ls[...] = jnp.zeros_like(ls)
        pv[...] = jnp.zeros_like(pv)
        finish_all(copies)

        def scores(c):
            first = begin_col + WIDE * c
            col = first + lanes
            bias[...] = jnp.where((col >= st_rows) & (col <= rows), 0.0, NEG)
            for i in range(PER):
                keys = kcat[0, i, at(LANES + first, WIDE), :]
                s = lax.dot_general(q_ref[i], keys, (((1,), (1,)), ((), ())), preferred_element_type=F32)
                s = s * (dm.hd ** -0.5 * LOG2E) + bias[...]
                sc[i, :, at(c * WIDE, WIDE)] = s
                mx[i] = jnp.maximum(mx[i], jnp.max(s, axis=1, keepdims=True))
        each(n, scores)

        def values(c):
            for i in range(PER):
                p = jnp.exp2(sc[i, :, at(c * WIDE, WIDE)] - mx[i][:, :1])
                ls[i] += jnp.sum(p, axis=1, keepdims=True)
                vals = kcat[1, i, at(LANES + begin_col + WIDE * c, WIDE), :]
                pv[i] += jnp.dot(p.astype(BF), vals, preferred_element_type=F32)
        each(n, values)
        for i in range(PER):
            o_ref[:, i * dm.hd:(i + 1) * dm.hd] = (pv[i] / ls[i]).astype(BF)

    stat = pltpu.VMEM((PER, hb, LANES), F32)
    grid_spec = pltpu.PrefetchScalarGridSpec(
        num_scalar_prefetch=1, grid=(groups,),
        in_specs=[pl.BlockSpec((PER, hb, dm.hd), lambda g, mt: (g, mt[0], 0))] + [ANY] * 4,
        out_specs=pl.BlockSpec((hb, PER * dm.hd), lambda g, mt: (0, g)),
        scratch_shapes=[pltpu.VMEM((2, PER, nk, dm.hd), BF), pltpu.VMEM((PER, hb, wmax), F32), pltpu.VMEM((hb, WIDE), F32), stat, stat, stat, sem((4,))])
    return pl.pallas_call(
        kern, out_shape=sds((hb, dm.loc), BF), grid_spec=grid_spec,
        compiler_params=params(dimension_semantics=("arbitrary",)), name="general_attn")(meta, qh, *kvs)


def post_call(dm, layer, first, resid, co, do, ci, di, kv3, w_out, w_gate, w_up, w_down):
    nb = 6
    kc = dm.model
    ffh = dm.ff // 2
    n_out = dm.model // CHUNK
    n_full = ffh // WIDE
    rem = ffh - n_full * WIDE
    n_gu = n_full + 1
    n_dn = n_out
    ksz = [kc, ffh - kc]
    nk = len(ksz)
    gu0, dn0 = n_out, n_out + n_gu
    total = dn0 + n_dn * nk
    assert rem and n_full % 2
    m = dm.blk
    h, d = dm.half, dm.dhalf
    crow = dm.rows // n_dn
    nr = len(resid)
    cut = EARLY_SENT * CHUNK

    def kern(*refs):
        rin = refs[:nr]
        (co_r, do_r, ci_r, di_r, kv, wo, wg, wu, wd, oa, ot, ob, os, kvx, kvp, kvq,
         h1, h1p, xn, act, tmp, wb, acc_a, acc_b, psend, precv, pown, ss, ssp,
         wsem, isem, osem, hss, hrs, pss, prs, yss, yrs, xss, xrs, fss, frs, dss, drs) = refs[nr:]
        tp = lax.axis_index('tp')
        side = lax.axis_index('side')
        core = lax.rem(side, 2)
        to_core = {'side': side + 1 - 2 * core}
        to_x = {'side': lax.rem(side + 2, 4)}
        to_y = {'tp': 1 - tp}

        def cols(j):
            return at(j * CHUNK, CHUNK)

        def block(i, fn):
            slot = lax.rem(i, nb)

            @pl.when(i < gu0)
            def _():
                fn(dma(wo.at[layer, :, cols(i)], wb.at[slot], wsem.at[slot, 0]))

            for on, w in (((i >= gu0) & (i < dn0 - 1), WIDE), (i == dn0 - 1, rem)):
                @pl.when(on)
                def _(w=w):
                    c = at(core * ffh + (i - gu0) * WIDE, w)
                    for n, ref in enumerate((wg, wu)):
                        fn(dma(ref.at[layer, :, c], wb.at[slot, :, pl.ds(n * w, w)], wsem.at[slot, n]))

            j = i - dn0
            for n in range(nk):
                @pl.when((j >= 0) & (i < total) & (lax.rem(j, nk) == n))
                def _(n=n):
                    r = at(core * ffh + n * kc, ksz[n])
                    fn(dma(wd.at[layer, r, cols(j // nk)], wb.at[slot, pl.ds(0, ksz[n])], wsem.at[slot, 0]))

        def start(i):
            block(i, lambda c: c.start())

        def wait(i):
            block(i, lambda c: c.wait())

        mine, theirs = at(tp * h, h, SUB), at(tp * d, d, SUB)
        head_rows, tail_rows = pl.ds(0, h), pl.ds(h, d)
        pairs = [(co_r, tmp.at[0, head_rows]), (do_r, tmp.at[0, tail_rows]), (ci_r, tmp.at[1, head_rows]), (di_r, tmp.at[1, tail_rows])]
        if first:
            pairs += [(rin[0].at[mine], h1.at[head_rows]), (rin[1].at[theirs], h1.at[tail_rows])]
        else:
            pairs += [(rin[0], h1.at[:, pl.ds(0, cut)]), (rin[1], h1.at[:, pl.ds(cut, dm.model - cut)])]
        loads = [dma(a, b, isem.at[n]) for n, (a, b) in enumerate(pairs)]
        begin(loads)
        for i in range(nb - 1):
            start(jnp.int32(i))
        meet([to_core, to_x, to_y])

        def bulk(i):
            r = at(i * crow, crow, SUB)
            return remote(kv.at[:, r], kvx.at[:, r], xss.at[i], xrs.at[i], to_x)

        def forward(i):
            r = at(i * crow, crow, SUB)
            return remote(kvx.at[:, r], kvq.at[:, r], fss.at[i], frs.at[i], to_core)

        near = remote(kv, kvp, dss.at[0], drs.at[0], to_core)
        each(n_dn, lambda i: bulk(i).start())
        finish_all(loads)
        for i in range(dm.heads):
            for n, t in enumerate((tp, 1 - tp)):
                xn[:m, at((2 * i + t) * dm.hd, dm.hd)] = tmp[n, :, i * dm.hd:(i + 1) * dm.hd]
        ss[...] = jnp.zeros_like(ss)

        def hsend(j):
            return remote(h1.at[:, cols(j)], h1p.at[:, cols(j)], hss.at[j], hrs.at[j], to_core)

        ss_send = remote(ss, ssp, dss.at[1], drs.at[1], to_core)

        def add_to_hidden(cs, acc):
            out = (h1[:, cs].astype(F32) + acc.astype(BF).astype(F32)).astype(BF)
            h1[:, cs] = out
            return out.astype(F32)

        def out_step(i):
            pl.when(i > 0)(lambda: hsend(i - 1).start())
            start(i + nb - 1)
            wait(i)
            slot = lax.rem(i, nb)
            for n in HALVES:
                acc = jnp.dot(xn[:m, :], wb[slot, :, n:n + WIDE], preferred_element_type=F32)
                out = add_to_hidden(at(i * CHUNK + n, WIDE), acc)
                ss[...] += out[:, :LANES] * out[:, :LANES] + out[:, LANES:] * out[:, LANES:]
        each(n_out, out_step)

        def apply_norm(src, stat, base):
            total_sq = jnp.sum(stat[...], axis=1, keepdims=True)
            stat[...] = jnp.broadcast_to(lax.rsqrt(total_sq / dm.model + NORM_EPS), stat.shape)

            def step(i):
                sl = at(i * SUB, SUB, SUB)
                for c in range(*dm.lanes):
                    xn[at(base + i * SUB, SUB, SUB), c:c + LANES] = (src[sl, c:c + LANES].astype(F32) * stat[sl, :]).astype(BF)
            each(m // SUB, step)

        ss_send.start()
        hsend(n_out - 1).start()
        ss_send.wait_send()
        apply_norm(h1, ss, 0)
        ss_send.wait_recv()
        each(n_out, lambda j: hsend(j).wait_recv())
        near.start()
        apply_norm(h1p, ssp, m)

        def dots(i, acc):
            start(i + nb - 1)
            wait(i)
            acc[...] = jnp.dot(xn[...], wb[lax.rem(i, nb)], preferred_element_type=F32)

        def glu(acc, j, w):
            gate = acc[:, :w].astype(BF).astype(F32)
            upper = acc[:, w:2 * w].astype(BF).astype(F32)
            act[:, at(j * WIDE, w)] = (jax.nn.silu(gate) * upper).astype(BF)

        dots(jnp.int32(gu0), acc_a)

        def gu_pair(q):
            dots(gu0 + 2 * q + 1, acc_b)
            glu(acc_a, 2 * q, WIDE)
            dots(gu0 + 2 * q + 2, acc_a)
            glu(acc_b, 2 * q + 1, WIDE)
        each(n_full // 2, gu_pair)
        start(jnp.int32(dn0 - 1 + nb - 1))
        wait(jnp.int32(dn0 - 1))
        acc_b[:, :2 * rem] = jnp.dot(xn[...], wb[(dn0 - 1) % nb, :, :2 * rem], preferred_element_type=F32)
        glu(acc_a, n_full - 1, WIDE)
        glu(acc_b, n_full, rem)

        def share(j):
            return remote(h1.at[:, cols(j)], ob.at[:, cols(j)], yss.at[j], yrs.at[j], to_y)

        def keeps(j, fn):
            @pl.when(j < EARLY_SENT)
            def _():
                fn(dma(h1.at[:, cols(j)], oa.at[:, cols(j)], osem.at[j]))

            @pl.when(j >= EARLY_SENT)
            def _():
                fn(dma(h1.at[:, cols(j)], ot.at[:, cols(j - EARLY_SENT)], osem.at[j]))

        def deliver(j):
            keeps(j, lambda c: c.start())
            pl.when(j < EARLY_SENT)(lambda: share(j).start())

        def psend_copy(j):
            return remote(psend.at[lax.rem(j, 2)], precv.at[j], pss.at[j], prs.at[j], to_core)

        def finish(j):
            for n in HALVES:
                out = add_to_hidden(at(j * CHUNK + n, WIDE), pown[lax.rem(j, 2), :, n:n + WIDE] + precv[j, :, n:n + WIDE])
                ss[...] += out[:, :LANES] * out[:, :LANES] + out[:, LANES:] * out[:, LANES:]

        def part(rows, slots, n):
            return sum(jnp.dot(act[rows, i * kc:i * kc + ksz[i]], wb[slots[i], :ksz[i], n:n + WIDE], preferred_element_type=F32) for i in range(nk))

        def down(j, first):
            i0 = dn0 + j * nk
            if not first:
                start(i0 + nb - 2)
            start(i0 + nb - 1)
            slots = []
            for n in range(nk):
                wait(i0 + n)
                slots.append(lax.rem(i0 + n, nb))
            half = lax.rem(j, 2)
            pl.when(j > 1)(lambda: psend_copy(j - 2).wait_send())
            for n in HALVES:
                psend[half, :, n:n + WIDE] = part(slice(m, 2 * m), slots, n)
            if not first:
                psend_copy(j - 1).wait_recv()
            psend_copy(j).start()
            if not first:
                finish(j - 1)
            for n in HALVES:
                pown[half, :, n:n + WIDE] = part(slice(0, m), slots, n)
            if not first:
                deliver(j - 1)
            bulk(j).wait_recv()
            forward(j).start()

        each(n_out, lambda j: hsend(j).wait_send())
        ss[...] = jnp.zeros_like(ss)
        down(jnp.int32(0), True)
        each(n_dn - 1, lambda j: down(j + 1, False))
        psend_copy(n_dn - 1).wait_recv()
        finish(n_dn - 1)
        for j in (n_dn - 2, n_dn - 1):
            psend_copy(j).wait_send()
        near.wait()
        deliver(n_dn - 1)
        ss_keep = dma(ss, os, isem.at[0])
        ss_keep.start()
        ss_keep.wait()

        def last(j):
            bulk(j).wait_send()
            forward(j).wait()
            keeps(j, lambda c: c.wait())
            pl.when(j < EARLY_SENT)(lambda: share(j).wait())
        each(n_dn, last)

    part1, part2 = sds((m, cut), BF), sds((m, dm.model - cut), BF)
    two = sds(kv3.shape, BF)
    acc = pltpu.VMEM((2 * m, CHUNK), F32)
    pair = pltpu.VMEM((2, m, CHUNK), F32)
    vec = sem((n_dn,))
    stat = pltpu.VMEM((m, LANES), F32)
    return pl.pallas_call(
        kern, out_shape=(part1, part2, part1, sds((m, LANES), F32), two, two, two),
        in_specs=[ANY] * (nr + 9), out_specs=(ANY,) * 7,
        scratch_shapes=[
            pltpu.VMEM((m, dm.model), BF), pltpu.VMEM((m, dm.model), BF), pltpu.VMEM((2 * m, dm.model), BF),
            pltpu.VMEM((2 * m, ffh), BF), pltpu.VMEM((2, m, dm.loc), BF), pltpu.VMEM((nb, kc, CHUNK), BF),
            acc, acc, pair, pltpu.VMEM((n_dn, m, CHUNK), F32), pair, stat, stat,
            sem((nb, 2)), sem((6,)), vec, vec, vec, vec, vec, vec, vec, vec, vec, vec, vec, sem((2,)), sem((2,))],
        compiler_params=params(collective_id=2 + layer, has_side_effects=True),
        cost_estimate=cost(2 * m * dm.model * (dm.model + 3 * dm.ff), dm.model * (2 * dm.model + 3 * dm.ff)),
        name="post")(*resid, co, do, ci, di, kv3, w_out, w_gate, w_up, w_down)


def tail_call(dm, meta, lengths, kv3, news, kc, vc):
    layers, batch, cache = kc.shape[1:4]
    bits = [1 << b for b in reversed(range(dm.rows.bit_length()))]
    nsrc = len(kv3[0])
    per_layer = batch // PER
    steps = layers * per_layer
    ring = 6
    lag = 2

    def kern(meta_ref, len_ref, *refs):
        srcs, refs = refs[:layers * nsrc], refs[layers * nsrc:]
        dec, refs = refs[:layers], refs[layers:]
        kc_ref, vc_ref, ko, vo, kn, vn, buf, slots, dv, lsem, osem, dsem, isem, wsem = refs
        side = lax.axis_index('side')
        start, length = meta_ref[0], meta_ref[1]

        def pieces(fn):
            for k in range(nsrc):
                first = dm.rows * (side ^ k)
                lo = jnp.maximum(start, first)
                cnt = jnp.maximum(jnp.minimum(start + length, first + dm.rows) - lo, 0)
                for n, bit in enumerate(bits):
                    @pl.when((cnt & bit) != 0)
                    def _(k=k, n=n, bit=bit, first=first, lo=lo, cnt=cnt):
                        off = cnt // (2 * bit) * (2 * bit)
                        for l in range(layers):
                            fn(dma(srcs[l * nsrc + k].at[:, pl.ds(lo - first + off, bit)], buf.at[l, :, pl.ds(lo - start + off, bit)], lsem.at[l, k, n]))

        def spot(i):
            return i // per_layer, at(PER * lax.rem(i, per_layer), PER, PER), lax.rem(i, ring)

        def read(i):
            lay, b, slot = spot(i)
            return [dma(ref.at[0, lay, b], slots.at[slot, n], isem.at[slot, n]) for n, ref in enumerate((kc_ref, vc_ref))]

        def write(i):
            lay, b, slot = spot(i)
            return [dma(slots.at[slot, n], ref.at[0, lay, b], wsem.at[slot, n]) for n, ref in enumerate((kn, vn))]

        dloads = [dma(ref, dv.at[n], dsem.at[n]) for n, ref in enumerate(dec)]
        begin(dloads)
        pieces(lambda c: c.start())
        for i in range(ring - lag):
            begin(read(jnp.int32(i)))

        def zero(r, c):
            buf[:, :, r] = jnp.zeros((layers, 2, dm.heads, dm.hd), BF)
            return c
        lax.fori_loop(length, dm.max_req, zero, 0)
        finish_all(dloads)
        pieces(lambda c: c.wait())
        outs = [dma(buf.at[l, n], ref.at[0, l], osem.at[l, n]) for l in range(layers) for n, ref in enumerate((ko, vo))]
        begin(outs)

        def step(i):
            lay, _, slot = spot(i)
            finish_all(read(i))
            for n in range(PER):
                b = PER * lax.rem(i, per_layer) + n
                for kind in range(2):
                    slots[slot, kind, n, len_ref[b]] = dv[lay, kind, b]
            pl.when(i > 0)(lambda: begin(write(i - 1)))

            @pl.when(i + ring - lag < steps)
            def _():
                pl.when(i >= lag)(lambda: finish_all(write(i - lag)))
                begin(read(i + ring - lag))
        each(steps, step)
        begin(write(jnp.int32(steps - 1)))
        each(ring, lambda i: finish_all(write(steps - ring + i)))
        finish_all(outs)

    shape = sds((1, layers, dm.max_req, dm.heads, dm.hd), BF)
    three = (dm.heads, dm.hd)
    flat = [ref for group in kv3 for ref in group]
    pair = sem((layers, 2))
    return pl.pallas_call(
        kern, out_shape=(shape, shape, sds(kc.shape, BF), sds(vc.shape, BF)),
        in_specs=[SMEM, SMEM] + [ANY] * (len(flat) + layers + 2), out_specs=(ANY,) * 4,
        scratch_shapes=[pltpu.VMEM((layers, 2, dm.max_req) + three, BF), pltpu.VMEM((ring, 2, PER, cache) + three, BF), pltpu.VMEM((layers,) + news[0].shape, BF),
                        sem((layers, nsrc, len(bits))), pair, sem((layers,)), sem((ring, 2)), sem((ring, 2))],
        compiler_params=params(),
        cost_estimate=cost(10**11, kc.size),
        name="tail")(meta, lengths, *flat, *news, kc, vc)


def close_call(dm, mine, theirs):
    cut = mine[0].shape[1]
    h, d, k = dm.half, dm.dhalf, dm.blk

    def kern(a1, a2, b1, b2, hid, dec, buf, lsem, osem):
        tp = lax.axis_index('tp')
        loads = []
        for n, (ref, blk, col) in enumerate(((a1, tp, 0), (a2, tp, cut), (b1, 1 - tp, 0), (b2, 1 - tp, cut))):
            loads.append(dma(ref, buf.at[at(blk * k, k, SUB), pl.ds(col, ref.shape[1])], lsem.at[n]))
        begin(loads)
        finish_all(loads)
        outs = []
        for n in range(2):
            outs.append(dma(buf.at[pl.ds(n * k, h)], hid.at[pl.ds(n * h, h)], osem.at[2 * n]))
            outs.append(dma(buf.at[pl.ds(n * k + h, d)], dec.at[pl.ds(n * d, d)], osem.at[2 * n + 1]))
        begin(outs)
        finish_all(outs)

    return pl.pallas_call(
        kern, out_shape=(sds((dm.rows, dm.model), BF), sds((dm.dec, dm.model), BF)),
        in_specs=[ANY] * 4, out_specs=(ANY, ANY),
        scratch_shapes=[pltpu.VMEM((dm.all, dm.model), BF), sem((4,)), sem((4,))],
        compiler_params=params(), name="close")(*mine, *theirs)


def solution(mesh):
    tp_size = mesh.shape['tp']
    side_size = mesh.shape['side']
    rows_spec = P(('pair', 'side'), None)
    batch_spec = P(('pair', 'side'), None, None)
    cache_spec = P(('pair', 'side'), None, None, None, 'tp', None)
    prompt_spec = P(('pair', 'side'), None, None, 'tp', None)

    def swap(val, axis, bit):
        size = tp_size if axis == 'tp' else side_size
        return lax.ppermute(val, axis, [(i, i ^ bit) for i in range(size)])

    def local_step(x_loc, req_len, dest, w_qkv, w_out, w_gate, w_up, w_down, y_loc, kc, vc, clen_loc):
        side = lax.axis_index('side')
        tp = lax.axis_index('tp')
        layers = w_qkv.shape[0]
        rows = x_loc.shape[0]
        y = y_loc[0]
        lengths = clen_loc[0]
        dm = Dims(rows, y.shape[0], x_loc.shape[1], kc.shape[-2], kc.shape[-1], w_gate.shape[2], 2 * rows - rows // 4)
        h, d = dm.half, dm.dhalf

        ends = jnp.sum(jnp.where(jnp.arange(side_size)[:, None] >= jnp.arange(side_size)[None, :], req_len[None, :], 0), axis=1)
        row_ids = rows * side + jnp.arange(rows)
        seg_start = jnp.max(jnp.where(row_ids[:, None] >= ends[None, :], ends[None, :], 0), axis=1)
        pos = row_ids - seg_start
        positions = jnp.concatenate([pos[:h], lengths[:d], pos[h:], lengths[d:]]).astype(F32)
        half_dim = dm.hd // 2
        inv_freq = ROPE_BASE ** (-jnp.arange(half_dim, dtype=F32) / half_dim)
        angles = positions[:, None] * inv_freq[None, :]
        cos_val, sin_val = jnp.cos(angles), jnp.sin(angles)
        tab_c = jnp.concatenate([cos_val, cos_val], axis=1)
        tab_s = jnp.concatenate([-sin_val, sin_val], axis=1)

        mine = dest == side
        inst_meta = jnp.stack([jnp.sum(jnp.where(mine, ends - req_len, 0)), jnp.sum(jnp.where(mine, req_len, 0))])
        mid = rows * side_size // 2
        fast = mid - jnp.max(jnp.where(ends <= mid, ends, 0)) <= LANES

        span = SUB * dm.heads
        src = jnp.arange(span)
        perm = ((src % dm.heads * SUB + src // dm.heads)[:, None] == src[None, :]).astype(BF)

        ins = resid = (x_loc, y)
        fresh, kv_all = [], []
        for layer in range(layers):
            first = layer == 0
            kvh, kv3, qh, dec, co, ci, do, di = front_call(dm, layer, first, ins, w_qkv, tab_c, tab_s, perm, lengths, ends, kc, vc)
            fresh.append(dec)

            def general(i, ctx):
                kv, q, edges, _ = lax.optimization_barrier((kvh, qh, ends, i))
                kvx = swap(kv, 'side', 2)
                kvs = (kv, swap(kv, 'side', 1), kvx, swap(kvx, 'side', 1))
                own, other = (general_attention(dm, jnp.concatenate([b[None], edges]), q, kvs) for b in (tp, 1 - tp))
                return own, swap(other, 'tp', 1)
            co, ci = lax.fori_loop(0, jnp.where(fast, 0, 1), general, (co, ci))
            o1, o2, p1, stat, kv3_x, kv3_p, kv3_q = post_call(dm, layer, first, resid, co, do, ci, di, kv3, w_out, w_gate, w_up, w_down)
            if layer == layers - 1:
                p2 = swap(o2, 'tp', 1)
            kv_all.append((kv3, kv3_p, kv3_x, kv3_q))
            ins, resid = (o1, o2, p1, stat), (o1, o2)
        k_prompt, v_prompt, k_new, v_new = tail_call(dm, inst_meta, lengths, kv_all, fresh, kc, vc)
        hidden, dec_out = close_call(dm, (o1, o2), (p1, p2))
        return hidden, dec_out[None], k_prompt, v_prompt, k_new, v_new

    return jax.shard_map(local_step, mesh=mesh,
                         in_specs=(rows_spec, P('pair'), P('pair'), P(), P(), P(), P(), P(), batch_spec, cache_spec, cache_spec, rows_spec),
                         out_specs=(rows_spec, batch_spec, prompt_spec, prompt_spec, cache_spec, cache_spec),
                         check_vma=False)
```

```python
import jax
import jax.numpy as jnp
from jax import lax
from jax.experimental import pallas as pl
from jax.experimental.pallas import tpu as pltpu
from jax.sharding import PartitionSpec as P

ROPE_BASE = 10000.0
NORM_EPS = 1e-5
NEG = -1e30
BF = jnp.bfloat16
F32 = jnp.float32
ANY = pl.BlockSpec(memory_space=pl.ANY)
SMEM = pl.BlockSpec(memory_space=pltpu.SMEM)
WHOLE = pl.BlockSpec(memory_space=pltpu.VMEM)
VMEM_LIMIT = 61 * 2**20
LOG2E = 1.4426950408889634
LANES = 128
WIDE = 256
CHUNK = 512
HALVES = (0, WIDE)
SUB = 16
PER = 4
EARLY_SENT = (4, 3)
NT = (((1,), (1,)), ((), ()))
dma = pltpu.make_async_copy
sds = jax.ShapeDtypeStruct
sem = pltpu.SemaphoreType.DMA


def at(start, size, multiple=LANES):
    return pl.ds(pl.multiple_of(start, multiple), size)


def cost(flops, size):
    return pl.CostEstimate(flops=flops, bytes_accessed=size, transcendentals=0)


def params(**kw):
    return pltpu.CompilerParams(vmem_limit_bytes=VMEM_LIMIT, **kw)


def remote(src, dst, send, recv, dev):
    return pltpu.make_async_remote_copy(src_ref=src, dst_ref=dst, send_sem=send, recv_sem=recv, device_id=dev, device_id_type=pl.DeviceIdType.MESH)


def meet(devices):
    barrier = pltpu.get_barrier_semaphore()
    for dev in devices:
        pl.semaphore_signal(barrier, device_id=dev, device_id_type=pl.DeviceIdType.MESH)
    pl.semaphore_wait(barrier, len(devices))


def each(count, fn):
    lax.fori_loop(0, count, lambda i, c: (fn(i), c)[1], 0)


def begin(copies):
    for cp in copies:
        cp.start()


def finish_all(copies):
    for cp in copies:
        cp.wait()


def row_sum(x):
    return jnp.sum(x, axis=1, keepdims=True)


def row_max(x):
    return jnp.max(x, axis=1, keepdims=True)


def norm_rows(ref, base, rows):
    group = 2 if rows % (2 * SUB) == 0 else 1

    def step(i):
        for n in range(group):
            sl = at(base + (group * i + n) * SUB, SUB, SUB)
            wide = ref[sl, :].astype(F32)
            scale = lax.rsqrt(jnp.mean(wide * wide, axis=-1, keepdims=True) + NORM_EPS)
            ref[sl, :] = (wide * scale).astype(BF)
    each(rows // SUB // group, step)


def request_ends(len_ref):
    ends = [len_ref[0]]
    for r in range(1, 4):
        ends.append(ends[-1] + len_ref[r])
    return ends


def segment_start(row, ends):
    start = jnp.zeros_like(row)
    for end in ends:
        start = jnp.where(row >= end, end, start)
    return start


class Dims:
    def __init__(self, rows, dec, model, heads, head_dim, ff, max_req):
        self.rows, self.half = rows, rows // 2
        self.dec, self.dhalf = dec, dec // 2
        self.blk = self.half + self.dhalf
        self.all = 2 * self.blk
        self.model, self.heads, self.hd, self.ff = model, heads, head_dim, ff
        self.max_req = max_req
        self.loc = heads * head_dim
        self.window = LANES + 2 * rows
        self.lanes = (0, model, LANES)


def front_call(dm, layer, first, ins, w_qkv, freq, lengths, req_len, kc, vc):
    nb = 4
    per_sec = dm.heads // PER
    steps = 3 * per_sec
    kv_steps = 2 * per_sec
    h, d, k = dm.half, dm.dhalf, dm.blk
    m = dm.all if first else k
    npass = dm.all // m
    width = PER * dm.hd
    lead = dm.window - dm.rows
    batch, cache = kc.shape[2], kc.shape[3]
    flat = cache * dm.heads
    ring = 4
    dsteps = batch // PER
    ni = len(ins)

    def kern(*refs):
        rin = refs[:ni]
        (w_ref, f_ref, len_ref, req_ref, k_ref, v_ref, kvh, kv3, qh, dec, co, ci, do, di, tab_out,
         tab, perm_ref, xn, wb, kcat, qv, sd, dv, acc_a, acc_b, bias, sbuf, pbuf, cbuf, cr, dsc, dbuf, dout, o3, stat,
         wsem, isem, csem, tsem, pss, prs, ess, ers, yss, yrs, lss, lrs) = refs[ni:]
        tp = lax.axis_index('tp')
        side = lax.axis_index('side')
        odd = lax.rem(side, 2)
        to_y = {'tp': 1 - tp}

        def wcopies(i):
            slot = lax.rem(i, nb)
            j = lax.rem(i, steps)
            sec = j // per_sec
            base = jnp.where(sec == 2, 0, (sec + 1) * 2 * dm.loc)
            out = []
            for n in range(PER):
                col = base + (2 * (PER * lax.rem(j, per_sec) + n) + tp) * dm.hd
                out.append(dma(w_ref.at[layer, :, at(col, dm.hd)], wb.at[slot, :, pl.ds(n * dm.hd, dm.hd)], wsem.at[slot, n]))
            return out

        def group_of(i):
            return lax.rem(i + tp * (dsteps // 2), dsteps)

        def caches(i):
            slot = lax.rem(i, ring)
            b = at(PER * group_of(i), PER, PER)
            return [dma(ref.at[0, layer, b], cr.at[slot, n], csem.at[slot, n]) for n, ref in enumerate((k_ref, v_ref))]

        if first:
            parts = [(rin[0], 0, 0, h), (rin[1], 0, h, d), (rin[0], h, k, h), (rin[1], d, k + h, d)]
            loads = [dma(ref.at[pl.ds(src, n)], xn.at[pl.ds(dst, n)], isem.at[i]) for i, (ref, src, dst, n) in enumerate(parts)]
        else:
            own1, own2, peer1, ss_in, tab_in = rin
            cut = own1.shape[1]
            head_cols, tail_cols = pl.ds(0, cut), pl.ds(cut, dm.model - cut)
            top, low_rows = pl.ds(0, k), pl.ds(k, k)
            loads = [dma(own1, xn.at[top, head_cols], isem.at[0]), dma(own2, xn.at[top, tail_cols], isem.at[1]),
                     dma(ss_in, stat.at[0], isem.at[2]), dma(peer1, xn.at[low_rows, head_cols], isem.at[3]), dma(tab_in, tab, tsem.at[1])]
        begin(loads)
        for i in range(nb - 1):
            begin(wcopies(jnp.int32(i)))
        for i in range(2):
            begin(caches(jnp.int32(i)))

        def zero(i):
            kcat[:, i, pl.ds(0, lead), :] = jnp.zeros((2, lead, dm.hd), BF)
        each(dm.heads, zero)
        src = lax.broadcasted_iota(jnp.int32, perm_ref.shape, 0)
        dst = lax.broadcasted_iota(jnp.int32, perm_ref.shape, 1)
        perm_ref[...] = (lax.rem(src, dm.heads) * SUB + src // dm.heads == dst).astype(F32).astype(BF)
        ends = request_ends(req_ref)

        def table(row, pos):
            size = pos.shape[0]
            ang = pos.astype(F32) * f_ref[...]
            sign = jnp.where(lax.broadcasted_iota(jnp.int32, pos.shape, 1) < dm.hd // 2, -1.0, 1.0)
            tab[0, at(row, size, SUB), :] = jnp.cos(ang)
            tab[1, at(row, size, SUB), :] = jnp.sin(ang) * sign

        if first:
            for b in range(2):
                def rows_table(i):
                    row = dm.rows * side + b * h + i * PER * SUB + lax.broadcasted_iota(jnp.int32, (PER * SUB, LANES), 0)
                    table(b * k + i * PER * SUB, row - segment_start(row, ends))
                each(h // SUB // PER, rows_table)
                which = lax.broadcasted_iota(jnp.int32, (d, LANES), 0)
                pos = jnp.zeros_like(which)
                for i in range(d):
                    pos = jnp.where(which == i, len_ref[b * d + i], pos)
                table(b * k + h, pos)
        meet([{'side': lax.rem(side + i, 4)} for i in range(1, 4)] + [to_y])
        late = []
        if not first:
            late = [remote(own2, xn.at[low_rows, tail_cols], lss.at[0], lrs.at[0], to_y),
                    remote(ss_in, stat.at[1], lss.at[1], lrs.at[1], to_y)]
            begin(late[::-1])

        def own_part(j):
            return kcat.at[j // per_sec, at(PER * lax.rem(j, per_sec), PER, PER), pl.ds(lead, dm.rows)]

        def edge_part(j, row):
            return kcat.at[j // per_sec, at(PER * lax.rem(j, per_sec), PER, PER), pl.ds(row, LANES)]

        def peer_copy(j):
            dst = kcat.at[j // per_sec, at(PER * lax.rem(j, per_sec), PER, PER), pl.ds(LANES, dm.rows)]
            return remote(own_part(j), dst, pss.at[j], prs.at[j], {'side': side + 1})

        def edge_copy(j, to):
            row = dm.window - LANES if to == 2 else dm.rows
            return remote(edge_part(j, row), edge_part(j, (3 - to) * dm.rows), ess.at[j], ers.at[j], {'side': to})

        def send(j):
            pl.when(odd == 0)(lambda: peer_copy(j).start())
            pl.when(side == 1)(lambda: edge_copy(j, 2).start())

        def arrived(j):
            pl.when(odd == 1)(lambda: peer_copy(j).wait_recv())

            @pl.when(side == 2)
            def _():
                edge_copy(j, 2).wait_recv()
                edge_copy(j, 3).start()
            pl.when(side == 3)(lambda: edge_copy(j, 3).wait_recv())

        def sent(j):
            pl.when(odd == 0)(lambda: peer_copy(j).wait_send())
            pl.when(side == 1)(lambda: edge_copy(j, 2).wait_send())
            pl.when(side == 2)(lambda: edge_copy(j, 3).wait_send())

        def ahead(i):
            @pl.when(i + nb - 1 < npass * steps)
            def _():
                begin(wcopies(i + nb - 1))

        def fetch(i, more):
            if more:
                ahead(i)
            finish_all(wcopies(i))

        def multiply(i, rows, acc):
            acc[...] = jnp.dot(xn[rows, :], wb[lax.rem(i, nb)], preferred_element_type=F32)

        def dots(i, rows, acc):
            fetch(i, True)
            multiply(i, rows, acc)

        def epilogue(j, acc, blocks, is_q):
            sec, jj = j // per_sec, lax.rem(j, per_sec)
            for r0, b in blocks:
                rows = slice(r0, r0 + k)
                cv, sv = tab[0, at(b * k, k, SUB), :], tab[1, at(b * k, k, SUB), :]
                for n in range(PER):
                    head = PER * jj + n
                    val = acc[rows, n * dm.hd:(n + 1) * dm.hd].astype(BF).astype(F32)
                    rot = val * cv + pltpu.roll(val, dm.hd // 2, 1) * sv
                    low = (rot if is_q else jnp.where(sec == 1, val, rot)).astype(BF)
                    if is_q:
                        qv[head, at(b * h, h, SUB), :] = low[:h]
                    else:
                        kcat[sec, head, at(lead + b * h, h, SUB), :] = low[:h]
                    sd[sec, head, at(b * d, d, d), :] = low[h:]

        def run(p, blocks):
            rows = pl.ds(p * m, m)
            base = p * steps
            final = p == npass - 1
            last = kv_steps

            def done(j):
                if final:
                    pl.when(j > 0)(lambda: send(j - 1))

            dots(jnp.int32(base), rows, acc_a)

            def pair(q):
                i = base + 2 * q + 1
                fetch(i, True)
                fetch(i + 1, False)
                multiply(i, rows, acc_b)
                epilogue(2 * q, acc_a, blocks, False)
                multiply(i + 1, rows, acc_a)
                epilogue(2 * q + 1, acc_b, blocks, False)
                ahead(i + 1)
                done(2 * q)
                done(2 * q + 1)
            each(last // 2 - 1, pair)
            dots(jnp.int32(base + last - 1), rows, acc_b)
            epilogue(jnp.int32(last - 2), acc_a, blocks, False)
            done(jnp.int32(last - 2))
            if final:
                epilogue(jnp.int32(last - 1), acc_b, blocks, False)
                done(jnp.int32(last - 1))
                return
            dots(jnp.int32(base + last), rows, acc_a)
            epilogue(jnp.int32(last - 1), acc_b, blocks, False)
            for n in range(1, per_sec):
                prev, acc = (acc_a, acc_b) if n % 2 else (acc_b, acc_a)
                dots(jnp.int32(base + last + n), rows, acc)
                epilogue(jnp.int32(last + n - 1), prev, blocks, True)
            epilogue(jnp.int32(steps - 1), acc, blocks, True)

        def apply_norm(n, base):
            total_sq = row_sum(stat[n])
            stat[n] = jnp.broadcast_to(lax.rsqrt(total_sq / dm.model + NORM_EPS), (k, LANES))

            def step(i):
                sl = at(base + i * SUB, SUB, SUB)
                for c in range(*dm.lanes):
                    xn[sl, c:c + LANES] = (xn[sl, c:c + LANES].astype(F32) * stat[n, at(i * SUB, SUB, SUB), :]).astype(BF)
            each(k // SUB, step)

        def cols(g):
            return at(width * g, width)

        def ctx_send(g):
            return remote(cbuf.at[0, :, cols(g)], ci.at[:, cols(g)], yss.at[g], yrs.at[g], to_y)

        dec_send = remote(dout.at[at((1 - tp) * d, d, SUB)], di, yss.at[per_sec], yrs.at[per_sec], to_y)
        dec_keep = dma(dout.at[at(tp * d, d, SUB)], do, isem.at[0])

        def score(b, w, head, n):
            sbuf[n % 2, :, :w] = lax.dot_general(qv[head, b * h:(b + 1) * h, :], kcat[0, head, :w, :], NT, preferred_element_type=F32)

        def value(ph, w, head, n):
            s = sbuf[n % 2, :, :w] * (dm.hd ** -0.5 * LOG2E) + bias[:, :w]
            p = jnp.exp2(s - row_max(s))
            pbuf[n % 2, :, :w] = p.astype(BF)
            tot = row_sum(p)
            o = jnp.dot(pbuf[n % 2, :, :w], kcat[1, head, :w, :], preferred_element_type=F32)
            cbuf[ph, :, at(head * dm.hd, dm.hd)] = (o / tot).astype(BF)

        def turn_rows(rows, out):
            x = jnp.concatenate([r.reshape(SUB * dm.heads, dm.hd) for r in rows], axis=1)
            y = jnp.dot(perm_ref[...], x, preferred_element_type=F32).astype(BF)
            for n, dst in enumerate(out):
                dst(y[:, n * dm.hd:(n + 1) * dm.hd].reshape(SUB, dm.heads, dm.hd))

        def decode_half(part):
            col = lax.broadcasted_iota(jnp.int32, (dm.heads, flat), 1)
            row = lax.broadcasted_iota(jnp.int32, (dm.heads, flat), 0)
            pos = jnp.where(lax.rem(col, dm.heads) == row, col // dm.heads, flat)
            scale = dm.hd ** -0.5
            count = dsteps // 2

            def look(n):
                i = part * count + n

                @pl.when(i + 2 < dsteps)
                def _():
                    begin(caches(i + 2))
                finish_all(caches(i))
                for r in range(PER):
                    keys = cr[lax.rem(i, ring), 0, r].reshape(flat, dm.hd)
                    dsc[n % 2, r] = lax.dot_general(dv[2, PER * group_of(i) + r], keys, NT, preferred_element_type=F32)

            def gather(n):
                i = part * count + n
                for r in range(PER):
                    bi = PER * group_of(i) + r
                    q, kn, vn = (dv[c, bi].astype(F32) for c in (2, 0, 1))
                    s = jnp.where(pos < len_ref[bi], dsc[n % 2, r] * scale, NEG)
                    fresh = row_sum(q * kn) * scale
                    top = jnp.maximum(row_max(s), fresh)
                    p = jnp.exp(s - top)
                    pf = jnp.exp(fresh - top)
                    inv = 1.0 / (row_sum(p) + pf)
                    vals = cr[lax.rem(i, ring), 1, r].reshape(flat, dm.hd)
                    o = jnp.dot((p * inv).astype(BF), vals, preferred_element_type=F32)
                    dbuf[bi] = o + (pf * inv).astype(BF).astype(F32) * vn

            look(0)
            for n in range(count):
                if n + 1 < count:
                    look(n + 1)
                gather(n)

        def put(ref, *idx):
            def store(val):
                ref[idx] = val
            return store

        def turn_block(b):
            sl = at(b * d, d, SUB)
            turn_rows([sd[n, :, sl, :] for n in range(3)], [put(dv, n, sl) for n in range(3)])

            def block(i):
                for n in range(PER):
                    row = b * h + (PER * i + n) * SUB
                    sl, own = at(row, SUB, SUB), at(lead + row, SUB, SUB)
                    turn_rows([kcat[n2, :, own, :] for n2 in range(2)], [put(o3, n2, sl) for n2 in range(2)])
            each(h // SUB // PER, block)

        if first:
            tab_copy = dma(tab, tab_out, tsem.at[1])
            tab_copy.start()
            for cp, (_, _, row, size) in zip(loads, parts):
                cp.wait()
                norm_rows(xn, row, size)
            blocks = [(0, 0), (k, 1)]
        else:
            finish_all(loads[:3] + loads[4:])
            apply_norm(0, 0)
            run(0, [(0, tp)])
            turn_block(tp)
            decode_half(0)
            loads[3].wait()
            finish_all(late)
            apply_norm(1, k)
            blocks = [(0, 1 - tp)]
        run(npass - 1, blocks)

        kv3_copy = dma(o3, kv3, tsem.at[0])
        kvh_copy = dma(kcat.at[:, :, pl.ds(lead, dm.rows)], kvh, isem.at[2])
        q_copy = dma(qv, qh, tsem.at[2])
        dec_copy = dma(dv, dec, tsem.at[3])

        def stage(t):
            ph, g = t // per_sec, lax.rem(t, per_sec)
            b = lax.rem(1 + tp + ph, 2)

            @pl.when(ph == 0)
            def _():
                dots(npass * steps - per_sec + g, pl.ds((npass - 1) * m, m), acc_a)
                epilogue(kv_steps + g, acc_a, blocks, True)
                pl.when(g == 0)(lambda: send(kv_steps - 1))
                arrived(g)
                arrived(per_sec + g)

            @pl.when(t == per_sec)
            def _():
                ctx_send(per_sec - 1).start()
                if first:
                    each(2, turn_block)
                    each(2, decode_half)
                else:
                    turn_block(1 - tp)
                    decode_half(1)
                for n in range(dm.heads):
                    dout[:, n * dm.hd:(n + 1) * dm.hd] = dbuf[:, n, :].astype(BF)
                begin([kv3_copy, kvh_copy, q_copy, dec_copy])

            @pl.when(g == 0)
            def _():
                rows = dm.rows * side + h * b + lax.broadcasted_iota(jnp.int32, (h, LANES), 0)
                start = segment_start(rows, ends)
                lane = dm.rows * side - lead + lax.broadcasted_iota(jnp.int32, (h, LANES), 1)
                for c in range(dm.window // LANES):
                    col = lane + c * LANES
                    bias[:, c * LANES:(c + 1) * LANES] = jnp.where((col >= start) & (col <= rows), 0.0, NEG)
            pl.when(t == per_sec)(lambda: begin([dec_send, dec_keep]))

            for bb, w in enumerate((dm.window - h, dm.window)):
                @pl.when(b == bb)
                def _(bb=bb, w=w):
                    score(bb, w, PER * g, 0)
                    for n in range(PER):
                        if n + 1 < PER:
                            score(bb, w, PER * g + n + 1, n + 1)
                        value(ph, w, PER * g + n, n)
            pl.when((ph == 0) & (g > 0))(lambda: ctx_send(g - 1).start())
        each(2 * per_sec, stage)

        if first:
            tab_copy.wait()
        keep = dma(cbuf.at[1], co, isem.at[1])
        keep.start()
        each(kv_steps, sent)
        finish_all([kv3_copy, kvh_copy, q_copy, dec_copy, dec_keep, dec_send])
        each(per_sec, lambda g: ctx_send(g).wait())
        keep.wait()

    heads = (dm.heads, dm.rows, dm.hd)
    three = (dm.heads, dm.hd)
    flops = 2 * dm.all * dm.model * width * steps
    outs = [(2,) + heads, (2, dm.rows) + three, heads, (3, dm.dec) + three, (h, dm.loc), (h, dm.loc), (d, dm.loc), (d, dm.loc)]
    acc = pltpu.VMEM((m, width), F32)
    tabs = sds((2, dm.all, LANES), F32)
    vec = sem((kv_steps,))
    return pl.pallas_call(
        kern, out_shape=tuple(sds(s, BF) for s in outs) + (tabs,),
        in_specs=[ANY] * (ni + 1) + [WHOLE] + [SMEM] * 2 + [ANY] * 2, out_specs=(ANY,) * (len(outs) + 1),
        scratch_shapes=[
            pltpu.VMEM(tabs.shape, F32), pltpu.VMEM((SUB * dm.heads, SUB * dm.heads), BF),
            pltpu.VMEM((dm.all, dm.model), BF), pltpu.VMEM((nb, dm.model, width), BF), pltpu.VMEM((2, dm.heads, dm.window, dm.hd), BF),
            pltpu.VMEM(heads, BF), pltpu.VMEM((3, dm.heads, dm.dec, dm.hd), BF), pltpu.VMEM((3, dm.dec) + three, BF), acc, acc,
            pltpu.VMEM((h, dm.window), F32), pltpu.VMEM((2, h, dm.window), F32), pltpu.VMEM((2, h, dm.window), BF), pltpu.VMEM((2, h, dm.loc), BF),
            pltpu.VMEM((ring, 2, PER, cache) + three, BF), pltpu.VMEM((2, PER, dm.heads, flat), F32), pltpu.VMEM((batch,) + three, F32),
            pltpu.VMEM((batch, dm.loc), BF), pltpu.VMEM((2, dm.rows) + three, BF), pltpu.VMEM((2, k, LANES), F32),
            sem((nb, PER)), sem((4,)), sem((ring, 2)), sem((4,)), vec, vec, vec, vec,
            sem((per_sec + 1,)), sem((per_sec + 1,)), sem((2,)), sem((2,))],
        compiler_params=params(collective_id=layer, has_side_effects=True),
        cost_estimate=cost(flops, dm.model * width * steps * 2),
        name="front")(*ins, w_qkv, freq, lengths, req_len, kc, vc)


def general_attention(dm, meta, qh, kvs):
    nk = LANES + 4 * dm.rows
    groups = dm.heads // PER
    hb = dm.half
    wmax = dm.max_req + hb + WIDE

    def kern(meta_ref, q_ref, *refs):
        srcs = refs[:4]
        o_ref, kcat, sc, bias, mx, ls, pv, lsem = refs[4:]
        g = pl.program_id(0)
        side = lax.axis_index('side')
        row0 = dm.rows * side + hb * meta_ref[0]
        copies = [dma(ref.at[:, at(PER * g, PER, PER)], kcat.at[:, :, at(LANES + dm.rows * (side ^ n), dm.rows)], lsem.at[n]) for n, ref in enumerate(srcs)]
        kcat[:, :, :LANES, :] = jnp.zeros((2, PER, LANES, dm.hd), BF)
        begin(copies)

        ends = [meta_ref[r] for r in range(1, meta_ref.shape[0])]
        n = (row0 + hb - segment_start(row0, ends) // LANES * LANES + WIDE - 1) // WIDE
        begin_col = row0 + hb - WIDE * n
        rows = row0 + lax.broadcasted_iota(jnp.int32, (hb, WIDE), 0)
        st_rows = segment_start(rows, ends)
        lanes = lax.broadcasted_iota(jnp.int32, (hb, WIDE), 1)
        mx[...] = jnp.full_like(mx, NEG)
        ls[...] = jnp.zeros_like(ls)
        pv[...] = jnp.zeros_like(pv)
        finish_all(copies)

        def scores(c):
            first = begin_col + WIDE * c
            col = first + lanes
            bias[...] = jnp.where((col >= st_rows) & (col <= rows), 0.0, NEG)
            for i in range(PER):
                keys = kcat[0, i, at(LANES + first, WIDE), :]
                s = lax.dot_general(q_ref[i], keys, NT, preferred_element_type=F32)
                s = s * (dm.hd ** -0.5 * LOG2E) + bias[...]
                sc[i, :, at(c * WIDE, WIDE)] = s
                mx[i] = jnp.maximum(mx[i], row_max(s))
        each(n, scores)

        def values(c):
            for i in range(PER):
                p = jnp.exp2(sc[i, :, at(c * WIDE, WIDE)] - mx[i][:, :1])
                ls[i] += row_sum(p)
                vals = kcat[1, i, at(LANES + begin_col + WIDE * c, WIDE), :]
                pv[i] += jnp.dot(p.astype(BF), vals, preferred_element_type=F32)
        each(n, values)
        for i in range(PER):
            o_ref[:, i * dm.hd:(i + 1) * dm.hd] = (pv[i] / ls[i]).astype(BF)

    stat = pltpu.VMEM((PER, hb, LANES), F32)
    grid_spec = pltpu.PrefetchScalarGridSpec(
        num_scalar_prefetch=1, grid=(groups,),
        in_specs=[pl.BlockSpec((PER, hb, dm.hd), lambda g, mt: (g, mt[0], 0))] + [ANY] * 4,
        out_specs=pl.BlockSpec((hb, PER * dm.hd), lambda g, mt: (0, g)),
        scratch_shapes=[pltpu.VMEM((2, PER, nk, dm.hd), BF), pltpu.VMEM((PER, hb, wmax), F32), pltpu.VMEM((hb, WIDE), F32), stat, stat, stat, sem((4,))])
    return pl.pallas_call(
        kern, out_shape=sds((hb, dm.loc), BF), grid_spec=grid_spec,
        compiler_params=params(dimension_semantics=("arbitrary",)), name="general_attn")(meta, qh, *kvs)


def post_call(dm, layer, first, resid, co, do, ci, di, kv3, w_out, w_gate, w_up, w_down):
    nb = 6
    kc = dm.model
    ffh = dm.ff // 2
    n_out = dm.model // CHUNK
    n_full = ffh // WIDE
    rem = ffh - n_full * WIDE
    n_gu = n_full + 1
    n_dn = n_out
    ksz = [kc, ffh - kc]
    nk = len(ksz)
    gu0, dn0 = n_out, n_out + n_gu
    total = dn0 + n_dn * nk
    assert rem and n_full % 2
    m = dm.blk
    h, d = dm.half, dm.dhalf
    crow = dm.rows // n_dn
    nr = len(resid)
    early = EARLY_SENT[0 if first else -1]
    cut = early * CHUNK

    def kern(*refs):
        rin = refs[:nr]
        (co_r, do_r, ci_r, di_r, kv, wo, wg, wu, wd, oa, ot, ob, os, kvx, kvp, kvq,
         h1, h1p, xn, act, tmp, wb, acc_a, acc_b, psend, precv, pown, ss, ssp,
         wsem, isem, osem, hss, hrs, pss, prs, yss, yrs, xss, xrs, fss, frs, dss, drs) = refs[nr:]
        tp = lax.axis_index('tp')
        side = lax.axis_index('side')
        core = lax.rem(side, 2)
        to_core = {'side': side + 1 - 2 * core}
        to_x = {'side': lax.rem(side + 2, 4)}
        to_y = {'tp': 1 - tp}

        def cols(j):
            return at(j * CHUNK, CHUNK)

        def out_block(i):
            slot = lax.rem(i, nb)
            return [dma(wo.at[layer, :, cols(i)], wb.at[slot], wsem.at[slot, 0])]

        def gu_block(i, w=WIDE):
            slot = lax.rem(i, nb)
            c = at(core * ffh + (i - gu0) * WIDE, w)
            return [dma(ref.at[layer, :, c], wb.at[slot, :, pl.ds(n * w, w)], wsem.at[slot, n]) for n, ref in enumerate((wg, wu))]

        def dn_block(i, n):
            slot = lax.rem(i, nb)
            r = at(core * ffh + n * kc, ksz[n])
            return [dma(wd.at[layer, r, cols((i - dn0) // nk)], wb.at[slot, pl.ds(0, ksz[n])], wsem.at[slot, 0])]

        def start_late(i):
            pl.when(i < dn0 - 1)(lambda: begin(gu_block(i)))

            @pl.when(i >= dn0 - 1)
            def _():
                pl.when(i == dn0 - 1)(lambda: begin(gu_block(i, rem)))
                for n in range(nk):
                    pl.when((i >= dn0) & (lax.rem(i - dn0, nk) == n))(lambda n=n: begin(dn_block(i, n)))

        mine, theirs = at(tp * h, h, SUB), at(tp * d, d, SUB)
        head_rows, tail_rows = pl.ds(0, h), pl.ds(h, d)
        pairs = [(co_r, tmp.at[0, head_rows]), (do_r, tmp.at[0, tail_rows]), (ci_r, tmp.at[1, head_rows]), (di_r, tmp.at[1, tail_rows])]
        if first:
            pairs += [(rin[0].at[mine], h1.at[head_rows]), (rin[1].at[theirs], h1.at[tail_rows])]
        else:
            split = rin[0].shape[1]
            pairs += [(rin[0], h1.at[:, pl.ds(0, split)]), (rin[1], h1.at[:, pl.ds(split, dm.model - split)])]
        loads = [dma(a, b, isem.at[n]) for n, (a, b) in enumerate(pairs)]
        begin(loads)
        for i in range(nb - 1):
            begin(out_block(jnp.int32(i)))
        meet([to_core, to_x, to_y])

        def bulk(i):
            r = at(i * crow, crow, SUB)
            return remote(kv.at[:, r], kvx.at[:, r], xss.at[i], xrs.at[i], to_x)

        def forward(i):
            r = at(i * crow, crow, SUB)
            return remote(kvx.at[:, r], kvq.at[:, r], fss.at[i], frs.at[i], to_core)

        near = remote(kv, kvp, dss.at[0], drs.at[0], to_core)
        each(n_dn, lambda i: bulk(i).start())
        finish_all(loads)
        for i in range(dm.heads):
            for n, t in enumerate((tp, 1 - tp)):
                xn[:m, at((2 * i + t) * dm.hd, dm.hd)] = tmp[n, :, i * dm.hd:(i + 1) * dm.hd]
        ss[...] = jnp.zeros_like(ss)

        def hsend(j):
            return remote(h1.at[:, cols(j)], h1p.at[:, cols(j)], hss.at[j], hrs.at[j], to_core)

        ss_send = remote(ss, ssp, dss.at[1], drs.at[1], to_core)

        def add_to_hidden(cs, acc):
            out = (h1[:, cs].astype(F32) + acc.astype(BF).astype(F32)).astype(BF)
            h1[:, cs] = out
            return out.astype(F32)

        def out_step(i):
            pl.when(i > 0)(lambda: hsend(i - 1).start())
            pl.when(i + nb - 1 < gu0)(lambda: begin(out_block(i + nb - 1)))
            pl.when(i + nb - 1 >= gu0)(lambda: begin(gu_block(i + nb - 1)))
            finish_all(out_block(i))
            slot = lax.rem(i, nb)
            for n in HALVES:
                acc = jnp.dot(xn[:m, :], wb[slot, :, n:n + WIDE], preferred_element_type=F32)
                out = add_to_hidden(at(i * CHUNK + n, WIDE), acc)
                ss[...] += out[:, :LANES] * out[:, :LANES] + out[:, LANES:] * out[:, LANES:]
        each(n_out, out_step)

        def apply_norm(src, stat, base):
            total_sq = row_sum(stat[...])
            stat[...] = jnp.broadcast_to(lax.rsqrt(total_sq / dm.model + NORM_EPS), stat.shape)

            def step(i):
                sl = at(i * SUB, SUB, SUB)
                for c in range(*dm.lanes):
                    xn[at(base + i * SUB, SUB, SUB), c:c + LANES] = (src[sl, c:c + LANES].astype(F32) * stat[sl, :]).astype(BF)
            each(m // SUB, step)

        ss_send.start()
        hsend(n_out - 1).start()
        ss_send.wait_send()
        apply_norm(h1, ss, 0)
        ss_send.wait_recv()
        each(n_out, lambda j: hsend(j).wait_recv())
        near.start()
        apply_norm(h1p, ssp, m)

        def multiply(i, acc):
            acc[...] = jnp.dot(xn[...], wb[lax.rem(i, nb)], preferred_element_type=F32)

        def glu(acc, j, w):
            gate = acc[:, :w].astype(BF).astype(F32)
            upper = acc[:, w:2 * w].astype(BF).astype(F32)
            act[:, at(j * WIDE, w)] = (jax.nn.silu(gate) * upper).astype(BF)

        begin(gu_block(jnp.int32(gu0 + nb - 1)))
        finish_all(gu_block(jnp.int32(gu0)))
        multiply(jnp.int32(gu0), acc_a)

        def gu_pair(q):
            i = gu0 + 2 * q + 1
            start_late(i + nb - 1)
            finish_all(gu_block(i) + gu_block(i + 1))
            multiply(i, acc_b)
            glu(acc_a, 2 * q, WIDE)
            multiply(i + 1, acc_a)
            glu(acc_b, 2 * q + 1, WIDE)
            start_late(i + nb)
        each(n_full // 2, gu_pair)
        start_late(jnp.int32(dn0 - 2 + nb))
        finish_all(gu_block(jnp.int32(dn0 - 1), rem))
        acc_b[:, :2 * rem] = jnp.dot(xn[...], wb[(dn0 - 1) % nb, :, :2 * rem], preferred_element_type=F32)
        glu(acc_a, n_full - 1, WIDE)
        glu(acc_b, n_full, rem)

        def share(j):
            return remote(h1.at[:, cols(j)], ob.at[:, cols(j)], yss.at[j], yrs.at[j], to_y)

        def keeps(j, fn):
            @pl.when(j < early)
            def _():
                fn(dma(h1.at[:, cols(j)], oa.at[:, cols(j)], osem.at[j]))

            @pl.when(j >= early)
            def _():
                fn(dma(h1.at[:, cols(j)], ot.at[:, cols(j - early)], osem.at[j]))

        def deliver(j):
            keeps(j, lambda c: c.start())
            pl.when(j < early)(lambda: share(j).start())

        def psend_copy(j):
            return remote(psend.at[lax.rem(j, 2)], precv.at[j], pss.at[j], prs.at[j], to_core)

        def finish(j):
            for n in HALVES:
                out = add_to_hidden(at(j * CHUNK + n, WIDE), pown[lax.rem(j, 2), :, n:n + WIDE] + precv[j, :, n:n + WIDE])
                ss[...] += out[:, :LANES] * out[:, :LANES] + out[:, LANES:] * out[:, LANES:]

        def part(rows, slots, n):
            return sum(jnp.dot(act[rows, i * kc:i * kc + ksz[i]], wb[slots[i], :ksz[i], n:n + WIDE], preferred_element_type=F32) for i in range(nk))

        def down(j, lead_in):
            i0 = dn0 + j * nk
            @pl.when(i0 + nb <= total)
            def _():
                if not lead_in:
                    begin(dn_block(i0 + nb - 2, 0))
                begin(dn_block(i0 + nb - 1, 1))
            slots = []
            for n in range(nk):
                finish_all(dn_block(i0 + n, n))
                slots.append(lax.rem(i0 + n, nb))
            half = lax.rem(j, 2)
            pl.when(j > 1)(lambda: psend_copy(j - 2).wait_send())
            if not lead_in:
                psend_copy(j - 1).wait_recv()
                finish(j - 1)
            for n in HALVES:
                psend[half, :, n:n + WIDE] = part(slice(m, 2 * m), slots, n)
            psend_copy(j).start()
            if not lead_in:
                deliver(j - 1)
            for n in HALVES:
                pown[half, :, n:n + WIDE] = part(slice(0, m), slots, n)
            bulk(j).wait_recv()
            forward(j).start()

        each(n_out, lambda j: hsend(j).wait_send())
        ss[...] = jnp.zeros_like(ss)
        down(jnp.int32(0), True)
        each(n_dn - 1, lambda j: down(j + 1, False))
        psend_copy(n_dn - 1).wait_recv()
        finish(n_dn - 1)
        for j in (n_dn - 2, n_dn - 1):
            psend_copy(j).wait_send()
        near.wait()
        deliver(n_dn - 1)
        ss_keep = dma(ss, os, isem.at[0])
        ss_keep.start()
        ss_keep.wait()

        def last(j):
            bulk(j).wait_send()
            forward(j).wait()
            keeps(j, lambda c: c.wait())
            pl.when(j < early)(lambda: share(j).wait())
        each(n_dn, last)

    part1, part2 = sds((m, cut), BF), sds((m, dm.model - cut), BF)
    two = sds(kv3.shape, BF)
    acc = pltpu.VMEM((2 * m, CHUNK), F32)
    pair = pltpu.VMEM((2, m, CHUNK), F32)
    vec = sem((n_dn,))
    stat = pltpu.VMEM((m, LANES), F32)
    return pl.pallas_call(
        kern, out_shape=(part1, part2, part1, sds((m, LANES), F32), two, two, two),
        in_specs=[ANY] * (nr + 9), out_specs=(ANY,) * 7,
        scratch_shapes=[
            pltpu.VMEM((m, dm.model), BF), pltpu.VMEM((m, dm.model), BF), pltpu.VMEM((2 * m, dm.model), BF),
            pltpu.VMEM((2 * m, ffh), BF), pltpu.VMEM((2, m, dm.loc), BF), pltpu.VMEM((nb, kc, CHUNK), BF),
            acc, acc, pair, pltpu.VMEM((n_dn, m, CHUNK), F32), pair, stat, stat,
            sem((nb, 2)), sem((6,)), vec, vec, vec, vec, vec, vec, vec, vec, vec, vec, vec, sem((2,)), sem((2,))],
        compiler_params=params(collective_id=2 + layer, has_side_effects=True),
        cost_estimate=cost(PER * dm.all * dm.model * dm.ff, PER * dm.model * dm.ff),
        name="post")(*resid, co, do, ci, di, kv3, w_out, w_gate, w_up, w_down)


def tail_call(dm, req_len, dest, lengths, kv3, news, kc, vc):
    layers, batch, cache = kc.shape[1:4]
    bits = [1 << b for b in reversed(range(dm.rows.bit_length()))]
    nsrc = len(kv3[0])
    per_layer = batch // PER
    steps = layers * per_layer
    ring = 6
    lag = 2

    def kern(req_ref, dest_ref, len_ref, *refs):
        srcs, refs = refs[:layers * nsrc], refs[layers * nsrc:]
        dec, refs = refs[:layers], refs[layers:]
        kc_ref, vc_ref, ko, vo, kn, vn, buf, slots, dv, lsem, osem, dsem, isem, wsem = refs
        side = lax.axis_index('side')
        start, length = 0, 0
        for r, end in enumerate(request_ends(req_ref)):
            here = dest_ref[r] == side
            start = jnp.where(here, end - req_ref[r], start)
            length = jnp.where(here, req_ref[r], length)

        def pieces(fn):
            for k in range(nsrc):
                first = dm.rows * (side ^ k)
                lo = jnp.maximum(start, first)
                cnt = jnp.maximum(jnp.minimum(start + length, first + dm.rows) - lo, 0)
                for n, bit in enumerate(bits):
                    @pl.when((cnt & bit) != 0)
                    def _(k=k, n=n, bit=bit, first=first, lo=lo, cnt=cnt):
                        off = cnt // (2 * bit) * (2 * bit)
                        for l in range(layers):
                            fn(dma(srcs[l * nsrc + k].at[:, pl.ds(lo - first + off, bit)], buf.at[l, :, pl.ds(lo - start + off, bit)], lsem.at[l, k, n]))

        def spot(i):
            return i // per_layer, at(PER * lax.rem(i, per_layer), PER, PER), lax.rem(i, ring)

        def read(i):
            lay, b, slot = spot(i)
            return [dma(ref.at[0, lay, b], slots.at[slot, n], isem.at[slot, n]) for n, ref in enumerate((kc_ref, vc_ref))]

        def write(i):
            lay, b, slot = spot(i)
            return [dma(slots.at[slot, n], ref.at[0, lay, b], wsem.at[slot, n]) for n, ref in enumerate((kn, vn))]

        dloads = [dma(ref, dv.at[n], dsem.at[n]) for n, ref in enumerate(dec)]
        begin(dloads)
        pieces(lambda c: c.start())
        for i in range(ring - lag):
            begin(read(jnp.int32(i)))

        def zero(r, c):
            buf[:, :, r] = jnp.zeros((layers, 2, dm.heads, dm.hd), BF)
            return c
        lax.fori_loop(length, dm.max_req, zero, 0)
        finish_all(dloads)
        pieces(lambda c: c.wait())
        outs = [dma(buf.at[l, n], ref.at[0, l], osem.at[l, n]) for l in range(layers) for n, ref in enumerate((ko, vo))]
        begin(outs)

        def step(i):
            lay, _, slot = spot(i)
            finish_all(read(i))
            for n in range(PER):
                b = PER * lax.rem(i, per_layer) + n
                for kind in range(2):
                    slots[slot, kind, n, len_ref[b]] = dv[lay, kind, b]
            pl.when(i > 0)(lambda: begin(write(i - 1)))

            @pl.when(i + ring - lag < steps)
            def _():
                pl.when(i >= lag)(lambda: finish_all(write(i - lag)))
                begin(read(i + ring - lag))
        each(steps, step)
        begin(write(jnp.int32(steps - 1)))
        each(ring, lambda i: finish_all(write(steps - ring + i)))
        finish_all(outs)

    shape = sds((1, layers, dm.max_req, dm.heads, dm.hd), BF)
    three = (dm.heads, dm.hd)
    flat = [ref for group in kv3 for ref in group]
    pair = sem((layers, 2))
    return pl.pallas_call(
        kern, out_shape=(shape, shape, sds(kc.shape, BF), sds(vc.shape, BF)),
        in_specs=[SMEM] * 3 + [ANY] * (len(flat) + layers + 2), out_specs=(ANY,) * 4,
        scratch_shapes=[pltpu.VMEM((layers, 2, dm.max_req) + three, BF), pltpu.VMEM((ring, 2, PER, cache) + three, BF), pltpu.VMEM((layers,) + news[0].shape, BF),
                        sem((layers, nsrc, len(bits))), pair, sem((layers,)), sem((ring, 2)), sem((ring, 2))],
        compiler_params=params(),
        cost_estimate=cost(10**11, kc.size),
        name="tail")(req_len, dest, lengths, *flat, *news, kc, vc)


def close_call(dm, mine, theirs):
    cut = mine[0].shape[1]
    h, d, k = dm.half, dm.dhalf, dm.blk

    def kern(a1, a2, b1, b2, hid, dec, buf, lsem, osem):
        tp = lax.axis_index('tp')
        moves = []
        for n, (ref, blk, col) in enumerate(((a1, tp, 0), (a2, tp, cut), (b1, 1 - tp, 0), (b2, 1 - tp, cut))):
            cs = pl.ds(col, ref.shape[1])
            rows = blk * k
            moves.append((dma(ref, buf.at[at(rows, k, SUB), cs], lsem.at[n]),
                          [dma(buf.at[at(rows, h, SUB), cs], hid.at[at(blk * h, h, SUB), cs], osem.at[0, n]),
                           dma(buf.at[at(rows + h, d, SUB), cs], dec.at[at(blk * d, d, SUB), cs], osem.at[1, n])]))
        begin([load for load, _ in moves])
        for load, outs in moves:
            load.wait()
            begin(outs)
        for _, outs in moves:
            finish_all(outs)

    return pl.pallas_call(
        kern, out_shape=(sds((dm.rows, dm.model), BF), sds((dm.dec, dm.model), BF)),
        in_specs=[ANY] * 4, out_specs=(ANY, ANY),
        scratch_shapes=[pltpu.VMEM((dm.all, dm.model), BF), sem((4,)), sem((2, 4))],
        compiler_params=params(), name="close")(*mine, *theirs)


def solution(mesh):
    tp_size = mesh.shape['tp']
    side_size = mesh.shape['side']
    rows_spec = P(('pair', 'side'), None)
    batch_spec = P(('pair', 'side'), None, None)
    cache_spec = P(('pair', 'side'), None, None, None, 'tp', None)
    prompt_spec = P(('pair', 'side'), None, None, 'tp', None)

    def swap(val, axis, bit):
        size = tp_size if axis == 'tp' else side_size
        return lax.ppermute(val, axis, [(i, i ^ bit) for i in range(size)])

    def local_step(x_loc, req_len, dest, w_qkv, w_out, w_gate, w_up, w_down, y_loc, kc, vc, clen_loc):
        side = lax.axis_index('side')
        tp = lax.axis_index('tp')
        layers = w_qkv.shape[0]
        rows = x_loc.shape[0]
        y = y_loc[0]
        lengths = clen_loc[0]
        dm = Dims(rows, y.shape[0], x_loc.shape[1], kc.shape[-2], kc.shape[-1], w_gate.shape[2], 2 * rows - rows // 4)

        ends = jnp.sum(jnp.where(jnp.arange(side_size)[:, None] >= jnp.arange(side_size)[None, :], req_len[None, :], 0), axis=1)
        mid = rows * side_size // 2
        fast = mid - jnp.max(jnp.where(ends <= mid, ends, 0)) <= LANES
        half_dim = dm.hd // 2
        inv_freq = ROPE_BASE ** (-jnp.arange(half_dim, dtype=F32) / half_dim)
        freq = jnp.concatenate([inv_freq, inv_freq])[None]

        ins = resid = (x_loc, y)
        fresh, kv_all = [], []
        for layer in range(layers):
            first = layer == 0
            kvh, kv3, qh, dec, co, ci, do, di, tab = front_call(dm, layer, first, ins, w_qkv, freq, lengths, req_len, kc, vc)
            fresh.append(dec)

            def general(i, ctx):
                kv, q, edges, _ = lax.optimization_barrier((kvh, qh, ends, i))
                kvx = swap(kv, 'side', 2)
                kvs = (kv, swap(kv, 'side', 1), kvx, swap(kvx, 'side', 1))
                own, other = (general_attention(dm, jnp.concatenate([b[None], edges]), q, kvs) for b in (tp, 1 - tp))
                return own, swap(other, 'tp', 1)
            co, ci = lax.fori_loop(0, jnp.where(fast, 0, 1), general, (co, ci))
            o1, o2, p1, stat, kv3_x, kv3_p, kv3_q = post_call(dm, layer, first, resid, co, do, ci, di, kv3, w_out, w_gate, w_up, w_down)
            if layer == layers - 1:
                p2 = swap(o2, 'tp', 1)
            kv_all.append((kv3, kv3_p, kv3_x, kv3_q))
            ins, resid = (o1, o2, p1, stat, tab), (o1, o2)
        k_prompt, v_prompt, k_new, v_new = tail_call(dm, req_len, dest, lengths, kv_all, fresh, kc, vc)
        hidden, dec_out = close_call(dm, (o1, o2), (p1, p2))
        return hidden, dec_out[None], k_prompt, v_prompt, k_new, v_new

    return jax.shard_map(local_step, mesh=mesh,
                         in_specs=(rows_spec, P('pair'), P('pair'), P(), P(), P(), P(), P(), batch_spec, cache_spec, cache_spec, rows_spec),
                         out_specs=(rows_spec, batch_spec, prompt_spec, prompt_spec, cache_spec, cache_spec),
                         check_vma=False)
```

```python
import jax
import jax.numpy as jnp
from jax import lax
from jax.experimental import pallas as pl
from jax.experimental.pallas import tpu as pltpu
from jax.sharding import PartitionSpec as P

ROPE_BASE = 10000.0
NORM_EPS = 1e-5
NEG = -1e30
BF = jnp.bfloat16
F32 = jnp.float32
ANY = pl.BlockSpec(memory_space=pl.ANY)
SMEM = pl.BlockSpec(memory_space=pltpu.SMEM)
WHOLE = pl.BlockSpec(memory_space=pltpu.VMEM)
HBM = pl.BlockSpec(memory_space=pltpu.HBM)
VMEM_LIMIT = 61 * 2**20
LOG2E = 1.4426950408889634
LANES = 128
WIDE = 256
CHUNK = 512
HALVES = (0, WIDE)
SUB = 16
PER = 4
EARLY_SENT = (4, 3)
NT = (((1,), (1,)), ((), ()))
dma = pltpu.make_async_copy
sds = jax.ShapeDtypeStruct
sem = pltpu.SemaphoreType.DMA


def at(start, size, multiple=LANES):
    return pl.ds(pl.multiple_of(start, multiple), size)


def cost(flops, size):
    return pl.CostEstimate(flops=flops, bytes_accessed=size, transcendentals=0)


def params(**kw):
    return pltpu.CompilerParams(vmem_limit_bytes=VMEM_LIMIT, **kw)


def remote(src, dst, send, recv, dev):
    return pltpu.make_async_remote_copy(src_ref=src, dst_ref=dst, send_sem=send, recv_sem=recv, device_id=dev, device_id_type=pl.DeviceIdType.MESH)


def meet(devices):
    barrier = pltpu.get_barrier_semaphore()
    for dev in devices:
        pl.semaphore_signal(barrier, device_id=dev, device_id_type=pl.DeviceIdType.MESH)
    pl.semaphore_wait(barrier, len(devices))


def each(count, fn):
    lax.fori_loop(0, count, lambda i, c: (fn(i), c)[1], 0)


def begin(copies):
    for cp in copies:
        cp.start()


def finish_all(copies):
    for cp in copies:
        cp.wait()


def row_sum(x):
    return jnp.sum(x, axis=1, keepdims=True)


def row_max(x):
    return jnp.max(x, axis=1, keepdims=True)


def norm_rows(ref, base, rows):
    group = 2 if rows % (2 * SUB) == 0 else 1

    def step(i):
        for n in range(group):
            sl = at(base + (group * i + n) * SUB, SUB, SUB)
            wide = ref[sl, :].astype(F32)
            scale = lax.rsqrt(jnp.mean(wide * wide, axis=-1, keepdims=True) + NORM_EPS)
            ref[sl, :] = (wide * scale).astype(BF)
    each(rows // SUB // group, step)


def request_ends(len_ref):
    ends = [len_ref[0]]
    for r in range(1, 4):
        ends.append(ends[-1] + len_ref[r])
    return ends


def segment_start(row, ends):
    start = jnp.zeros_like(row)
    for end in ends:
        start = jnp.where(row >= end, end, start)
    return start


class Dims:
    def __init__(self, rows, dec, model, heads, head_dim, ff, max_req):
        self.rows, self.half = rows, rows // 2
        self.dec, self.dhalf = dec, dec // 2
        self.blk = self.half + self.dhalf
        self.all = 2 * self.blk
        self.model, self.heads, self.hd, self.ff = model, heads, head_dim, ff
        self.max_req = max_req
        self.loc = heads * head_dim
        self.window = LANES + 2 * rows
        self.lanes = (0, model, LANES)


def front_call(dm, layer, first, ins, w_qkv, freq, lengths, req_len, kc, vc):
    nb = 4
    per_sec = dm.heads // PER
    steps = 3 * per_sec
    kv_steps = 2 * per_sec
    h, d, k = dm.half, dm.dhalf, dm.blk
    m = dm.all if first else k
    npass = dm.all // m
    width = PER * dm.hd
    lead = dm.window - dm.rows
    batch, cache = kc.shape[2], kc.shape[3]
    flat = cache * dm.heads
    ring = 4
    dsteps = batch // PER
    ni = len(ins)

    def kern(*refs):
        rin = refs[:ni]
        (w_ref, f_ref, len_ref, req_ref, k_ref, v_ref, kvh, kv3, qh, dec, co, ci, do, di, tab_out,
         tab, perm_ref, xn, wb, kcat, qv, sd, dv, acc_a, acc_b, bias, sbuf, pbuf, cbuf, cr, dsc, dbuf, dout, o3, stat,
         wsem, isem, csem, tsem, pss, prs, ess, ers, yss, yrs, lss, lrs, ksem) = refs[ni:]
        tp = lax.axis_index('tp')
        side = lax.axis_index('side')
        odd = lax.rem(side, 2)
        to_y = {'tp': 1 - tp}

        def wcopies(i):
            slot = lax.rem(i, nb)
            j = lax.rem(i, steps)
            sec = j // per_sec
            base = jnp.where(sec == 2, 0, (sec + 1) * 2 * dm.loc)
            out = []
            for n in range(PER):
                col = base + (2 * (PER * lax.rem(j, per_sec) + n) + tp) * dm.hd
                out.append(dma(w_ref.at[layer, :, at(col, dm.hd)], wb.at[slot, :, pl.ds(n * dm.hd, dm.hd)], wsem.at[slot, n]))
            return out

        def group_of(i):
            return lax.rem(i + tp * (dsteps // 2), dsteps)

        def caches(i):
            slot = lax.rem(i, ring)
            b = at(PER * group_of(i), PER, PER)
            return [dma(ref.at[0, layer, b], cr.at[slot, n], csem.at[slot, n]) for n, ref in enumerate((k_ref, v_ref))]

        if first:
            parts = [(rin[0], 0, 0, h), (rin[1], 0, h, d), (rin[0], h, k, h), (rin[1], d, k + h, d)]
            loads = [dma(ref.at[pl.ds(src, n)], xn.at[pl.ds(dst, n)], isem.at[i]) for i, (ref, src, dst, n) in enumerate(parts)]
        else:
            own1, own2, peer1, ss_in, tab_in = rin
            cut = own1.shape[1]
            head_cols, tail_cols = pl.ds(0, cut), pl.ds(cut, dm.model - cut)
            top, low_rows = pl.ds(0, k), pl.ds(k, k)
            loads = [dma(own1, xn.at[top, head_cols], isem.at[0]), dma(own2, xn.at[top, tail_cols], isem.at[1]),
                     dma(ss_in, stat.at[0], isem.at[2]), dma(peer1, xn.at[low_rows, head_cols], isem.at[3]), dma(tab_in, tab, tsem.at[1])]
        begin(loads)
        begin(wcopies(jnp.int32(0)))

        def zero(i):
            kcat[:, i, pl.ds(0, lead), :] = jnp.zeros((2, lead, dm.hd), BF)
        each(dm.heads, zero)
        src = lax.broadcasted_iota(jnp.int32, perm_ref.shape, 0)
        dst = lax.broadcasted_iota(jnp.int32, perm_ref.shape, 1)
        perm_ref[...] = (lax.rem(src, dm.heads) * SUB + src // dm.heads == dst).astype(F32).astype(BF)
        ends = request_ends(req_ref)

        def table(row, pos):
            size = pos.shape[0]
            ang = pos.astype(F32) * f_ref[...]
            sign = jnp.where(lax.broadcasted_iota(jnp.int32, pos.shape, 1) < dm.hd // 2, -1.0, 1.0)
            tab[0, at(row, size, SUB), :] = jnp.cos(ang)
            tab[1, at(row, size, SUB), :] = jnp.sin(ang) * sign

        if first:
            for b in range(2):
                def rows_table(i):
                    row = dm.rows * side + b * h + i * PER * SUB + lax.broadcasted_iota(jnp.int32, (PER * SUB, LANES), 0)
                    table(b * k + i * PER * SUB, row - segment_start(row, ends))
                each(h // SUB // PER, rows_table)
                which = lax.broadcasted_iota(jnp.int32, (d, LANES), 0)
                pos = jnp.zeros_like(which)
                for i in range(d):
                    pos = jnp.where(which == i, len_ref[b * d + i], pos)
                table(b * k + h, pos)
        meet([{'side': lax.rem(side + i, 4)} for i in range(1, 4)] + [to_y])
        late = []
        if not first:
            late = [remote(own2, xn.at[low_rows, tail_cols], lss.at[0], lrs.at[0], to_y),
                    remote(ss_in, stat.at[1], lss.at[1], lrs.at[1], to_y)]
            begin(late[::-1])

        def own_part(j):
            return kcat.at[j // per_sec, at(PER * lax.rem(j, per_sec), PER, PER), pl.ds(lead, dm.rows)]

        def edge_part(j, row):
            return kcat.at[j // per_sec, at(PER * lax.rem(j, per_sec), PER, PER), pl.ds(row, LANES)]

        def peer_copy(j):
            dst = kcat.at[j // per_sec, at(PER * lax.rem(j, per_sec), PER, PER), pl.ds(LANES, dm.rows)]
            return remote(own_part(j), dst, pss.at[j], prs.at[j], {'side': side + 1})

        def edge_copy(j, to):
            row = dm.window - LANES if to == 2 else dm.rows
            return remote(edge_part(j, row), edge_part(j, (3 - to) * dm.rows), ess.at[j], ers.at[j], {'side': to})

        def send(j):
            pl.when(odd == 0)(lambda: peer_copy(j).start())
            pl.when(side == 1)(lambda: edge_copy(j, 2).start())

        def arrived(j):
            pl.when(odd == 1)(lambda: peer_copy(j).wait_recv())

            @pl.when(side == 2)
            def _():
                edge_copy(j, 2).wait_recv()
                edge_copy(j, 3).start()
            pl.when(side == 3)(lambda: edge_copy(j, 3).wait_recv())

        def sent(j):
            pl.when(odd == 0)(lambda: peer_copy(j).wait_send())
            pl.when(side == 1)(lambda: edge_copy(j, 2).wait_send())
            pl.when(side == 2)(lambda: edge_copy(j, 3).wait_send())

        def ahead(i):
            @pl.when(i + nb - 1 < npass * steps)
            def _():
                begin(wcopies(i + nb - 1))

        def fetch(i, more):
            if more:
                ahead(i)
            finish_all(wcopies(i))

        def multiply(i, rows, acc):
            acc[...] = jnp.dot(xn[rows, :], wb[lax.rem(i, nb)], preferred_element_type=F32)

        def dots(i, rows, acc):
            fetch(i, True)
            multiply(i, rows, acc)

        def epilogue(j, acc, blocks, is_q):
            sec, jj = j // per_sec, lax.rem(j, per_sec)
            for r0, b in blocks:
                rows = slice(r0, r0 + k)
                cv, sv = tab[0, at(b * k, k, SUB), :], tab[1, at(b * k, k, SUB), :]
                for n in range(PER):
                    head = PER * jj + n
                    val = acc[rows, n * dm.hd:(n + 1) * dm.hd].astype(BF).astype(F32)
                    rot = val * cv + pltpu.roll(val, dm.hd // 2, 1) * sv
                    low = (rot if is_q else jnp.where(sec == 1, val, rot)).astype(BF)
                    if is_q:
                        qv[head, at(b * h, h, SUB), :] = low[:h]
                    else:
                        kcat[sec, head, at(lead + b * h, h, SUB), :] = low[:h]
                    sd[sec, head, at(b * d, d, d), :] = low[h:]

        def run(p, blocks):
            rows = pl.ds(p * m, m)
            base = p * steps
            final = p == npass - 1
            last = kv_steps

            def done(j):
                if final:
                    pl.when(j > 0)(lambda: send(j - 1))

            dots(jnp.int32(base), rows, acc_a)

            def pair(q):
                i = base + 2 * q + 1
                fetch(i, True)
                fetch(i + 1, False)
                multiply(i, rows, acc_b)
                epilogue(2 * q, acc_a, blocks, False)
                multiply(i + 1, rows, acc_a)
                epilogue(2 * q + 1, acc_b, blocks, False)
                ahead(i + 1)
                done(2 * q)
                done(2 * q + 1)
            each(last // 2 - 1, pair)
            dots(jnp.int32(base + last - 1), rows, acc_b)
            epilogue(jnp.int32(last - 2), acc_a, blocks, False)
            done(jnp.int32(last - 2))
            if final:
                epilogue(jnp.int32(last - 1), acc_b, blocks, False)
                done(jnp.int32(last - 1))
                return
            dots(jnp.int32(base + last), rows, acc_a)
            epilogue(jnp.int32(last - 1), acc_b, blocks, False)
            for n in range(1, per_sec):
                prev, acc = (acc_a, acc_b) if n % 2 else (acc_b, acc_a)
                dots(jnp.int32(base + last + n), rows, acc)
                epilogue(jnp.int32(last + n - 1), prev, blocks, True)
            epilogue(jnp.int32(steps - 1), acc, blocks, True)

        def apply_norm(n, base):
            total_sq = row_sum(stat[n])
            stat[n] = jnp.broadcast_to(lax.rsqrt(total_sq / dm.model + NORM_EPS), (k, LANES))

            def step(i):
                sl = at(base + i * SUB, SUB, SUB)
                for c in range(*dm.lanes):
                    xn[sl, c:c + LANES] = (xn[sl, c:c + LANES].astype(F32) * stat[n, at(i * SUB, SUB, SUB), :]).astype(BF)
            each(k // SUB, step)

        def fill():
            for i in range(1, nb - 1):
                begin(wcopies(jnp.int32(i)))
            for i in range(2):
                begin(caches(jnp.int32(i)))

        def cols(g):
            return at(width * g, width)

        def ctx_send(g):
            return remote(cbuf.at[0, :, cols(g)], ci.at[:, cols(g)], yss.at[g], yrs.at[g], to_y)

        def ctx_keep(g):
            return dma(cbuf.at[1, :, cols(g)], co.at[:, cols(g)], ksem.at[g])

        dec_send = remote(dout.at[at((1 - tp) * d, d, SUB)], di, yss.at[per_sec], yrs.at[per_sec], to_y)
        dec_keep = dma(dout.at[at(tp * d, d, SUB)], do, isem.at[0])

        def score(b, w, head, n):
            sbuf[n % 2, :, :w] = lax.dot_general(qv[head, b * h:(b + 1) * h, :], kcat[0, head, :w, :], NT, preferred_element_type=F32)

        def value(ph, w, head, n):
            s = sbuf[n % 2, :, :w] * (dm.hd ** -0.5 * LOG2E) + bias[:, :w]
            p = jnp.exp2(s - row_max(s))
            pbuf[n % 2, :, :w] = p.astype(BF)
            tot = row_sum(p)
            o = jnp.dot(pbuf[n % 2, :, :w], kcat[1, head, :w, :], preferred_element_type=F32)
            cbuf[ph, :, at(head * dm.hd, dm.hd)] = (o / tot).astype(BF)

        def turn_rows(rows, out):
            x = jnp.concatenate([r.reshape(SUB * dm.heads, dm.hd) for r in rows], axis=1)
            y = jnp.dot(perm_ref[...], x, preferred_element_type=F32).astype(BF)
            for n, dst in enumerate(out):
                dst(y[:, n * dm.hd:(n + 1) * dm.hd].reshape(SUB, dm.heads, dm.hd))

        def decode_half(part):
            col = lax.broadcasted_iota(jnp.int32, (dm.heads, flat), 1)
            row = lax.broadcasted_iota(jnp.int32, (dm.heads, flat), 0)
            pos = jnp.where(lax.rem(col, dm.heads) == row, col // dm.heads, flat)
            scale = dm.hd ** -0.5
            count = dsteps // 2

            def look(n):
                i = part * count + n

                @pl.when(i + 2 < dsteps)
                def _():
                    begin(caches(i + 2))
                finish_all(caches(i))
                for r in range(PER):
                    keys = cr[lax.rem(i, ring), 0, r].reshape(flat, dm.hd)
                    dsc[n % 2, r] = lax.dot_general(dv[2, PER * group_of(i) + r], keys, NT, preferred_element_type=F32)

            def gather(n):
                i = part * count + n
                for r in range(PER):
                    bi = PER * group_of(i) + r
                    q, kn, vn = (dv[c, bi].astype(F32) for c in (2, 0, 1))
                    s = jnp.where(pos < len_ref[bi], dsc[n % 2, r] * scale, NEG)
                    fresh = row_sum(q * kn) * scale
                    top = jnp.maximum(row_max(s), fresh)
                    p = jnp.exp(s - top)
                    pf = jnp.exp(fresh - top)
                    inv = 1.0 / (row_sum(p) + pf)
                    vals = cr[lax.rem(i, ring), 1, r].reshape(flat, dm.hd)
                    o = jnp.dot((p * inv).astype(BF), vals, preferred_element_type=F32)
                    dbuf[bi] = o + (pf * inv).astype(BF).astype(F32) * vn

            look(0)
            for n in range(count):
                if n + 1 < count:
                    look(n + 1)
                gather(n)

        def put(ref, *idx):
            def store(val):
                ref[idx] = val
            return store

        def turn_block(b):
            sl = at(b * d, d, SUB)
            turn_rows([sd[n, :, sl, :] for n in range(3)], [put(dv, n, sl) for n in range(3)])

            def block(i):
                for n in range(PER):
                    row = b * h + (PER * i + n) * SUB
                    sl, own = at(row, SUB, SUB), at(lead + row, SUB, SUB)
                    turn_rows([kcat[n2, :, own, :] for n2 in range(2)], [put(o3, n2, sl) for n2 in range(2)])
            each(h // SUB // PER, block)

        if first:
            tab_copy = dma(tab, tab_out, tsem.at[1])
            tab_copy.start()
            for cp, (_, _, row, size) in zip(loads, parts):
                cp.wait()
                if row == h:
                    fill()
                norm_rows(xn, row, size)
            blocks = [(0, 0), (k, 1)]
        else:
            finish_all(loads[:3] + loads[4:])
            fill()
            apply_norm(0, 0)
            run(0, [(0, tp)])
            turn_block(tp)
            decode_half(0)
            loads[3].wait()
            finish_all(late)
            apply_norm(1, k)
            blocks = [(0, 1 - tp)]
        run(npass - 1, blocks)

        kv3_copy = dma(o3, kv3, tsem.at[0])
        kvh_copy = dma(kcat.at[:, :, pl.ds(lead, dm.rows)], kvh, isem.at[2])
        q_copy = dma(qv, qh, tsem.at[2])
        dec_copy = dma(dv, dec, tsem.at[3])

        def stage(t):
            ph, g = t // per_sec, lax.rem(t, per_sec)
            b = lax.rem(1 + tp + ph, 2)

            @pl.when(ph == 0)
            def _():
                dots(npass * steps - per_sec + g, pl.ds((npass - 1) * m, m), acc_a)
                epilogue(kv_steps + g, acc_a, blocks, True)
                pl.when(g == 0)(lambda: send(kv_steps - 1))
                arrived(g)
                arrived(per_sec + g)

            @pl.when(t == per_sec)
            def _():
                ctx_send(per_sec - 1).start()
                if first:
                    each(2, turn_block)
                    each(2, decode_half)
                else:
                    turn_block(1 - tp)
                    decode_half(1)
                for n in range(dm.heads):
                    dout[:, n * dm.hd:(n + 1) * dm.hd] = dbuf[:, n, :].astype(BF)
                begin([kv3_copy, kvh_copy, q_copy, dec_copy])

            @pl.when(g == 0)
            def _():
                rows = dm.rows * side + h * b + lax.broadcasted_iota(jnp.int32, (h, LANES), 0)
                start = segment_start(rows, ends)
                lane = dm.rows * side - lead + lax.broadcasted_iota(jnp.int32, (h, LANES), 1)
                for c in range(dm.window // LANES):
                    col = lane + c * LANES
                    bias[:, c * LANES:(c + 1) * LANES] = jnp.where((col >= start) & (col <= rows), 0.0, NEG)
            pl.when(t == per_sec)(lambda: begin([dec_send, dec_keep]))

            for bb, w in enumerate((dm.window - h, dm.window)):
                @pl.when(b == bb)
                def _(bb=bb, w=w):
                    score(bb, w, PER * g, 0)
                    for n in range(PER):
                        if n + 1 < PER:
                            score(bb, w, PER * g + n + 1, n + 1)
                        value(ph, w, PER * g + n, n)
            pl.when((ph == 0) & (g > 0))(lambda: ctx_send(g - 1).start())
            pl.when((ph > 0) & (g > 0))(lambda: ctx_keep(g - 1).start())
        each(2 * per_sec, stage)

        if first:
            tab_copy.wait()
        ctx_keep(per_sec - 1).start()
        each(kv_steps, sent)
        finish_all([kv3_copy, kvh_copy, q_copy, dec_copy, dec_keep, dec_send])
        each(per_sec, lambda g: ctx_keep(g).wait())
        each(per_sec, lambda g: ctx_send(g).wait())

    heads = (dm.heads, dm.rows, dm.hd)
    three = (dm.heads, dm.hd)
    flops = 2 * dm.all * dm.model * width * steps
    outs = [(2,) + heads, (2, dm.rows) + three, heads, (3, dm.dec) + three, (h, dm.loc), (h, dm.loc), (d, dm.loc), (d, dm.loc)]
    acc = pltpu.VMEM((m, width), F32)
    tabs = sds((2, dm.all, LANES), F32)
    vec = sem((kv_steps,))
    return pl.pallas_call(
        kern, out_shape=tuple(sds(s, BF) for s in outs) + (tabs,),
        in_specs=[ANY] * (ni + 1) + [WHOLE] + [SMEM] * 2 + [ANY] * 2, out_specs=(ANY,) * (len(outs) + 1),
        scratch_shapes=[
            pltpu.VMEM(tabs.shape, F32), pltpu.VMEM((SUB * dm.heads, SUB * dm.heads), BF),
            pltpu.VMEM((dm.all, dm.model), BF), pltpu.VMEM((nb, dm.model, width), BF), pltpu.VMEM((2, dm.heads, dm.window, dm.hd), BF),
            pltpu.VMEM(heads, BF), pltpu.VMEM((3, dm.heads, dm.dec, dm.hd), BF), pltpu.VMEM((3, dm.dec) + three, BF), acc, acc,
            pltpu.VMEM((h, dm.window), F32), pltpu.VMEM((2, h, dm.window), F32), pltpu.VMEM((2, h, dm.window), BF), pltpu.VMEM((2, h, dm.loc), BF),
            pltpu.VMEM((ring, 2, PER, cache) + three, BF), pltpu.VMEM((2, PER, dm.heads, flat), F32), pltpu.VMEM((batch,) + three, F32),
            pltpu.VMEM((batch, dm.loc), BF), pltpu.VMEM((2, dm.rows) + three, BF), pltpu.VMEM((2, k, LANES), F32),
            sem((nb, PER)), sem((4,)), sem((ring, 2)), sem((4,)), vec, vec, vec, vec,
            sem((per_sec + 1,)), sem((per_sec + 1,)), sem((2,)), sem((2,)), sem((per_sec,))],
        compiler_params=params(collective_id=layer, has_side_effects=True),
        cost_estimate=cost(flops, dm.model * width * steps * 2),
        name="front")(*ins, w_qkv, freq, lengths, req_len, kc, vc)


def general_attention(dm, meta, qh, kvs):
    nk = LANES + 4 * dm.rows
    groups = dm.heads // PER
    hb = dm.half
    wmax = dm.max_req + hb + WIDE

    def kern(meta_ref, q_ref, *refs):
        srcs = refs[:4]
        o_ref, kcat, sc, bias, mx, ls, pv, lsem = refs[4:]
        g = pl.program_id(0)
        side = lax.axis_index('side')
        row0 = dm.rows * side + hb * meta_ref[0]
        copies = [dma(ref.at[:, at(PER * g, PER, PER)], kcat.at[:, :, at(LANES + dm.rows * (side ^ n), dm.rows)], lsem.at[n]) for n, ref in enumerate(srcs)]
        kcat[:, :, :LANES, :] = jnp.zeros((2, PER, LANES, dm.hd), BF)
        begin(copies)

        ends = [meta_ref[r] for r in range(1, meta_ref.shape[0])]
        n = (row0 + hb - segment_start(row0, ends) // LANES * LANES + WIDE - 1) // WIDE
        begin_col = row0 + hb - WIDE * n
        rows = row0 + lax.broadcasted_iota(jnp.int32, (hb, WIDE), 0)
        st_rows = segment_start(rows, ends)
        lanes = lax.broadcasted_iota(jnp.int32, (hb, WIDE), 1)
        mx[...] = jnp.full_like(mx, NEG)
        ls[...] = jnp.zeros_like(ls)
        pv[...] = jnp.zeros_like(pv)
        finish_all(copies)

        def scores(c):
            first = begin_col + WIDE * c
            col = first + lanes
            bias[...] = jnp.where((col >= st_rows) & (col <= rows), 0.0, NEG)
            for i in range(PER):
                keys = kcat[0, i, at(LANES + first, WIDE), :]
                s = lax.dot_general(q_ref[i], keys, NT, preferred_element_type=F32)
                s = s * (dm.hd ** -0.5 * LOG2E) + bias[...]
                sc[i, :, at(c * WIDE, WIDE)] = s
                mx[i] = jnp.maximum(mx[i], row_max(s))
        each(n, scores)

        def values(c):
            for i in range(PER):
                p = jnp.exp2(sc[i, :, at(c * WIDE, WIDE)] - mx[i][:, :1])
                ls[i] += row_sum(p)
                vals = kcat[1, i, at(LANES + begin_col + WIDE * c, WIDE), :]
                pv[i] += jnp.dot(p.astype(BF), vals, preferred_element_type=F32)
        each(n, values)
        for i in range(PER):
            o_ref[:, i * dm.hd:(i + 1) * dm.hd] = (pv[i] / ls[i]).astype(BF)

    stat = pltpu.VMEM((PER, hb, LANES), F32)
    grid_spec = pltpu.PrefetchScalarGridSpec(
        num_scalar_prefetch=1, grid=(groups,),
        in_specs=[pl.BlockSpec((PER, hb, dm.hd), lambda g, mt: (g, mt[0], 0))] + [ANY] * 4,
        out_specs=pl.BlockSpec((hb, PER * dm.hd), lambda g, mt: (0, g)),
        scratch_shapes=[pltpu.VMEM((2, PER, nk, dm.hd), BF), pltpu.VMEM((PER, hb, wmax), F32), pltpu.VMEM((hb, WIDE), F32), stat, stat, stat, sem((4,))])
    return pl.pallas_call(
        kern, out_shape=sds((hb, dm.loc), BF), grid_spec=grid_spec,
        compiler_params=params(dimension_semantics=("arbitrary",)), name="general_attn")(meta, qh, *kvs)


def post_call(dm, layer, first, resid, co, do, ci, di, kv3, w_out, w_gate, w_up, w_down):
    nb = 6
    kc = dm.model
    ffh = dm.ff // 2
    n_out = dm.model // CHUNK
    n_full = ffh // WIDE
    rem = ffh - n_full * WIDE
    n_gu = n_full + 1
    n_dn = n_out
    ksz = [kc, ffh - kc]
    nk = len(ksz)
    gu0, dn0 = n_out, n_out + n_gu
    total = dn0 + n_dn * nk
    assert rem and n_full % 2
    m = dm.blk
    h, d = dm.half, dm.dhalf
    crow = dm.rows // n_dn
    nr = len(resid)
    early = EARLY_SENT[0 if first else -1]
    cut = early * CHUNK

    def kern(*refs):
        rin = refs[:nr]
        (co_r, do_r, ci_r, di_r, kv, wo, wg, wu, wd, oa, ot, ob, os, kvx, kvp, kvq,
         h1, h1p, xn, act, tmp, wb, acc_a, acc_b, psend, precv, pown, ss, ssp,
         wsem, isem, osem, hss, hrs, pss, prs, yss, yrs, xss, xrs, fss, frs, dss, drs) = refs[nr:]
        tp = lax.axis_index('tp')
        side = lax.axis_index('side')
        core = lax.rem(side, 2)
        to_core = {'side': side + 1 - 2 * core}
        to_x = {'side': lax.rem(side + 2, 4)}
        to_y = {'tp': 1 - tp}

        def cols(j):
            return at(j * CHUNK, CHUNK)

        def out_block(i):
            slot = lax.rem(i, nb)
            return [dma(wo.at[layer, :, cols(i)], wb.at[slot], wsem.at[slot, 0])]

        def gu_block(i, w=WIDE):
            slot = lax.rem(i, nb)
            c = at(core * ffh + (i - gu0) * WIDE, w)
            return [dma(ref.at[layer, :, c], wb.at[slot, :, pl.ds(n * w, w)], wsem.at[slot, n]) for n, ref in enumerate((wg, wu))]

        def dn_block(i, n):
            slot = lax.rem(i, nb)
            r = at(core * ffh + n * kc, ksz[n])
            return [dma(wd.at[layer, r, cols((i - dn0) // nk)], wb.at[slot, pl.ds(0, ksz[n])], wsem.at[slot, 0])]

        def start_late(i):
            pl.when(i < dn0 - 1)(lambda: begin(gu_block(i)))

            @pl.when(i >= dn0 - 1)
            def _():
                pl.when(i == dn0 - 1)(lambda: begin(gu_block(i, rem)))
                for n in range(nk):
                    pl.when((i >= dn0) & (lax.rem(i - dn0, nk) == n))(lambda n=n: begin(dn_block(i, n)))

        mine, theirs = at(tp * h, h, SUB), at(tp * d, d, SUB)
        head_rows, tail_rows = pl.ds(0, h), pl.ds(h, d)
        pairs = [(co_r, tmp.at[0, head_rows]), (do_r, tmp.at[0, tail_rows]), (ci_r, tmp.at[1, head_rows]), (di_r, tmp.at[1, tail_rows])]
        if first:
            pairs += [(rin[0].at[mine], h1.at[head_rows]), (rin[1].at[theirs], h1.at[tail_rows])]
        else:
            split = rin[0].shape[1]
            pairs += [(rin[0], h1.at[:, pl.ds(0, split)]), (rin[1], h1.at[:, pl.ds(split, dm.model - split)])]
        loads = [dma(a, b, isem.at[n]) for n, (a, b) in enumerate(pairs)]
        begin(loads)
        begin(out_block(jnp.int32(0)))
        meet([to_core, to_x, to_y])

        def bulk(i):
            r = at(i * crow, crow, SUB)
            return remote(kv.at[:, r], kvx.at[:, r], xss.at[i], xrs.at[i], to_x)

        def forward(i):
            r = at(i * crow, crow, SUB)
            return remote(kvx.at[:, r], kvq.at[:, r], fss.at[i], frs.at[i], to_core)

        near = remote(kv, kvp, dss.at[0], drs.at[0], to_core)
        finish_all(loads)
        for i in range(1, nb - 1):
            begin(out_block(jnp.int32(i)))
        each(n_dn, lambda i: bulk(i).start())
        for i in range(dm.heads):
            for n, t in enumerate((tp, 1 - tp)):
                xn[:m, at((2 * i + t) * dm.hd, dm.hd)] = tmp[n, :, i * dm.hd:(i + 1) * dm.hd]
        ss[...] = jnp.zeros_like(ss)

        def hsend(j):
            return remote(h1.at[:, cols(j)], h1p.at[:, cols(j)], hss.at[j], hrs.at[j], to_core)

        ss_send = remote(ss, ssp, dss.at[1], drs.at[1], to_core)

        def add_to_hidden(cs, acc):
            out = (h1[:, cs].astype(F32) + acc.astype(BF).astype(F32)).astype(BF)
            h1[:, cs] = out
            return out.astype(F32)

        def out_step(i):
            pl.when(i > 0)(lambda: hsend(i - 1).start())
            pl.when(i + nb - 1 < gu0)(lambda: begin(out_block(i + nb - 1)))
            pl.when(i + nb - 1 >= gu0)(lambda: begin(gu_block(i + nb - 1)))
            finish_all(out_block(i))
            slot = lax.rem(i, nb)
            for n in HALVES:
                acc = jnp.dot(xn[:m, :], wb[slot, :, n:n + WIDE], preferred_element_type=F32)
                out = add_to_hidden(at(i * CHUNK + n, WIDE), acc)
                ss[...] += out[:, :LANES] * out[:, :LANES] + out[:, LANES:] * out[:, LANES:]
        each(n_out, out_step)

        def apply_norm(src, stat, base):
            total_sq = row_sum(stat[...])
            stat[...] = jnp.broadcast_to(lax.rsqrt(total_sq / dm.model + NORM_EPS), stat.shape)

            def step(i):
                sl = at(i * SUB, SUB, SUB)
                for c in range(*dm.lanes):
                    xn[at(base + i * SUB, SUB, SUB), c:c + LANES] = (src[sl, c:c + LANES].astype(F32) * stat[sl, :]).astype(BF)
            each(m // SUB, step)

        ss_send.start()
        hsend(n_out - 1).start()
        ss_send.wait_send()
        apply_norm(h1, ss, 0)
        ss_send.wait_recv()
        each(n_out, lambda j: hsend(j).wait_recv())
        near.start()
        apply_norm(h1p, ssp, m)

        def multiply(i, acc):
            acc[...] = jnp.dot(xn[...], wb[lax.rem(i, nb)], preferred_element_type=F32)

        def glu(acc, j, w):
            gate = acc[:, :w].astype(BF).astype(F32)
            upper = acc[:, w:2 * w].astype(BF).astype(F32)
            act[:, at(j * WIDE, w)] = (jax.nn.silu(gate) * upper).astype(BF)

        begin(gu_block(jnp.int32(gu0 + nb - 1)))
        finish_all(gu_block(jnp.int32(gu0)))
        multiply(jnp.int32(gu0), acc_a)

        def gu_pair(q):
            i = gu0 + 2 * q + 1
            start_late(i + nb - 1)
            finish_all(gu_block(i) + gu_block(i + 1))
            multiply(i, acc_b)
            glu(acc_a, 2 * q, WIDE)
            multiply(i + 1, acc_a)
            glu(acc_b, 2 * q + 1, WIDE)
            start_late(i + nb)
        each(n_full // 2, gu_pair)
        start_late(jnp.int32(dn0 - 2 + nb))
        finish_all(gu_block(jnp.int32(dn0 - 1), rem))
        acc_b[:, :2 * rem] = jnp.dot(xn[...], wb[(dn0 - 1) % nb, :, :2 * rem], preferred_element_type=F32)
        glu(acc_a, n_full - 1, WIDE)
        glu(acc_b, n_full, rem)

        def share(j):
            return remote(h1.at[:, cols(j)], ob.at[:, cols(j)], yss.at[j], yrs.at[j], to_y)

        def keeps(j, fn):
            @pl.when(j < early)
            def _():
                fn(dma(h1.at[:, cols(j)], oa.at[:, cols(j)], osem.at[j]))

            @pl.when(j >= early)
            def _():
                fn(dma(h1.at[:, cols(j)], ot.at[:, cols(j - early)], osem.at[j]))

        def deliver(j):
            keeps(j, lambda c: c.start())
            pl.when(j < early)(lambda: share(j).start())

        def psend_copy(j):
            return remote(psend.at[lax.rem(j, 2)], precv.at[j], pss.at[j], prs.at[j], to_core)

        def finish(j):
            for n in HALVES:
                out = add_to_hidden(at(j * CHUNK + n, WIDE), pown[lax.rem(j, 2), :, n:n + WIDE] + precv[j, :, n:n + WIDE])
                ss[...] += out[:, :LANES] * out[:, :LANES] + out[:, LANES:] * out[:, LANES:]

        def part(rows, slots, n):
            return sum(jnp.dot(act[rows, i * kc:i * kc + ksz[i]], wb[slots[i], :ksz[i], n:n + WIDE], preferred_element_type=F32) for i in range(nk))

        def down(j, lead_in):
            i0 = dn0 + j * nk
            @pl.when(i0 + nb <= total)
            def _():
                if not lead_in:
                    begin(dn_block(i0 + nb - 2, 0))
                begin(dn_block(i0 + nb - 1, 1))
            slots = []
            for n in range(nk):
                finish_all(dn_block(i0 + n, n))
                slots.append(lax.rem(i0 + n, nb))
            half = lax.rem(j, 2)
            pl.when(j > 1)(lambda: psend_copy(j - 2).wait_send())
            if not lead_in:
                psend_copy(j - 1).wait_recv()
                finish(j - 1)
            for n in HALVES:
                psend[half, :, n:n + WIDE] = part(slice(m, 2 * m), slots, n)
            psend_copy(j).start()
            if not lead_in:
                deliver(j - 1)
            for n in HALVES:
                pown[half, :, n:n + WIDE] = part(slice(0, m), slots, n)
            bulk(j).wait_recv()
            forward(j).start()

        each(n_out, lambda j: hsend(j).wait_send())
        ss[...] = jnp.zeros_like(ss)
        down(jnp.int32(0), True)
        each(n_dn - 1, lambda j: down(j + 1, False))
        psend_copy(n_dn - 1).wait_recv()
        finish(n_dn - 1)
        for j in (n_dn - 2, n_dn - 1):
            psend_copy(j).wait_send()
        near.wait()
        deliver(n_dn - 1)
        ss_keep = dma(ss, os, isem.at[0])
        ss_keep.start()
        ss_keep.wait()

        def last(j):
            bulk(j).wait_send()
            forward(j).wait()
            keeps(j, lambda c: c.wait())
            pl.when(j < early)(lambda: share(j).wait())
        each(n_dn, last)

    part1, part2 = sds((m, cut), BF), sds((m, dm.model - cut), BF)
    two = sds(kv3.shape, BF)
    acc = pltpu.VMEM((2 * m, CHUNK), F32)
    pair = pltpu.VMEM((2, m, CHUNK), F32)
    vec = sem((n_dn,))
    stat = pltpu.VMEM((m, LANES), F32)
    return pl.pallas_call(
        kern, out_shape=(part1, part2, part1, sds((m, LANES), F32), two, two, two),
        in_specs=[ANY] * (nr + 9), out_specs=(ANY,) * 7,
        scratch_shapes=[
            pltpu.VMEM((m, dm.model), BF), pltpu.VMEM((m, dm.model), BF), pltpu.VMEM((2 * m, dm.model), BF),
            pltpu.VMEM((2 * m, ffh), BF), pltpu.VMEM((2, m, dm.loc), BF), pltpu.VMEM((nb, kc, CHUNK), BF),
            acc, acc, pair, pltpu.VMEM((n_dn, m, CHUNK), F32), pair, stat, stat,
            sem((nb, 2)), sem((6,)), vec, vec, vec, vec, vec, vec, vec, vec, vec, vec, vec, sem((2,)), sem((2,))],
        compiler_params=params(collective_id=2 + layer, has_side_effects=True),
        cost_estimate=cost(PER * dm.all * dm.model * dm.ff, PER * dm.model * dm.ff),
        name="post")(*resid, co, do, ci, di, kv3, w_out, w_gate, w_up, w_down)


def tail_call(dm, req_len, dest, lengths, kv3, news, kc, vc):
    layers, batch, cache = kc.shape[1:4]
    bits = [1 << b for b in reversed(range(dm.rows.bit_length()))]
    nsrc = len(kv3[0])
    per_layer = batch // PER
    steps = layers * per_layer
    ring = 6
    lag = 2

    def kern(req_ref, dest_ref, len_ref, *refs):
        srcs, refs = refs[:layers * nsrc], refs[layers * nsrc:]
        dec, refs = refs[:layers], refs[layers:]
        kc_ref, vc_ref, ko, vo, kn, vn, buf, slots, dv, lsem, osem, dsem, isem, wsem = refs
        side = lax.axis_index('side')
        start, length = 0, 0
        for r, end in enumerate(request_ends(req_ref)):
            here = dest_ref[r] == side
            start = jnp.where(here, end - req_ref[r], start)
            length = jnp.where(here, req_ref[r], length)

        def pieces(fn):
            for k in range(nsrc):
                first = dm.rows * (side ^ k)
                lo = jnp.maximum(start, first)
                cnt = jnp.maximum(jnp.minimum(start + length, first + dm.rows) - lo, 0)
                for n, bit in enumerate(bits):
                    @pl.when((cnt & bit) != 0)
                    def _(k=k, n=n, bit=bit, first=first, lo=lo, cnt=cnt):
                        off = cnt // (2 * bit) * (2 * bit)
                        for l in range(layers):
                            fn(dma(srcs[l * nsrc + k].at[:, pl.ds(lo - first + off, bit)], buf.at[l, :, pl.ds(lo - start + off, bit)], lsem.at[l, k, n]))

        def spot(i):
            return i // per_layer, at(PER * lax.rem(i, per_layer), PER, PER), lax.rem(i, ring)

        def read(i):
            lay, b, slot = spot(i)
            return [dma(ref.at[0, lay, b], slots.at[slot, n], isem.at[slot, n]) for n, ref in enumerate((kc_ref, vc_ref))]

        def write(i):
            lay, b, slot = spot(i)
            return [dma(slots.at[slot, n], ref.at[0, lay, b], wsem.at[slot, n]) for n, ref in enumerate((kn, vn))]

        dloads = [dma(ref, dv.at[n], dsem.at[n]) for n, ref in enumerate(dec)]
        begin(dloads)
        pieces(lambda c: c.start())
        for i in range(ring - lag):
            begin(read(jnp.int32(i)))

        def zero(r, c):
            buf[:, :, r] = jnp.zeros((layers, 2, dm.heads, dm.hd), BF)
            return c
        lax.fori_loop(length, dm.max_req, zero, 0)
        finish_all(dloads)
        pieces(lambda c: c.wait())
        outs = [dma(buf.at[l, n], ref.at[0, l], osem.at[l, n]) for l in range(layers) for n, ref in enumerate((ko, vo))]
        begin(outs)

        def step(i):
            lay, _, slot = spot(i)
            finish_all(read(i))
            for n in range(PER):
                b = PER * lax.rem(i, per_layer) + n
                for kind in range(2):
                    slots[slot, kind, n, len_ref[b]] = dv[lay, kind, b]
            pl.when(i > 0)(lambda: begin(write(i - 1)))

            @pl.when(i + ring - lag < steps)
            def _():
                pl.when(i >= lag)(lambda: finish_all(write(i - lag)))
                begin(read(i + ring - lag))
        each(steps, step)
        begin(write(jnp.int32(steps - 1)))
        each(ring, lambda i: finish_all(write(steps - ring + i)))
        finish_all(outs)

    shape = sds((1, layers, dm.max_req, dm.heads, dm.hd), BF)
    three = (dm.heads, dm.hd)
    flat = [ref for group in kv3 for ref in group]
    pair = sem((layers, 2))
    return pl.pallas_call(
        kern, out_shape=(shape, shape, sds(kc.shape, BF), sds(vc.shape, BF)),
        in_specs=[SMEM] * 3 + [ANY] * (len(flat) + layers + 2), out_specs=(ANY,) * 4,
        scratch_shapes=[pltpu.VMEM((layers, 2, dm.max_req) + three, BF), pltpu.VMEM((ring, 2, PER, cache) + three, BF), pltpu.VMEM((layers,) + news[0].shape, BF),
                        sem((layers, nsrc, len(bits))), pair, sem((layers,)), sem((ring, 2)), sem((ring, 2))],
        compiler_params=params(),
        cost_estimate=cost(10**11, kc.size),
        name="tail")(req_len, dest, lengths, *flat, *news, kc, vc)


def close_call(dm, mine, theirs):
    cut = mine[0].shape[1]
    h, d, k = dm.half, dm.dhalf, dm.blk

    def kern(a1, a2, b1, b2, hid, dec, buf, lsem, osem):
        tp = lax.axis_index('tp')
        moves = []
        for n, (ref, blk, col) in enumerate(((a1, tp, 0), (a2, tp, cut), (b1, 1 - tp, 0), (b2, 1 - tp, cut))):
            cs = pl.ds(col, ref.shape[1])
            rows = blk * k
            moves.append((dma(ref, buf.at[at(rows, k, SUB), cs], lsem.at[n]),
                          [dma(buf.at[at(rows, h, SUB), cs], hid.at[at(blk * h, h, SUB), cs], osem.at[0, n]),
                           dma(buf.at[at(rows + h, d, SUB), cs], dec.at[at(blk * d, d, SUB), cs], osem.at[1, n])]))
        begin([load for load, _ in moves])
        for load, outs in moves:
            load.wait()
            begin(outs)
        for _, outs in moves:
            finish_all(outs)

    return pl.pallas_call(
        kern, out_shape=(sds((dm.rows, dm.model), BF), sds((dm.dec, dm.model), BF)),
        in_specs=[HBM] * 4, out_specs=(ANY, ANY),
        scratch_shapes=[pltpu.VMEM((dm.all, dm.model), BF), sem((4,)), sem((2, 4))],
        compiler_params=params(), name="close")(*mine, *theirs)


def solution(mesh):
    tp_size = mesh.shape['tp']
    side_size = mesh.shape['side']
    rows_spec = P(('pair', 'side'), None)
    batch_spec = P(('pair', 'side'), None, None)
    cache_spec = P(('pair', 'side'), None, None, None, 'tp', None)
    prompt_spec = P(('pair', 'side'), None, None, 'tp', None)

    def swap(val, axis, bit):
        size = tp_size if axis == 'tp' else side_size
        return lax.ppermute(val, axis, [(i, i ^ bit) for i in range(size)])

    def local_step(x_loc, req_len, dest, w_qkv, w_out, w_gate, w_up, w_down, y_loc, kc, vc, clen_loc):
        side = lax.axis_index('side')
        tp = lax.axis_index('tp')
        layers = w_qkv.shape[0]
        rows = x_loc.shape[0]
        y = y_loc[0]
        lengths = clen_loc[0]
        dm = Dims(rows, y.shape[0], x_loc.shape[1], kc.shape[-2], kc.shape[-1], w_gate.shape[2], 2 * rows - rows // 4)

        ends = jnp.sum(jnp.where(jnp.arange(side_size)[:, None] >= jnp.arange(side_size)[None, :], req_len[None, :], 0), axis=1)
        mid = rows * side_size // 2
        fast = mid - jnp.max(jnp.where(ends <= mid, ends, 0)) <= LANES
        half_dim = dm.hd // 2
        inv_freq = ROPE_BASE ** (-jnp.arange(half_dim, dtype=F32) / half_dim)
        freq = jnp.concatenate([inv_freq, inv_freq])[None]

        ins = resid = (x_loc, y)
        fresh, kv_all = [], []
        for layer in range(layers):
            first = layer == 0
            kvh, kv3, qh, dec, co, ci, do, di, tab = front_call(dm, layer, first, ins, w_qkv, freq, lengths, req_len, kc, vc)
            fresh.append(dec)

            def general(i, ctx):
                kv, q, edges, _ = lax.optimization_barrier((kvh, qh, ends, i))
                kvx = swap(kv, 'side', 2)
                kvs = (kv, swap(kv, 'side', 1), kvx, swap(kvx, 'side', 1))
                own, other = (general_attention(dm, jnp.concatenate([b[None], edges]), q, kvs) for b in (tp, 1 - tp))
                return own, swap(other, 'tp', 1)
            co, ci = lax.fori_loop(0, jnp.where(fast, 0, 1), general, (co, ci))
            o1, o2, p1, stat, kv3_x, kv3_p, kv3_q = post_call(dm, layer, first, resid, co, do, ci, di, kv3, w_out, w_gate, w_up, w_down)
            if layer == layers - 1:
                p2 = swap(o2, 'tp', 1)
            kv_all.append((kv3, kv3_p, kv3_x, kv3_q))
            ins, resid = (o1, o2, p1, stat, tab), (o1, o2)
        k_prompt, v_prompt, k_new, v_new = tail_call(dm, req_len, dest, lengths, kv_all, fresh, kc, vc)
        hidden, dec_out = close_call(dm, (o1, o2), (p1, p2))
        return hidden, dec_out[None], k_prompt, v_prompt, k_new, v_new

    return jax.shard_map(local_step, mesh=mesh,
                         in_specs=(rows_spec, P('pair'), P('pair'), P(), P(), P(), P(), P(), batch_spec, cache_spec, cache_spec, rows_spec),
                         out_specs=(rows_spec, batch_spec, prompt_spec, prompt_spec, cache_spec, cache_spec),
                         check_vma=False)
```

```python
import jax
import jax.numpy as jnp
import numpy as np
from jax import lax
from jax.experimental import pallas as pl
from jax.experimental.pallas import tpu as pltpu
from jax.sharding import PartitionSpec as P

ROPE_BASE = 10000.0
NORM_EPS = 1e-5
NEG = -1e30
BF = jnp.bfloat16
F32 = jnp.float32
ANY = pl.BlockSpec(memory_space=pl.ANY)
SMEM = pl.BlockSpec(memory_space=pltpu.SMEM)
WHOLE = pl.BlockSpec(memory_space=pltpu.VMEM)
HBM = pl.BlockSpec(memory_space=pltpu.HBM)
VMEM_LIMIT = 61 * 2**20
LOG2E = 1.4426950408889634
LANES = 128
WIDE = 256
CHUNK = 512
HALVES = (0, WIDE)
SUB = 16
PER = 4
EARLY_SENT = (4, 3)
NT = (((1,), (1,)), ((), ()))
dma = pltpu.make_async_copy
sds = jax.ShapeDtypeStruct
sem = pltpu.SemaphoreType.DMA


def at(start, size, multiple=LANES):
    return pl.ds(pl.multiple_of(start, multiple), size)


def cost(flops, size):
    return pl.CostEstimate(flops=flops, bytes_accessed=size, transcendentals=0)


def params(**kw):
    return pltpu.CompilerParams(vmem_limit_bytes=VMEM_LIMIT, **kw)


def remote(src, dst, send, recv, dev):
    return pltpu.make_async_remote_copy(src_ref=src, dst_ref=dst, send_sem=send, recv_sem=recv, device_id=dev, device_id_type=pl.DeviceIdType.MESH)


def meet(devices):
    barrier = pltpu.get_barrier_semaphore()
    for dev in devices:
        pl.semaphore_signal(barrier, device_id=dev, device_id_type=pl.DeviceIdType.MESH)
    pl.semaphore_wait(barrier, len(devices))


def each(count, fn):
    lax.fori_loop(0, count, lambda i, c: (fn(i), c)[1], 0)


def begin(copies):
    for cp in copies:
        cp.start()


def finish_all(copies):
    for cp in copies:
        cp.wait()


def row_sum(x):
    return jnp.sum(x, axis=1, keepdims=True)


def row_max(x):
    return jnp.max(x, axis=1, keepdims=True)


def norm_rows(ref, base, rows):
    group = 2 if rows % (2 * SUB) == 0 else 1

    def step(i):
        for n in range(group):
            sl = at(base + (group * i + n) * SUB, SUB, SUB)
            wide = ref[sl, :].astype(F32)
            scale = lax.rsqrt(jnp.mean(wide * wide, axis=-1, keepdims=True) + NORM_EPS)
            ref[sl, :] = (wide * scale).astype(BF)
    each(rows // SUB // group, step)


def request_ends(len_ref):
    ends = [len_ref[0]]
    for r in range(1, 4):
        ends.append(ends[-1] + len_ref[r])
    return ends


def segment_start(row, ends):
    start = jnp.zeros_like(row)
    for end in ends:
        start = jnp.where(row >= end, end, start)
    return start


class Dims:
    def __init__(self, rows, dec, model, heads, head_dim, ff, max_req):
        self.rows, self.half = rows, rows // 2
        self.dec, self.dhalf = dec, dec // 2
        self.blk = self.half + self.dhalf
        self.all = 2 * self.blk
        self.model, self.heads, self.hd, self.ff = model, heads, head_dim, ff
        self.max_req = max_req
        self.loc = heads * head_dim
        self.window = LANES + 2 * rows
        self.lanes = (0, model, LANES)


def front_call(dm, layer, first, ins, w_qkv, freq, lengths, req_len, kc, vc):
    nb = 4
    per_sec = dm.heads // PER
    steps = 3 * per_sec
    kv_steps = 2 * per_sec
    h, d, k = dm.half, dm.dhalf, dm.blk
    m = dm.all if first else k
    npass = dm.all // m
    width = PER * dm.hd
    lead = dm.window - dm.rows
    batch, cache = kc.shape[2], kc.shape[3]
    flat = cache * dm.heads
    ring = 4
    dsteps = batch // PER
    ni = len(ins)

    def kern(*refs):
        rin = refs[:ni]
        (w_ref, f_ref, len_ref, req_ref, k_ref, v_ref, kvh, kv3, qh, dec, co, ci, do, di, tab_out,
         tab, perm_ref, xn, wb, kcat, qv, sd, dv, acc_a, acc_b, bias, sbuf, pbuf, cbuf, cr, dsc, dbuf, dout, o3, stat,
         wsem, isem, csem, tsem, pss, prs, ess, ers, yss, yrs, lss, lrs, ksem) = refs[ni:]
        tp = lax.axis_index('tp')
        side = lax.axis_index('side')
        odd = lax.rem(side, 2)
        to_y = {'tp': 1 - tp}

        def wcopies(i):
            slot = lax.rem(i, nb)
            j = lax.rem(i, steps)
            sec = j // per_sec
            base = jnp.where(sec == 2, 0, (sec + 1) * 2 * dm.loc)
            out = []
            for n in range(PER):
                col = base + (2 * (PER * lax.rem(j, per_sec) + n) + tp) * dm.hd
                out.append(dma(w_ref.at[layer, :, at(col, dm.hd)], wb.at[slot, :, pl.ds(n * dm.hd, dm.hd)], wsem.at[slot, n]))
            return out

        def group_of(i):
            return lax.rem(i + tp * (dsteps // 2), dsteps)

        def caches(i):
            slot = lax.rem(i, ring)
            b = at(PER * group_of(i), PER, PER)
            return [dma(ref.at[0, layer, b], cr.at[slot, n], csem.at[slot, n]) for n, ref in enumerate((k_ref, v_ref))]

        if first:
            parts = [(rin[0], 0, 0, h), (rin[1], 0, h, d), (rin[0], h, k, h), (rin[1], d, k + h, d)]
            loads = [dma(ref.at[pl.ds(src, n)], xn.at[pl.ds(dst, n)], isem.at[i]) for i, (ref, src, dst, n) in enumerate(parts)]
        else:
            own1, own2, peer1, ss_in, tab_in = rin
            cut = own1.shape[1]
            head_cols, tail_cols = pl.ds(0, cut), pl.ds(cut, dm.model - cut)
            top, low_rows = pl.ds(0, k), pl.ds(k, k)
            loads = [dma(own1, xn.at[top, head_cols], isem.at[0]), dma(own2, xn.at[top, tail_cols], isem.at[1]),
                     dma(ss_in, stat.at[0], isem.at[2]), dma(peer1, xn.at[low_rows, head_cols], isem.at[3]), dma(tab_in, tab, tsem.at[1])]
        begin(loads)
        begin(wcopies(jnp.int32(0)))

        def zero(i):
            kcat[:, i, pl.ds(0, lead), :] = jnp.zeros((2, lead, dm.hd), BF)
        each(dm.heads, zero)
        src = lax.broadcasted_iota(jnp.int32, perm_ref.shape, 0)
        dst = lax.broadcasted_iota(jnp.int32, perm_ref.shape, 1)
        perm_ref[...] = (lax.rem(src, dm.heads) * SUB + src // dm.heads == dst).astype(F32).astype(BF)
        ends = request_ends(req_ref)

        def table(row, pos):
            size = pos.shape[0]
            ang = pos.astype(F32) * f_ref[...]
            sign = jnp.where(lax.broadcasted_iota(jnp.int32, pos.shape, 1) < dm.hd // 2, -1.0, 1.0)
            tab[0, at(row, size, SUB), :] = jnp.cos(ang)
            tab[1, at(row, size, SUB), :] = jnp.sin(ang) * sign

        if first:
            for b in range(2):
                def rows_table(i):
                    row = dm.rows * side + b * h + i * PER * SUB + lax.broadcasted_iota(jnp.int32, (PER * SUB, LANES), 0)
                    table(b * k + i * PER * SUB, row - segment_start(row, ends))
                each(h // SUB // PER, rows_table)
                which = lax.broadcasted_iota(jnp.int32, (d, LANES), 0)
                pos = jnp.zeros_like(which)
                for i in range(d):
                    pos = jnp.where(which == i, len_ref[b * d + i], pos)
                table(b * k + h, pos)
        meet([{'side': lax.rem(side + i, 4)} for i in range(1, 4)] + [to_y])
        late = []
        if not first:
            late = [remote(own2, xn.at[low_rows, tail_cols], lss.at[0], lrs.at[0], to_y),
                    remote(ss_in, stat.at[1], lss.at[1], lrs.at[1], to_y)]
            begin(late[::-1])

        def own_part(j):
            return kcat.at[j // per_sec, at(PER * lax.rem(j, per_sec), PER, PER), pl.ds(lead, dm.rows)]

        def edge_part(j, row):
            return kcat.at[j // per_sec, at(PER * lax.rem(j, per_sec), PER, PER), pl.ds(row, LANES)]

        def peer_copy(j):
            dst = kcat.at[j // per_sec, at(PER * lax.rem(j, per_sec), PER, PER), pl.ds(LANES, dm.rows)]
            return remote(own_part(j), dst, pss.at[j], prs.at[j], {'side': side + 1})

        def edge_copy(j, to):
            row = dm.window - LANES if to == 2 else dm.rows
            return remote(edge_part(j, row), edge_part(j, (3 - to) * dm.rows), ess.at[j], ers.at[j], {'side': to})

        def send(j):
            pl.when(odd == 0)(lambda: peer_copy(j).start())
            pl.when(side == 1)(lambda: edge_copy(j, 2).start())

        def arrived(j):
            pl.when(odd == 1)(lambda: peer_copy(j).wait_recv())

            @pl.when(side == 2)
            def _():
                edge_copy(j, 2).wait_recv()
                edge_copy(j, 3).start()
            pl.when(side == 3)(lambda: edge_copy(j, 3).wait_recv())

        def sent(j):
            pl.when(odd == 0)(lambda: peer_copy(j).wait_send())
            pl.when(side == 1)(lambda: edge_copy(j, 2).wait_send())
            pl.when(side == 2)(lambda: edge_copy(j, 3).wait_send())

        def ahead(i):
            @pl.when(i + nb - 1 < npass * steps)
            def _():
                begin(wcopies(i + nb - 1))

        def fetch(i, more):
            if more:
                ahead(i)
            finish_all(wcopies(i))

        def multiply(i, rows, acc):
            acc[...] = jnp.dot(xn[rows, :], wb[lax.rem(i, nb)], preferred_element_type=F32)

        def dots(i, rows, acc):
            fetch(i, True)
            multiply(i, rows, acc)

        def epilogue(j, acc, blocks, is_q):
            sec, jj = j // per_sec, lax.rem(j, per_sec)
            for r0, b in blocks:
                rows = slice(r0, r0 + k)
                cv, sv = tab[0, at(b * k, k, SUB), :], tab[1, at(b * k, k, SUB), :]
                for n in range(PER):
                    head = PER * jj + n
                    val = acc[rows, n * dm.hd:(n + 1) * dm.hd].astype(BF).astype(F32)
                    rot = val * cv + pltpu.roll(val, dm.hd // 2, 1) * sv
                    low = (rot if is_q else jnp.where(sec == 1, val, rot)).astype(BF)
                    if is_q:
                        qv[head, at(b * h, h, SUB), :] = low[:h]
                    else:
                        kcat[sec, head, at(lead + b * h, h, SUB), :] = low[:h]
                    sd[sec, head, at(b * d, d, d), :] = low[h:]

        def run(p, blocks):
            rows = pl.ds(p * m, m)
            base = p * steps
            final = p == npass - 1
            last = kv_steps

            def done(j):
                if final:
                    pl.when(j > 0)(lambda: send(j - 1))

            dots(jnp.int32(base), rows, acc_a)

            def pair(q):
                i = base + 2 * q + 1
                fetch(i, True)
                fetch(i + 1, False)
                multiply(i, rows, acc_b)
                epilogue(2 * q, acc_a, blocks, False)
                multiply(i + 1, rows, acc_a)
                epilogue(2 * q + 1, acc_b, blocks, False)
                ahead(i + 1)
                done(2 * q)
                done(2 * q + 1)
            each(last // 2 - 1, pair)
            dots(jnp.int32(base + last - 1), rows, acc_b)
            epilogue(jnp.int32(last - 2), acc_a, blocks, False)
            done(jnp.int32(last - 2))
            if final:
                epilogue(jnp.int32(last - 1), acc_b, blocks, False)
                done(jnp.int32(last - 1))
                return
            dots(jnp.int32(base + last), rows, acc_a)
            epilogue(jnp.int32(last - 1), acc_b, blocks, False)
            for n in range(1, per_sec):
                prev, acc = (acc_a, acc_b) if n % 2 else (acc_b, acc_a)
                dots(jnp.int32(base + last + n), rows, acc)
                epilogue(jnp.int32(last + n - 1), prev, blocks, True)
            epilogue(jnp.int32(steps - 1), acc, blocks, True)

        def apply_norm(n, base):
            total_sq = row_sum(stat[n])
            stat[n] = jnp.broadcast_to(lax.rsqrt(total_sq / dm.model + NORM_EPS), (k, LANES))

            def step(i):
                sl = at(base + i * SUB, SUB, SUB)
                for c in range(*dm.lanes):
                    xn[sl, c:c + LANES] = (xn[sl, c:c + LANES].astype(F32) * stat[n, at(i * SUB, SUB, SUB), :]).astype(BF)
            each(k // SUB, step)

        def fill():
            for i in range(1, nb - 1):
                begin(wcopies(jnp.int32(i)))
            for i in range(2):
                begin(caches(jnp.int32(i)))

        def cols(g):
            return at(width * g, width)

        def ctx_send(g):
            return remote(cbuf.at[0, :, cols(g)], ci.at[:, cols(g)], yss.at[g], yrs.at[g], to_y)

        def ctx_keep(g):
            return dma(cbuf.at[1, :, cols(g)], co.at[:, cols(g)], ksem.at[g])

        dec_send = remote(dout.at[at((1 - tp) * d, d, SUB)], di, yss.at[per_sec], yrs.at[per_sec], to_y)
        dec_keep = dma(dout.at[at(tp * d, d, SUB)], do, isem.at[0])

        def score(b, w, head, n):
            sbuf[n % 2, :, :w] = lax.dot_general(qv[head, b * h:(b + 1) * h, :], kcat[0, head, :w, :], NT, preferred_element_type=F32)

        def value(ph, w, head, n):
            s = sbuf[n % 2, :, :w] * (dm.hd ** -0.5 * LOG2E) + bias[:, :w]
            p = jnp.exp2(s - row_max(s))
            pbuf[n % 2, :, :w] = p.astype(BF)
            tot = row_sum(p)
            o = jnp.dot(pbuf[n % 2, :, :w], kcat[1, head, :w, :], preferred_element_type=F32)
            cbuf[ph, :, at(head * dm.hd, dm.hd)] = (o / tot).astype(BF)

        def turn_rows(rows, out):
            x = jnp.concatenate([r.reshape(SUB * dm.heads, dm.hd) for r in rows], axis=1)
            y = jnp.dot(perm_ref[...], x, preferred_element_type=F32).astype(BF)
            for n, dst in enumerate(out):
                dst(y[:, n * dm.hd:(n + 1) * dm.hd].reshape(SUB, dm.heads, dm.hd))

        def decode_half(part):
            col = lax.broadcasted_iota(jnp.int32, (dm.heads, flat), 1)
            row = lax.broadcasted_iota(jnp.int32, (dm.heads, flat), 0)
            pos = jnp.where(lax.rem(col, dm.heads) == row, col // dm.heads, flat)
            scale = dm.hd ** -0.5
            count = dsteps // 2

            def look(n):
                i = part * count + n

                @pl.when(i + 2 < dsteps)
                def _():
                    begin(caches(i + 2))
                finish_all(caches(i))
                for r in range(PER):
                    keys = cr[lax.rem(i, ring), 0, r].reshape(flat, dm.hd)
                    dsc[n % 2, r] = lax.dot_general(dv[2, PER * group_of(i) + r], keys, NT, preferred_element_type=F32)

            def gather(n):
                i = part * count + n
                for r in range(PER):
                    bi = PER * group_of(i) + r
                    q, kn, vn = (dv[c, bi].astype(F32) for c in (2, 0, 1))
                    s = jnp.where(pos < len_ref[bi], dsc[n % 2, r] * scale, NEG)
                    fresh = row_sum(q * kn) * scale
                    top = jnp.maximum(row_max(s), fresh)
                    p = jnp.exp(s - top)
                    pf = jnp.exp(fresh - top)
                    inv = 1.0 / (row_sum(p) + pf)
                    vals = cr[lax.rem(i, ring), 1, r].reshape(flat, dm.hd)
                    o = jnp.dot((p * inv).astype(BF), vals, preferred_element_type=F32)
                    dbuf[bi] = o + (pf * inv).astype(BF).astype(F32) * vn

            look(0)
            for n in range(count):
                if n + 1 < count:
                    look(n + 1)
                gather(n)

        def put(ref, *idx):
            def store(val):
                ref[idx] = val
            return store

        def turn_block(b):
            sl = at(b * d, d, SUB)
            turn_rows([sd[n, :, sl, :] for n in range(3)], [put(dv, n, sl) for n in range(3)])

            def block(i):
                for n in range(PER):
                    row = b * h + (PER * i + n) * SUB
                    sl, own = at(row, SUB, SUB), at(lead + row, SUB, SUB)
                    turn_rows([kcat[n2, :, own, :] for n2 in range(2)], [put(o3, n2, sl) for n2 in range(2)])
            each(h // SUB // PER, block)

        if first:
            tab_copy = dma(tab, tab_out, tsem.at[1])
            tab_copy.start()
            for cp, (_, _, row, size) in zip(loads, parts):
                cp.wait()
                if row == h:
                    fill()
                norm_rows(xn, row, size)
            blocks = [(0, 0), (k, 1)]
        else:
            finish_all(loads[:3] + loads[4:])
            fill()
            apply_norm(0, 0)
            run(0, [(0, tp)])
            turn_block(tp)
            decode_half(0)
            loads[3].wait()
            finish_all(late)
            apply_norm(1, k)
            blocks = [(0, 1 - tp)]
        run(npass - 1, blocks)

        kv3_copy = dma(o3, kv3, tsem.at[0])
        kvh_copy = dma(kcat.at[:, :, pl.ds(lead, dm.rows)], kvh, isem.at[2])
        q_copy = dma(qv, qh, tsem.at[2])
        dec_copy = dma(dv, dec, tsem.at[3])

        def stage(t):
            ph, g = t // per_sec, lax.rem(t, per_sec)
            b = lax.rem(1 + tp + ph, 2)

            @pl.when(ph == 0)
            def _():
                dots(npass * steps - per_sec + g, pl.ds((npass - 1) * m, m), acc_a)
                epilogue(kv_steps + g, acc_a, blocks, True)
                pl.when(g == 0)(lambda: send(kv_steps - 1))
                arrived(g)
                arrived(per_sec + g)

            @pl.when(t == per_sec)
            def _():
                ctx_send(per_sec - 1).start()
                if first:
                    each(2, turn_block)
                    each(2, decode_half)
                else:
                    turn_block(1 - tp)
                    decode_half(1)
                for n in range(dm.heads):
                    dout[:, n * dm.hd:(n + 1) * dm.hd] = dbuf[:, n, :].astype(BF)
                begin([kv3_copy, kvh_copy, q_copy, dec_copy])

            @pl.when(g == 0)
            def _():
                rows = dm.rows * side + h * b + lax.broadcasted_iota(jnp.int32, (h, LANES), 0)
                start = segment_start(rows, ends)
                lane = dm.rows * side - lead + lax.broadcasted_iota(jnp.int32, (h, LANES), 1)
                for c in range(dm.window // LANES):
                    col = lane + c * LANES
                    bias[:, c * LANES:(c + 1) * LANES] = jnp.where((col >= start) & (col <= rows), 0.0, NEG)
            pl.when(t == per_sec)(lambda: begin([dec_send, dec_keep]))

            for bb, w in enumerate((dm.window - h, dm.window)):
                @pl.when(b == bb)
                def _(bb=bb, w=w):
                    score(bb, w, PER * g, 0)
                    for n in range(PER):
                        if n + 1 < PER:
                            score(bb, w, PER * g + n + 1, n + 1)
                        value(ph, w, PER * g + n, n)
            pl.when((ph == 0) & (g > 0))(lambda: ctx_send(g - 1).start())
            pl.when((ph > 0) & (g > 0))(lambda: ctx_keep(g - 1).start())
        each(2 * per_sec, stage)

        if first:
            tab_copy.wait()
        ctx_keep(per_sec - 1).start()
        each(kv_steps, sent)
        finish_all([kv3_copy, kvh_copy, q_copy, dec_copy, dec_keep, dec_send])
        each(per_sec, lambda g: ctx_keep(g).wait())
        each(per_sec, lambda g: ctx_send(g).wait())

    heads = (dm.heads, dm.rows, dm.hd)
    three = (dm.heads, dm.hd)
    flops = 2 * dm.all * dm.model * width * steps
    outs = [(2,) + heads, (2, dm.rows) + three, heads, (3, dm.dec) + three, (h, dm.loc), (h, dm.loc), (d, dm.loc), (d, dm.loc)]
    acc = pltpu.VMEM((m, width), F32)
    tabs = sds((2, dm.all, LANES), F32)
    vec = sem((kv_steps,))
    return pl.pallas_call(
        kern, out_shape=tuple(sds(s, BF) for s in outs) + (tabs,),
        in_specs=[ANY] * (ni + 1) + [WHOLE] + [SMEM] * 2 + [ANY] * 2, out_specs=(ANY,) * (len(outs) + 1),
        scratch_shapes=[
            pltpu.VMEM(tabs.shape, F32), pltpu.VMEM((SUB * dm.heads, SUB * dm.heads), BF),
            pltpu.VMEM((dm.all, dm.model), BF), pltpu.VMEM((nb, dm.model, width), BF), pltpu.VMEM((2, dm.heads, dm.window, dm.hd), BF),
            pltpu.VMEM(heads, BF), pltpu.VMEM((3, dm.heads, dm.dec, dm.hd), BF), pltpu.VMEM((3, dm.dec) + three, BF), acc, acc,
            pltpu.VMEM((h, dm.window), F32), pltpu.VMEM((2, h, dm.window), F32), pltpu.VMEM((2, h, dm.window), BF), pltpu.VMEM((2, h, dm.loc), BF),
            pltpu.VMEM((ring, 2, PER, cache) + three, BF), pltpu.VMEM((2, PER, dm.heads, flat), F32), pltpu.VMEM((batch,) + three, F32),
            pltpu.VMEM((batch, dm.loc), BF), pltpu.VMEM((2, dm.rows) + three, BF), pltpu.VMEM((2, k, LANES), F32),
            sem((nb, PER)), sem((4,)), sem((ring, 2)), sem((4,)), vec, vec, vec, vec,
            sem((per_sec + 1,)), sem((per_sec + 1,)), sem((2,)), sem((2,)), sem((per_sec,))],
        compiler_params=params(collective_id=layer, has_side_effects=True),
        cost_estimate=cost(flops, dm.model * width * steps * 2),
        name="front")(*ins, w_qkv, freq, lengths, req_len, kc, vc)


def general_attention(dm, meta, qh, kvs):
    nk = LANES + 4 * dm.rows
    groups = dm.heads // PER
    hb = dm.half
    wmax = dm.max_req + hb + WIDE

    def kern(meta_ref, q_ref, *refs):
        srcs = refs[:4]
        o_ref, kcat, sc, bias, mx, ls, pv, lsem = refs[4:]
        g = pl.program_id(0)
        side = lax.axis_index('side')
        row0 = dm.rows * side + hb * meta_ref[0]
        copies = [dma(ref.at[:, at(PER * g, PER, PER)], kcat.at[:, :, at(LANES + dm.rows * (side ^ n), dm.rows)], lsem.at[n]) for n, ref in enumerate(srcs)]
        kcat[:, :, :LANES, :] = jnp.zeros((2, PER, LANES, dm.hd), BF)
        begin(copies)

        ends = [meta_ref[r] for r in range(1, meta_ref.shape[0])]
        n = (row0 + hb - segment_start(row0, ends) // LANES * LANES + WIDE - 1) // WIDE
        begin_col = row0 + hb - WIDE * n
        rows = row0 + lax.broadcasted_iota(jnp.int32, (hb, WIDE), 0)
        st_rows = segment_start(rows, ends)
        lanes = lax.broadcasted_iota(jnp.int32, (hb, WIDE), 1)
        mx[...] = jnp.full_like(mx, NEG)
        ls[...] = jnp.zeros_like(ls)
        pv[...] = jnp.zeros_like(pv)
        finish_all(copies)

        def scores(c):
            first = begin_col + WIDE * c
            col = first + lanes
            bias[...] = jnp.where((col >= st_rows) & (col <= rows), 0.0, NEG)
            for i in range(PER):
                keys = kcat[0, i, at(LANES + first, WIDE), :]
                s = lax.dot_general(q_ref[i], keys, NT, preferred_element_type=F32)
                s = s * (dm.hd ** -0.5 * LOG2E) + bias[...]
                sc[i, :, at(c * WIDE, WIDE)] = s
                mx[i] = jnp.maximum(mx[i], row_max(s))
        each(n, scores)

        def values(c):
            for i in range(PER):
                p = jnp.exp2(sc[i, :, at(c * WIDE, WIDE)] - mx[i][:, :1])
                ls[i] += row_sum(p)
                vals = kcat[1, i, at(LANES + begin_col + WIDE * c, WIDE), :]
                pv[i] += jnp.dot(p.astype(BF), vals, preferred_element_type=F32)
        each(n, values)
        for i in range(PER):
            o_ref[:, i * dm.hd:(i + 1) * dm.hd] = (pv[i] / ls[i]).astype(BF)

    stat = pltpu.VMEM((PER, hb, LANES), F32)
    grid_spec = pltpu.PrefetchScalarGridSpec(
        num_scalar_prefetch=1, grid=(groups,),
        in_specs=[pl.BlockSpec((PER, hb, dm.hd), lambda g, mt: (g, mt[0], 0))] + [ANY] * 4,
        out_specs=pl.BlockSpec((hb, PER * dm.hd), lambda g, mt: (0, g)),
        scratch_shapes=[pltpu.VMEM((2, PER, nk, dm.hd), BF), pltpu.VMEM((PER, hb, wmax), F32), pltpu.VMEM((hb, WIDE), F32), stat, stat, stat, sem((4,))])
    return pl.pallas_call(
        kern, out_shape=sds((hb, dm.loc), BF), grid_spec=grid_spec,
        compiler_params=params(dimension_semantics=("arbitrary",)), name="general_attn")(meta, qh, *kvs)


def post_call(dm, layer, first, resid, co, do, ci, di, kv3, w_out, w_gate, w_up, w_down):
    nb = 6
    kc = dm.model
    ffh = dm.ff // 2
    n_out = dm.model // CHUNK
    n_full = ffh // WIDE
    rem = ffh - n_full * WIDE
    n_gu = n_full + 1
    n_dn = n_out
    ksz = [kc, ffh - kc]
    nk = len(ksz)
    gu0, dn0 = n_out, n_out + n_gu
    total = dn0 + n_dn * nk
    assert rem and n_full % 2
    m = dm.blk
    h, d = dm.half, dm.dhalf
    crow = dm.rows // n_dn
    nr = len(resid)
    early = EARLY_SENT[0 if first else -1]
    cut = early * CHUNK

    def kern(*refs):
        rin = refs[:nr]
        (co_r, do_r, ci_r, di_r, kv, wo, wg, wu, wd, oa, ot, ob, os, kvx, kvp, kvq,
         h1, h1p, xn, act, tmp, wb, acc_a, acc_b, psend, precv, pown, ss, ssp,
         wsem, isem, osem, hss, hrs, pss, prs, yss, yrs, xss, xrs, fss, frs, dss, drs) = refs[nr:]
        tp = lax.axis_index('tp')
        side = lax.axis_index('side')
        core = lax.rem(side, 2)
        to_core = {'side': side + 1 - 2 * core}
        to_x = {'side': lax.rem(side + 2, 4)}
        to_y = {'tp': 1 - tp}

        def cols(j):
            return at(j * CHUNK, CHUNK)

        def out_block(i):
            slot = lax.rem(i, nb)
            return [dma(wo.at[layer, :, cols(i)], wb.at[slot], wsem.at[slot, 0])]

        def gu_block(i, w=WIDE):
            slot = lax.rem(i, nb)
            c = at(core * ffh + (i - gu0) * WIDE, w)
            return [dma(ref.at[layer, :, c], wb.at[slot, :, pl.ds(n * w, w)], wsem.at[slot, n]) for n, ref in enumerate((wg, wu))]

        def dn_block(i, n):
            slot = lax.rem(i, nb)
            r = at(core * ffh + n * kc, ksz[n])
            return [dma(wd.at[layer, r, cols((i - dn0) // nk)], wb.at[slot, pl.ds(0, ksz[n])], wsem.at[slot, 0])]

        def start_late(i):
            pl.when(i < dn0 - 1)(lambda: begin(gu_block(i)))

            @pl.when(i >= dn0 - 1)
            def _():
                pl.when(i == dn0 - 1)(lambda: begin(gu_block(i, rem)))
                for n in range(nk):
                    pl.when((i >= dn0) & (lax.rem(i - dn0, nk) == n))(lambda n=n: begin(dn_block(i, n)))

        mine, theirs = at(tp * h, h, SUB), at(tp * d, d, SUB)
        head_rows, tail_rows = pl.ds(0, h), pl.ds(h, d)
        pairs = [(co_r, tmp.at[0, head_rows]), (do_r, tmp.at[0, tail_rows]), (ci_r, tmp.at[1, head_rows]), (di_r, tmp.at[1, tail_rows])]
        if first:
            pairs += [(rin[0].at[mine], h1.at[head_rows]), (rin[1].at[theirs], h1.at[tail_rows])]
        else:
            split = rin[0].shape[1]
            pairs += [(rin[0], h1.at[:, pl.ds(0, split)]), (rin[1], h1.at[:, pl.ds(split, dm.model - split)])]
        loads = [dma(a, b, isem.at[n]) for n, (a, b) in enumerate(pairs)]
        begin(loads)
        begin(out_block(jnp.int32(0)))
        meet([to_core, to_x, to_y])

        def bulk(i):
            r = at(i * crow, crow, SUB)
            return remote(kv.at[:, r], kvx.at[:, r], xss.at[i], xrs.at[i], to_x)

        def forward(i):
            r = at(i * crow, crow, SUB)
            return remote(kvx.at[:, r], kvq.at[:, r], fss.at[i], frs.at[i], to_core)

        near = remote(kv, kvp, dss.at[0], drs.at[0], to_core)
        finish_all(loads[:PER])
        for i in range(1, nb - 1):
            begin(out_block(jnp.int32(i)))
        each(n_dn, lambda i: bulk(i).start())
        for i in range(dm.heads):
            for n, t in enumerate((tp, 1 - tp)):
                xn[:m, at((2 * i + t) * dm.hd, dm.hd)] = tmp[n, :, i * dm.hd:(i + 1) * dm.hd]
        ss[...] = jnp.zeros_like(ss)
        finish_all(loads[PER:])

        def hsend(j):
            return remote(h1.at[:, cols(j)], h1p.at[:, cols(j)], hss.at[j], hrs.at[j], to_core)

        ss_send = remote(ss, ssp, dss.at[1], drs.at[1], to_core)

        def add_to_hidden(cs, acc):
            out = (h1[:, cs].astype(F32) + acc.astype(BF).astype(F32)).astype(BF)
            h1[:, cs] = out
            return out.astype(F32)

        def out_step(i):
            pl.when(i > 0)(lambda: hsend(i - 1).start())
            pl.when(i + nb - 1 < gu0)(lambda: begin(out_block(i + nb - 1)))
            pl.when(i + nb - 1 >= gu0)(lambda: begin(gu_block(i + nb - 1)))
            finish_all(out_block(i))
            slot = lax.rem(i, nb)
            for n in HALVES:
                acc = jnp.dot(xn[:m, :], wb[slot, :, n:n + WIDE], preferred_element_type=F32)
                out = add_to_hidden(at(i * CHUNK + n, WIDE), acc)
                ss[...] += out[:, :LANES] * out[:, :LANES] + out[:, LANES:] * out[:, LANES:]
        each(n_out, out_step)

        def apply_norm(src, stat, base):
            total_sq = row_sum(stat[...])
            stat[...] = jnp.broadcast_to(lax.rsqrt(total_sq / dm.model + NORM_EPS), stat.shape)

            def step(i):
                sl = at(i * SUB, SUB, SUB)
                for c in range(*dm.lanes):
                    xn[at(base + i * SUB, SUB, SUB), c:c + LANES] = (src[sl, c:c + LANES].astype(F32) * stat[sl, :]).astype(BF)
            each(m // SUB, step)

        ss_send.start()
        hsend(n_out - 1).start()
        ss_send.wait_send()
        apply_norm(h1, ss, 0)
        ss_send.wait_recv()
        each(n_out, lambda j: hsend(j).wait_recv())
        near.start()
        apply_norm(h1p, ssp, m)

        def multiply(i, acc):
            acc[...] = jnp.dot(xn[...], wb[lax.rem(i, nb)], preferred_element_type=F32)

        def glu(acc, j, w):
            gate = acc[:, :w].astype(BF).astype(F32)
            upper = acc[:, w:2 * w].astype(BF).astype(F32)
            act[:, at(j * WIDE, w)] = (jax.nn.silu(gate) * upper).astype(BF)

        begin(gu_block(jnp.int32(gu0 + nb - 1)))
        finish_all(gu_block(jnp.int32(gu0)))
        multiply(jnp.int32(gu0), acc_a)

        def gu_pair(q):
            i = gu0 + 2 * q + 1
            start_late(i + nb - 1)
            finish_all(gu_block(i) + gu_block(i + 1))
            multiply(i, acc_b)
            glu(acc_a, 2 * q, WIDE)
            multiply(i + 1, acc_a)
            glu(acc_b, 2 * q + 1, WIDE)
            start_late(i + nb)
        each(n_full // 2, gu_pair)
        start_late(jnp.int32(dn0 - 2 + nb))
        finish_all(gu_block(jnp.int32(dn0 - 1), rem))
        acc_b[:, :2 * rem] = jnp.dot(xn[...], wb[(dn0 - 1) % nb, :, :2 * rem], preferred_element_type=F32)
        glu(acc_a, n_full - 1, WIDE)
        glu(acc_b, n_full, rem)

        def share(j):
            return remote(h1.at[:, cols(j)], ob.at[:, cols(j)], yss.at[j], yrs.at[j], to_y)

        def keeps(j, fn):
            @pl.when(j < early)
            def _():
                fn(dma(h1.at[:, cols(j)], oa.at[:, cols(j)], osem.at[j]))

            @pl.when(j >= early)
            def _():
                fn(dma(h1.at[:, cols(j)], ot.at[:, cols(j - early)], osem.at[j]))

        def deliver(j):
            keeps(j, lambda c: c.start())
            pl.when(j < early)(lambda: share(j).start())

        def psend_copy(j):
            return remote(psend.at[lax.rem(j, 2)], precv.at[j], pss.at[j], prs.at[j], to_core)

        def finish(j):
            for n in HALVES:
                out = add_to_hidden(at(j * CHUNK + n, WIDE), pown[lax.rem(j, 2), :, n:n + WIDE] + precv[j, :, n:n + WIDE])
                ss[...] += out[:, :LANES] * out[:, :LANES] + out[:, LANES:] * out[:, LANES:]

        def part(rows, slots, n):
            return sum(jnp.dot(act[rows, i * kc:i * kc + ksz[i]], wb[slots[i], :ksz[i], n:n + WIDE], preferred_element_type=F32) for i in range(nk))

        def down(j, lead_in):
            i0 = dn0 + j * nk
            @pl.when(i0 + nb <= total)
            def _():
                if not lead_in:
                    begin(dn_block(i0 + nb - 2, 0))
                begin(dn_block(i0 + nb - 1, 1))
            slots = []
            for n in range(nk):
                finish_all(dn_block(i0 + n, n))
                slots.append(lax.rem(i0 + n, nb))
            half = lax.rem(j, 2)
            pl.when(j > 1)(lambda: psend_copy(j - 2).wait_send())
            if not lead_in:
                psend_copy(j - 1).wait_recv()
                finish(j - 1)
            for n in HALVES:
                psend[half, :, n:n + WIDE] = part(slice(m, 2 * m), slots, n)
            psend_copy(j).start()
            if not lead_in:
                deliver(j - 1)
            for n in HALVES:
                pown[half, :, n:n + WIDE] = part(slice(0, m), slots, n)
            bulk(j).wait_recv()
            forward(j).start()

        each(n_out, lambda j: hsend(j).wait_send())
        ss[...] = jnp.zeros_like(ss)
        down(jnp.int32(0), True)
        each(n_dn - 1, lambda j: down(j + 1, False))
        psend_copy(n_dn - 1).wait_recv()
        finish(n_dn - 1)
        for j in (n_dn - 2, n_dn - 1):
            psend_copy(j).wait_send()
        near.wait()
        deliver(n_dn - 1)
        ss_keep = dma(ss, os, isem.at[0])
        ss_keep.start()
        ss_keep.wait()

        def last(j):
            bulk(j).wait_send()
            forward(j).wait()
            keeps(j, lambda c: c.wait())
            pl.when(j < early)(lambda: share(j).wait())
        each(n_dn, last)

    part1, part2 = sds((m, cut), BF), sds((m, dm.model - cut), BF)
    two = sds(kv3.shape, BF)
    acc = pltpu.VMEM((2 * m, CHUNK), F32)
    pair = pltpu.VMEM((2, m, CHUNK), F32)
    vec = sem((n_dn,))
    stat = pltpu.VMEM((m, LANES), F32)
    return pl.pallas_call(
        kern, out_shape=(part1, part2, part1, sds((m, LANES), F32), two, two, two),
        in_specs=[ANY] * (nr + 9), out_specs=(ANY,) * 7,
        scratch_shapes=[
            pltpu.VMEM((m, dm.model), BF), pltpu.VMEM((m, dm.model), BF), pltpu.VMEM((2 * m, dm.model), BF),
            pltpu.VMEM((2 * m, ffh), BF), pltpu.VMEM((2, m, dm.loc), BF), pltpu.VMEM((nb, kc, CHUNK), BF),
            acc, acc, pair, pltpu.VMEM((n_dn, m, CHUNK), F32), pair, stat, stat,
            sem((nb, 2)), sem((6,)), vec, vec, vec, vec, vec, vec, vec, vec, vec, vec, vec, sem((2,)), sem((2,))],
        compiler_params=params(collective_id=2 + layer, has_side_effects=True),
        cost_estimate=cost(PER * dm.all * dm.model * dm.ff, PER * dm.model * dm.ff),
        name="post")(*resid, co, do, ci, di, kv3, w_out, w_gate, w_up, w_down)


def tail_call(dm, req_len, dest, lengths, kv3, news, kc, vc):
    layers, batch, cache = kc.shape[1:4]
    bits = [1 << b for b in reversed(range(dm.rows.bit_length()))]
    nsrc = len(kv3[0])
    per_layer = batch // PER
    steps = layers * per_layer
    ring = 6
    lag = 2

    def kern(req_ref, dest_ref, len_ref, *refs):
        srcs, refs = refs[:layers * nsrc], refs[layers * nsrc:]
        dec, refs = refs[:layers], refs[layers:]
        kc_ref, vc_ref, ko, vo, kn, vn, buf, slots, dv, lsem, osem, dsem, isem, wsem = refs
        side = lax.axis_index('side')
        start, length = 0, 0
        for r, end in enumerate(request_ends(req_ref)):
            here = dest_ref[r] == side
            start = jnp.where(here, end - req_ref[r], start)
            length = jnp.where(here, req_ref[r], length)

        def pieces(fn):
            for k in range(nsrc):
                first = dm.rows * (side ^ k)
                lo = jnp.maximum(start, first)
                cnt = jnp.maximum(jnp.minimum(start + length, first + dm.rows) - lo, 0)
                for n, bit in enumerate(bits):
                    @pl.when((cnt & bit) != 0)
                    def _(k=k, n=n, bit=bit, first=first, lo=lo, cnt=cnt):
                        off = cnt // (2 * bit) * (2 * bit)
                        for l in range(layers):
                            fn(dma(srcs[l * nsrc + k].at[:, pl.ds(lo - first + off, bit)], buf.at[l, :, pl.ds(lo - start + off, bit)], lsem.at[l, k, n]))

        def spot(i):
            return i // per_layer, at(PER * lax.rem(i, per_layer), PER, PER), lax.rem(i, ring)

        def read(i):
            lay, b, slot = spot(i)
            return [dma(ref.at[0, lay, b], slots.at[slot, n], isem.at[slot, n]) for n, ref in enumerate((kc_ref, vc_ref))]

        def write(i):
            lay, b, slot = spot(i)
            return [dma(slots.at[slot, n], ref.at[0, lay, b], wsem.at[slot, n]) for n, ref in enumerate((kn, vn))]

        dloads = [dma(ref, dv.at[n], dsem.at[n]) for n, ref in enumerate(dec)]
        begin(dloads)
        pieces(lambda c: c.start())
        for i in range(ring - lag):
            begin(read(jnp.int32(i)))

        def zero(r, c):
            buf[:, :, r] = jnp.zeros((layers, 2, dm.heads, dm.hd), BF)
            return c
        lax.fori_loop(length, dm.max_req, zero, 0)
        finish_all(dloads)
        pieces(lambda c: c.wait())
        outs = [dma(buf.at[l, n], ref.at[0, l], osem.at[l, n]) for l in range(layers) for n, ref in enumerate((ko, vo))]
        begin(outs)

        def step(i):
            lay, _, slot = spot(i)
            finish_all(read(i))
            for n in range(PER):
                b = PER * lax.rem(i, per_layer) + n
                for kind in range(2):
                    slots[slot, kind, n, len_ref[b]] = dv[lay, kind, b]
            pl.when(i > 0)(lambda: begin(write(i - 1)))

            @pl.when(i + ring - lag < steps)
            def _():
                pl.when(i >= lag)(lambda: finish_all(write(i - lag)))
                begin(read(i + ring - lag))
        each(steps, step)
        begin(write(jnp.int32(steps - 1)))
        each(ring, lambda i: finish_all(write(steps - ring + i)))
        finish_all(outs)

    shape = sds((1, layers, dm.max_req, dm.heads, dm.hd), BF)
    three = (dm.heads, dm.hd)
    flat = [ref for group in kv3 for ref in group]
    pair = sem((layers, 2))
    return pl.pallas_call(
        kern, out_shape=(shape, shape, sds(kc.shape, BF), sds(vc.shape, BF)),
        in_specs=[SMEM] * 3 + [ANY] * (len(flat) + layers + 2), out_specs=(ANY,) * 4,
        scratch_shapes=[pltpu.VMEM((layers, 2, dm.max_req) + three, BF), pltpu.VMEM((ring, 2, PER, cache) + three, BF), pltpu.VMEM((layers,) + news[0].shape, BF),
                        sem((layers, nsrc, len(bits))), pair, sem((layers,)), sem((ring, 2)), sem((ring, 2))],
        compiler_params=params(),
        cost_estimate=cost(10**11, kc.size),
        name="tail")(req_len, dest, lengths, *flat, *news, kc, vc)


def close_call(dm, mine, theirs):
    cut = mine[0].shape[1]
    h, d, k = dm.half, dm.dhalf, dm.blk

    def kern(a1, a2, b1, b2, hid, dec, buf, lsem, osem):
        tp = lax.axis_index('tp')
        moves = []
        for n, (ref, blk, col) in enumerate(((a1, tp, 0), (a2, tp, cut), (b1, 1 - tp, 0), (b2, 1 - tp, cut))):
            cs = pl.ds(col, ref.shape[1])
            rows = blk * k
            moves.append((dma(ref, buf.at[at(rows, k, SUB), cs], lsem.at[n]),
                          [dma(buf.at[at(rows, h, SUB), cs], hid.at[at(blk * h, h, SUB), cs], osem.at[0, n]),
                           dma(buf.at[at(rows + h, d, SUB), cs], dec.at[at(blk * d, d, SUB), cs], osem.at[1, n])]))
        begin([load for load, _ in moves])
        for load, outs in moves:
            load.wait()
            begin(outs)
        for _, outs in moves:
            finish_all(outs)

    return pl.pallas_call(
        kern, out_shape=(sds((dm.rows, dm.model), BF), sds((dm.dec, dm.model), BF)),
        in_specs=[HBM] * 4, out_specs=(ANY, ANY),
        scratch_shapes=[pltpu.VMEM((dm.all, dm.model), BF), sem((4,)), sem((2, 4))],
        compiler_params=params(), name="close")(*mine, *theirs)


def solution(mesh):
    tp_size = mesh.shape['tp']
    side_size = mesh.shape['side']
    rows_spec = P(('pair', 'side'), None)
    batch_spec = P(('pair', 'side'), None, None)
    cache_spec = P(('pair', 'side'), None, None, None, 'tp', None)
    prompt_spec = P(('pair', 'side'), None, None, 'tp', None)

    def swap(val, axis, bit):
        size = tp_size if axis == 'tp' else side_size
        return lax.ppermute(val, axis, [(i, i ^ bit) for i in range(size)])

    def local_step(x_loc, req_len, dest, w_qkv, w_out, w_gate, w_up, w_down, y_loc, kc, vc, clen_loc):
        side = lax.axis_index('side')
        tp = lax.axis_index('tp')
        layers = w_qkv.shape[0]
        rows = x_loc.shape[0]
        y = y_loc[0]
        lengths = clen_loc[0]
        dm = Dims(rows, y.shape[0], x_loc.shape[1], kc.shape[-2], kc.shape[-1], w_gate.shape[2], 2 * rows - rows // 4)

        ends = jnp.sum(jnp.where(jnp.arange(side_size)[:, None] >= jnp.arange(side_size)[None, :], req_len[None, :], 0), axis=1)
        mid = rows * side_size // 2
        fast = mid - jnp.max(jnp.where(ends <= mid, ends, 0)) <= LANES
        half_dim = dm.hd // 2
        inv_freq = np.float32(ROPE_BASE) ** (-np.arange(half_dim, dtype=np.float32) / half_dim)
        freq = jnp.asarray(np.concatenate([inv_freq, inv_freq])[None], F32)

        ins = resid = (x_loc, y)
        fresh, kv_all = [], []
        for layer in range(layers):
            first = layer == 0
            kvh, kv3, qh, dec, co, ci, do, di, tab = front_call(dm, layer, first, ins, w_qkv, freq, lengths, req_len, kc, vc)
            fresh.append(dec)

            def general(i, ctx):
                kv, q, edges, _ = lax.optimization_barrier((kvh, qh, ends, i))
                kvx = swap(kv, 'side', 2)
                kvs = (kv, swap(kv, 'side', 1), kvx, swap(kvx, 'side', 1))
                own, other = (general_attention(dm, jnp.concatenate([b[None], edges]), q, kvs) for b in (tp, 1 - tp))
                return own, swap(other, 'tp', 1)
            co, ci = lax.fori_loop(0, jnp.where(fast, 0, 1), general, (co, ci))
            o1, o2, p1, stat, kv3_x, kv3_p, kv3_q = post_call(dm, layer, first, resid, co, do, ci, di, kv3, w_out, w_gate, w_up, w_down)
            if layer == layers - 1:
                p2 = swap(o2, 'tp', 1)
            kv_all.append((kv3, kv3_p, kv3_x, kv3_q))
            ins, resid = (o1, o2, p1, stat, tab), (o1, o2)
        k_prompt, v_prompt, k_new, v_new = tail_call(dm, req_len, dest, lengths, kv_all, fresh, kc, vc)
        hidden, dec_out = close_call(dm, (o1, o2), (p1, p2))
        return hidden, dec_out[None], k_prompt, v_prompt, k_new, v_new

    return jax.shard_map(local_step, mesh=mesh,
                         in_specs=(rows_spec, P('pair'), P('pair'), P(), P(), P(), P(), P(), batch_spec, cache_spec, cache_spec, rows_spec),
                         out_specs=(rows_spec, batch_spec, prompt_spec, prompt_spec, cache_spec, cache_spec),
                         check_vma=False)
```
